32 devices in a mesh: layer: 1 (over z), col: 4 (over y), row: 8 (over x, core).
Axes of the slice: x: 4, y: 4, z: 1, core: 2. Of those that a mesh axis runs over, the one named last changes fastest.
The devices are a block of a 4x4x8 slice.
Arguments:
- weight: float32 [1280, 5120], P(('layer', 'row'), 'col')
- grad_in: float32 [1280, 5120], P(('layer', 'row'), 'col')
- mom_first: float32 [1280, 5120], P(('layer', 'row'), 'col')
- mom_second: float32 [1280, 5120], P(('layer', 'row'), 'col')
- stat_left: float32 [1280, 1280], P(('layer', 'row'), 'col')
- stat_right: float32 [5120, 5120], P(('layer', 'row'), 'col')
- basis_left: float32 [1280, 1280], P(('layer', 'row'), 'col')
- basis_right: float32 [5120, 5120], P(('layer', 'row'), 'col')
Outputs:
- output 1: float32 [1280, 5120], P(('layer', 'row'), 'col')
- output 2: float32 [1280, 5120], P(('layer', 'row'), 'col')
- output 3: float32 [1280, 5120], P(('layer', 'row'), 'col')
- output 4: float32 [1280, 1280], P(('layer', 'row'), 'col')
- output 5: float32 [5120, 5120], P(('layer', 'row'), 'col')
All inputs are finite; a program needn't handle non-finite values.
Results may differ from the reference program's by a relative error of at most 0.001.
Values are sent between devices in bfloat16 or wider.
A program may use at most 768 MiB of HBM per device.

```python
import jax
import jax.numpy as jnp
from jax import lax

D = 1280
FF = 5120
STEP = 10
RANK = 16
FACTOR_SIDE = 16

BETA1 = 0.9
BETA2 = 0.9
EPS = 1e-8
LR = 0.1
BIAS_ONE = 1.0 - BETA1 ** STEP
BIAS_TWO = 1.0 - BETA2 ** STEP


def random_basis(base_key, matrix_order):
    sub_keys = jax.random.split(base_key, 5)
    side_b = matrix_order // FACTOR_SIDE
    outer_a = jnp.linalg.qr(jax.random.normal(sub_keys[0], (FACTOR_SIDE, FACTOR_SIDE), jnp.float32))[0]
    outer_b = jnp.linalg.qr(jax.random.normal(sub_keys[1], (side_b, side_b), jnp.float32))[0]
    inner_a = jnp.linalg.qr(jax.random.normal(sub_keys[2], (FACTOR_SIDE, FACTOR_SIDE), jnp.float32))[0]
    inner_b = jnp.linalg.qr(jax.random.normal(sub_keys[3], (side_b, side_b), jnp.float32))[0]
    col_order = jax.random.permutation(sub_keys[4], matrix_order)
    first_kron = jnp.kron(outer_a, outer_b)[:, col_order]
    blocks = first_kron.reshape(matrix_order, FACTOR_SIDE, side_b)
    mixed_basis = jnp.einsum("rst,sp,tq->rpq", blocks, inner_a, inner_b)
    return mixed_basis.reshape(matrix_order, matrix_order)


def setup_inputs(seed: int = 0, part: int = 0) -> dict:
    base_key = jax.random.fold_in(jax.random.key(seed), part)
    sub_keys = jax.random.split(base_key, 12)
    grad_scale = (10.0 / FF) ** 0.5
    noise_part = jax.random.normal(sub_keys[0], (D, FF), jnp.float32)
    left_fac = jax.random.normal(sub_keys[1], (D, RANK), jnp.float32)
    right_fac = jax.random.normal(sub_keys[2], (RANK, FF), jnp.float32)
    low_rank = jnp.dot(left_fac, right_fac) * (3.0 / RANK ** 0.5)
    grad_in = (noise_part + low_rank) * FF ** -0.5
    weight = 0.5 * jax.random.normal(sub_keys[3], (D, FF), jnp.float32)
    mom_first = 0.1 * grad_scale * jax.random.normal(sub_keys[4], (D, FF), jnp.float32)
    mom_second = 0.1 * grad_scale ** 2 * (0.25 + jax.random.normal(sub_keys[5], (D, FF), jnp.float32) ** 2)
    stat_fac_left = jax.random.normal(sub_keys[6], (D, RANK), jnp.float32)
    stat_left = 0.5 * ((9.0 / RANK) * jnp.dot(stat_fac_left, stat_fac_left.T) + jnp.eye(D, dtype=jnp.float32))
    stat_fac_right = jax.random.normal(sub_keys[7], (RANK, FF), jnp.float32)
    stat_right = 0.5 * (D / FF) * ((9.0 / RANK) * jnp.dot(stat_fac_right.T, stat_fac_right) + jnp.eye(FF, dtype=jnp.float32))
    basis_left = random_basis(sub_keys[8], D)
    basis_right = random_basis(sub_keys[9], FF)
    return {"weight": weight, "grad_in": grad_in, "mom_first": mom_first, "mom_second": mom_second, "stat_left": stat_left, "stat_right": stat_right, "basis_left": basis_left, "basis_right": basis_right}


def reference(weight, grad_in, mom_first, mom_second, stat_left, stat_right, basis_left, basis_right):
    highest = lax.Precision.HIGHEST
    new_left = BETA2 * stat_left + (1.0 - BETA2) * jnp.dot(grad_in, grad_in.T, precision=highest, preferred_element_type=jnp.float32)
    new_right = BETA2 * stat_right + (1.0 - BETA2) * jnp.dot(grad_in.T, grad_in, precision=highest, preferred_element_type=jnp.float32)
    left_bf = basis_left.astype(jnp.bfloat16)
    right_bf = basis_right.astype(jnp.bfloat16)
    inner_rot = jnp.dot(grad_in.astype(jnp.bfloat16), right_bf, preferred_element_type=jnp.float32).astype(jnp.bfloat16)
    rotated = jnp.dot(left_bf.T, inner_rot, preferred_element_type=jnp.float32)
    new_first = BETA1 * mom_first + (1.0 - BETA1) * rotated
    new_second = BETA2 * mom_second + (1.0 - BETA2) * rotated * rotated
    direction = (new_first / BIAS_ONE) / (jnp.sqrt(new_second / BIAS_TWO) + EPS)
    back_inner = jnp.dot(left_bf, direction.astype(jnp.bfloat16), preferred_element_type=jnp.float32).astype(jnp.bfloat16)
    step_update = jnp.dot(back_inner, right_bf.T, preferred_element_type=jnp.float32)
    new_weight = weight - LR * step_update
    return (new_weight, new_first, new_second, new_left, new_right)
```

```python
import jax
import jax.numpy as jnp
from jax import lax
from jax.experimental import pallas as pl
from jax.experimental.pallas import tpu as pltpu
from jax.sharding import PartitionSpec as P

BETA1 = 0.9
BETA2 = 0.9
EPS = 1e-8
LR = 0.1
STEP = 10
BIAS_ONE = 1.0 - BETA1 ** STEP
BIAS_TWO = 1.0 - BETA2 ** STEP
MESH = pl.DeviceIdType.MESH
N_REMOTE = 112
N_LOCAL = 16
F32 = jnp.float32
BF16 = jnp.bfloat16
SIX_PASSES = ((0, 0), (0, 1), (1, 0), (0, 2), (1, 1), (2, 0))


def dot(a, b, dims=((1,), (0,))):
    return lax.dot_general(a, b, (dims, ((), ())), preferred_element_type=F32)


def split_three(a):
    hi = a.astype(BF16)
    rest = a - hi.astype(F32)
    mid = rest.astype(BF16)
    return hi, mid, (rest - mid.astype(F32)).astype(BF16)


def kernel(w_in, g_in, m_in, v_in, l_in, r_in, ql_in, qr_in, w_out, m_out, v_out, l_out, r_out,
           gf, px, rac, qr, grf, gr, qlf, qlr, qlc, wx, mx, vx, h, nb, hp, hx, kb, uc, uf, un,
           lst, lc, lf, ln, lhs3, rhs3, ss, rs, ls):
    rc, cc = g_in.shape
    cr, hc = 2 * rc, cc // 2
    kk = 2 * cr
    nt = 256 if cc % 256 == 0 else cc
    tb = 128 if kk % 128 == 0 else kk
    row, y = lax.axis_index("row"), lax.axis_index("col")
    x, k = row // 2, row % 2
    d = (y - x + 4) % 4

    def ds(start, size, unit=None):
        return pl.ds(start if isinstance(start, int) else pl.multiple_of(start, unit or size), size)

    kcol, ocol = ds(k * hc, hc), ds((1 - k) * hc, hc)
    krow, orow = ds(k * rc, rc), ds((1 - k) * rc, rc)

    counter, pending = [0], []

    def remote(src, dst, dx=0, dk=0, dy=0, index=None, track=True):
        if index is None:
            index = counter[0]
            counter[0] += 1
        assert index < N_REMOTE
        copy = pltpu.make_async_remote_copy(
            src_ref=src, dst_ref=dst, send_sem=ss.at[index], recv_sem=rs.at[index],
            device_id={"row": ((x + dx + 4) % 4) * 2 + (k + dk) % 2, "col": (y + dy + 4) % 4}, device_id_type=MESH)
        if track:
            pending.append(copy)
        return copy

    lcounter = [0]

    def local(src, dst):
        index = lcounter[0]
        lcounter[0] += 1
        assert index < N_LOCAL
        copy = pltpu.make_async_copy(src, dst, ls.at[index])
        copy.start()
        return copy

    class Ring:
        def __init__(self, buf, rows, axis):
            def cp(s0, half, s1, step):
                return remote(buf.at[rows(s0, half)], buf.at[rows(s1, half)], **{axis: step})
            self.ra, self.lb = cp(0, 0, 1, 1), cp(0, 1, 3, -1)
            self.rb, self.la = cp(0, 1, 1, 1), cp(0, 0, 3, -1)
            self.fr, self.fl = cp(1, 0, 2, 1), cp(3, 1, 2, -1)

        def own(self):
            for c in (self.ra, self.lb, self.rb, self.la):
                c.start()

        def fwd(self):
            self.ra.wait_recv()
            self.fr.start()
            self.lb.wait_recv()
            self.fl.start()

        def near(self):
            self.rb.wait_recv()
            self.la.wait_recv()

        def far(self):
            self.fr.wait_recv()
            self.fl.wait_recv()

    def chunked(total, parts, body):
        size = total // parts

        @pl.loop(0, parts)
        def _(i):
            body(ds(i * size, size), i)

    cp_g = local(g_in, gf.at[krow])
    cp_gk = local(g_in.at[:, kcol], grf.at[krow])
    cp_ql = local(ql_in, qlf.at[krow])
    cp_qr = local(qr_in, rac)
    cp_own = [local(a.at[:, kcol], b.at[krow]) for a, b in ((m_in, mx), (v_in, vx), (w_in, wx))]
    cp_l = local(l_in, lst)
    barrier = pltpu.get_barrier_semaphore()
    for dx, dk, dy in ((1, 0, 0), (-1, 0, 0), (2, 0, 0), (0, 1, 0), (0, 0, 1), (0, 0, -1)):
        pl.semaphore_signal(barrier, inc=1, device_id={"row": ((x + dx + 4) % 4) * 2 + (k + dk) % 2, "col": (y + dy + 4) % 4},
                            device_id_type=MESH)
    pl.semaphore_wait(barrier, 6)

    d_gk = remote(g_in.at[:, ocol], grf.at[krow], dk=1)
    d_ql = remote(ql_in, qlf.at[krow], dk=1)
    d_g0 = remote(g_in, gf.at[krow], dk=1)
    d_own = [remote(a.at[:, ocol], b.at[krow], dk=1) for a, b in ((m_in, mx), (v_in, vx), (w_in, wx))]
    d_gk.start()
    d_ql.start()

    def grow(s, half):
        return ds((s * 2 + k) * rc + half * (rc // 2), rc // 2)

    def slot_rows(n):
        return lambda s, half: ds(s * n + half * (n // 2), n // 2)

    x1 = Ring(gf, grow, "dx")
    x2 = Ring(qr, slot_rows(hc), "dx")
    x3 = Ring(h, slot_rows(cr), "dx")
    x4 = Ring(nb, slot_rows(cr), "dx")
    y1 = Ring(gr, slot_rows(cr), "dy")
    y2 = Ring(qlr, slot_rows(cr), "dy")

    cp_g.wait()
    x1.own()
    cp_gk.wait()
    d_gk.wait_recv()
    chunked(cr, 4, lambda r, i: gr.__setitem__((r, slice(None)), grf[r, :].astype(BF16)))
    y1.own()
    cp_ql.wait()
    d_ql.wait_recv()
    qlr[ds(0, cr), :] = qlf[...].astype(BF16)
    y2.own()
    d_g0.start()
    for c in d_own:
        c.start()
    cp_qr.wait()
    chunked(hc, 8, lambda r, i: qr.__setitem__((r, slice(None)), rac[r, :].astype(BF16)))
    cp_r = local(r_in, rac)

    x1.fwd()
    x2.own()
    y1.fwd()
    y2.fwd()
    x1.near()

    def whole(s):
        return ds((s * 2 + k) * rc, rc)

    d_g = {s: remote(gf.at[whole(s)], gf.at[whole(s)], dk=1) for s in (1, 3, 2)}
    d_g[1].start()
    d_g[3].start()

    def prow(s, c):
        return ds((s * 2 + c) * rc, rc)

    p_src, p_fwd, q_src, q_fwd = {}, {}, {}, {}
    for s in (0, 1, 3, 2):
        pi, qi = counter[0], counter[0] + 1
        counter[0] += 2
        p_src[s] = remote(gf.at[prow(s, 0), kcol], px.at[prow(s, 0)], dy=1, index=pi, track=False)
        p_fwd[s] = remote(px.at[prow(s, 0)], px.at[prow(s, 0)], dy=1, index=pi, track=False)
        q_src[s] = remote(gf.at[prow(s, 1), kcol], px.at[prow(s, 1)], dy=-1, index=qi, track=False)
        q_fwd[s] = remote(px.at[prow(s, 1)], px.at[prow(s, 1)], dy=-1, index=qi, track=False)

    def panel_source(s):
        @pl.when(d == 0)
        def _():
            p_src[s].start()
            q_src[s].start()

    def panel_relay(s):
        @pl.when(d == 3)
        def _():
            q_fwd[s].wait_recv()
            q_fwd[s].start()

        @pl.when(d != 0)
        def _():
            p_fwd[s].wait_recv()

        @pl.when((d == 1) | (d == 2))
        def _():
            p_fwd[s].start()
            q_fwd[s].wait_recv()

        @pl.when(d == 2)
        def _():
            q_fwd[s].start()

    d_g0.wait_recv()
    panel_source(0)
    y1.near()
    y2.near()
    y1.far()
    y2.far()
    d_g[1].wait_recv()
    panel_source(1)
    d_g[3].wait_recv()
    panel_source(3)

    qlc[ds(0, cr), :] = qlr[ds(d * cr, cr), :]
    a2a = []
    for s in (1, 3, 2):
        t = (y - x - s + 8) % 4
        a2a.append((s, remote(qlr.at[ds(t * cr + k * rc, rc, rc)], qlc.at[whole(s)], dx=s)))
        a2a[-1][1].start()

    def h_part(s):
        t = (d + s) % 4

        def body(cols, i):
            part = dot(gr[ds(t * cr, cr), :], qr[ds(s * hc, hc), cols])
            if s == 0:
                hp[:, cols] = part
            else:
                hp[:, cols] += part

        chunked(cc, cc // nt, lambda cols, i: body(cols, i))

    h_part(0)
    x1.far()
    d_g[2].start()
    panel_relay(0)
    panel_relay(1)
    d_c = [remote(qlc.at[whole(s)], qlc.at[whole(s)], dk=1) for s, _ in a2a]
    for (s, c), e in zip(a2a, d_c):
        c.wait_recv()
        e.start()
    d_g[2].wait_recv()
    panel_source(2)

    def r_piece(p):
        base = p * kk

        @pl.when(d == 0)
        def _():
            chunked(kk, 4, lambda r, i: px.__setitem__(
                (ds(base + i * (kk // 4), kk // 4, 8), slice(None)), gf[ds(base + i * (kk // 4), kk // 4, 8), kcol]))

        def split_right(r, i):
            for q, piece in enumerate(split_three(gf[ds(base + i * (kk // 8), kk // 8, 8), :])):
                rhs3[ds(q * kk + i * (kk // 8), kk // 8, 8), :] = piece

        chunked(kk, 8, split_right)

        def split_left(cols, i):
            for q, piece in enumerate(split_three(px[ds(base + i * tb, tb, 8), :].T)):
                lhs3[ds(q * hc, hc), cols] = piece

        chunked(kk, kk // tb, split_left)

        def product(rows2, cols):
            acc = sum(dot(lhs3[ds(a * hc + rows2 * (hc // 2), hc // 2, 8), :], rhs3[ds(b * kk, kk), cols]) for a, b in SIX_PASSES)
            at = (ds(rows2 * (hc // 2), hc // 2), cols)
            if p == 0:
                rac[at] = BETA2 * rac[at] + (1.0 - BETA2) * acc
            else:
                rac[at] += (1.0 - BETA2) * acc

        @pl.loop(0, 2)
        def _(m):
            chunked(cc, cc // nt, lambda cols, i: product(m, cols))

    cp_r.wait()
    r_piece(0)
    x2.fwd()
    panel_relay(3)
    panel_relay(2)
    r_piece(1)
    out_r = local(rac, r_out)

    class Sum:
        def __init__(self, buf, far, near, n, compute):
            self.buf, self.far_, self.near_, self.n, self.compute = buf, far, near, n, compute
            hn = n // 2
            self.rows = lambda e, half: ds(e * n + half * hn, hn)
            rows = self.rows
            self.fa = remote(buf.at[rows(2, 0)], far.at[ds(0, hn)], dy=1)
            self.fb = remote(buf.at[rows(2, 1)], far.at[ds(hn, hn)], dy=-1)
            self.r1b = remote(buf.at[rows(1, 1)], near.at[ds(hn, hn)], dy=1)
            self.l1a = remote(buf.at[rows(3, 0)], near.at[ds(n, hn)], dy=-1)
            self.r1a = remote(buf.at[rows(1, 0)], near.at[ds(0, hn)], dy=1)
            self.l1b = remote(buf.at[rows(3, 1)], near.at[ds(n + hn, hn)], dy=-1)

        def begin(self):
            self.compute(2)
            self.fa.start()
            self.fb.start()
            self.compute(1)
            self.r1b.start()
            self.compute(3)
            self.l1a.start()
            self.compute(0)

        def middle(self):
            hn, buf, far, rows = self.n // 2, self.buf, self.far_, self.rows
            self.fa.wait_recv()
            buf[rows(1, 0), :] += far[ds(0, hn), :]
            self.r1a.start()
            self.fb.wait_recv()
            buf[rows(3, 1), :] += far[ds(hn, hn), :]
            self.l1b.start()

        def finish(self):
            for c in (self.r1b, self.l1a, self.r1a, self.l1b):
                c.wait_recv()

        def total(self, start, size):
            n = self.n
            return self.buf[ds(start, size, 8), :] + (self.near_[ds(start, size, 8), :] + self.near_[ds(n + start, size, 8), :])

    for q, piece in enumerate(split_three(gf[krow, :])):
        rhs3[ds(3 * cr + q * rc, rc), :] = piece

    def l_chunk(e):
        s = (x - y - e + 8) % 4

        def split_block(r, i):
            for q, piece in enumerate(split_three(gf[ds(s * cr + i * (cr // 4), cr // 4, 8), :])):
                rhs3[ds(q * cr + i * (cr // 4), cr // 4, 8), :] = piece

        chunked(cr, 4, split_block)
        lc[ds(e * rc, rc), :] = sum(
            dot(rhs3[ds(3 * cr + a * rc, rc), :], rhs3[ds(b * cr, cr), :], ((1,), (1,))) for a, b in SIX_PASSES)

    l_sum = Sum(lc, lf, ln, rc, l_chunk)
    l_sum.begin()
    l_sum.middle()

    x2.near()
    h_part(1)
    h_part(3)
    x2.far()
    h_part(2)
    d_h = remote(hp.at[:, ocol], hx, dk=1)
    d_h.start()
    d_h.wait_recv()
    chunked(cr, 4, lambda r, i: h.__setitem__((r, slice(None)), (hp[r, kcol] + hx[r, :]).astype(BF16)))
    x3.own()
    l_sum.finish()
    cp_l.wait()
    lst[...] = BETA2 * lst[...] + (1.0 - BETA2) * l_sum.total(0, rc)
    out_l = local(lst, l_out)
    for c in cp_own:
        c.wait()
    for c in d_own:
        c.wait_recv()
    for c in d_c:
        c.wait_recv()
    x3.fwd()
    x3.near()
    x3.far()

    hx[...] = dot(qlc[...], h[...], ((0,), (0,)))

    def moments(r, i):
        rotated = hx[r, :]
        new_first = BETA1 * mx[r, :] + (1.0 - BETA1) * rotated
        new_second = BETA2 * vx[r, :] + (1.0 - BETA2) * rotated * rotated
        mx[r, :] = new_first
        vx[r, :] = new_second
        direction = (new_first / BIAS_ONE) / (jnp.sqrt(new_second / BIAS_TWO) + EPS)
        nb[r, :] = direction.astype(BF16)

    chunked(cr, 10 if cr % 160 == 0 else 1, moments)
    x4.own()
    outs = []
    for buf, out in ((mx, m_out), (vx, v_out)):
        outs.append(remote(buf.at[orow], out.at[:, kcol], dk=1))
        outs[-1].start()
    out_own = [local(buf.at[krow], out.at[:, kcol]) for buf, out in ((mx, m_out), (vx, v_out))]
    x4.fwd()
    x4.near()
    x4.far()

    kval = sum(dot(qlr[ds(((d + s) % 4) * cr, cr), :], nb[ds(s * cr, cr), :]) for s in range(4))
    kb[ds(k * cr, cr), :] = kval.astype(BF16)
    d_k = remote(kb.at[ds(k * cr, cr)], kb.at[ds(k * cr, cr)], dk=1)
    d_k.start()
    d_k.wait_recv()

    def u_chunk(e):
        s = (x - y - e + 8) % 4
        rows = ds(s * hc, hc)
        uc[ds(e * cr, cr), :] = (dot(kb[ds(0, cr), :], qr[rows, ds(0, hc)], ((1,), (1,)))
                                 + dot(kb[ds(cr, cr), :], qr[rows, ds(hc, hc)], ((1,), (1,))))

    u_sum = Sum(uc, uf, un, cr, u_chunk)
    u_sum.begin()
    u_sum.middle()
    u_sum.finish()

    def final(r, i):
        wx[r, :] = wx[r, :] - LR * u_sum.total(i * (cr // 4), cr // 4)

    chunked(cr, 4, final)
    outs.append(remote(wx.at[orow], w_out.at[:, kcol], dk=1))
    outs[-1].start()
    out_own.append(local(wx.at[krow], w_out.at[:, kcol]))
    for c in outs:
        c.wait_recv()
    for c in out_own + [out_l, out_r]:
        c.wait()
    for c in pending:
        c.wait_send()
    for s in (0, 1, 3, 2):
        @pl.when(d != 3)
        def _():
            p_fwd[s].wait_send()

        @pl.when(d != 1)
        def _():
            q_fwd[s].wait_send()


def solution(mesh):
    tile_spec = P(("layer", "row"), "col")

    def step(weight, grad_in, mom_first, mom_second, stat_left, stat_right, basis_left, basis_right):
        rc, cc = grad_in.shape
        cr, hc, q = 2 * rc, cc // 2, basis_left.shape[1]
        scratch = [
            ((4 * cr, cc), F32), ((4 * cr, hc), F32), ((hc, cc), F32), ((4 * hc, cc), BF16),
            ((cr, hc), F32), ((4 * cr, hc), BF16),
            ((cr, q), F32), ((4 * cr, q), BF16), ((4 * cr, q), BF16),
            ((cr, hc), F32), ((cr, hc), F32), ((cr, hc), F32),
            ((4 * cr, hc), BF16), ((4 * cr, hc), BF16), ((cr, cc), F32), ((cr, hc), F32),
            ((2 * cr, hc), BF16), ((4 * cr, hc), F32), ((cr, hc), F32), ((2 * cr, hc), F32),
            ((rc, q), F32), ((4 * rc, q), F32), ((rc, q), F32), ((2 * rc, q), F32),
            ((3 * hc, 2 * cr), BF16), ((6 * cr, cc), BF16),
        ]
        args = (weight, grad_in, mom_first, mom_second, stat_left, stat_right, basis_left, basis_right)
        any_spec = pl.BlockSpec(memory_space=pl.ANY)
        return pl.pallas_call(
            kernel,
            out_shape=tuple(jax.ShapeDtypeStruct(a.shape, F32)
                            for a in (weight, mom_first, mom_second, stat_left, stat_right)),
            in_specs=[any_spec] * 8,
            out_specs=(any_spec,) * 5,
            scratch_shapes=[pltpu.VMEM(s, t) for s, t in scratch]
            + [pltpu.SemaphoreType.DMA((N_REMOTE,)), pltpu.SemaphoreType.DMA((N_REMOTE,)), pltpu.SemaphoreType.DMA((N_LOCAL,))],
            compiler_params=pltpu.CompilerParams(collective_id=0, has_side_effects=True, vmem_limit_bytes=67_000_000),
        )(*args)

    return jax.shard_map(step, mesh=mesh, in_specs=(tile_spec,) * 8, out_specs=(tile_spec,) * 5, check_vma=False)
```

```python
import jax
import jax.numpy as jnp
from jax import lax
from jax.experimental import pallas as pl
from jax.experimental.pallas import tpu as pltpu
from jax.sharding import PartitionSpec as P

BETA1 = 0.9
BETA2 = 0.9
EPS = 1e-8
LR = 0.1
STEP = 10
BIAS_ONE = 1.0 - BETA1 ** STEP
BIAS_TWO = 1.0 - BETA2 ** STEP
MESH = pl.DeviceIdType.MESH
N_REMOTE = 112
N_LOCAL = 16
F32 = jnp.float32
BF16 = jnp.bfloat16
SIX_PASSES = ((0, 0), (0, 1), (1, 0), (0, 2), (1, 1), (2, 0))


def dot(a, b, dims=((1,), (0,))):
    return lax.dot_general(a, b, (dims, ((), ())), preferred_element_type=F32)


def split_three(a):
    hi = a.astype(BF16)
    rest = a - hi.astype(F32)
    mid = rest.astype(BF16)
    return hi, mid, (rest - mid.astype(F32)).astype(BF16)


def kernel(w_in, g_in, m_in, v_in, l_in, r_in, ql_in, qr_in, w_out, m_out, v_out, l_out, r_out,
           gf, px, rac, qr, grf, gr, qlf, qlr, qlc, wx, mx, vx, h, nb, hp, hx, kb, uc, uf, un,
           lst, lc, lf, ln, lhs3, rhs3, la, ss, rs, ls):
    rc, cc = g_in.shape
    cr, hc = 2 * rc, cc // 2
    kk = 2 * cr
    nt = 256 if cc % 256 == 0 else cc
    tb = 128 if kk % 128 == 0 else kk
    row, y = lax.axis_index("row"), lax.axis_index("col")
    x, k = row // 2, row % 2
    d = (y - x + 4) % 4

    def ds(start, size, unit=None):
        return pl.ds(start if isinstance(start, int) else pl.multiple_of(start, unit or size), size)

    kcol, ocol = ds(k * hc, hc), ds((1 - k) * hc, hc)
    krow, orow = ds(k * rc, rc), ds((1 - k) * rc, rc)

    counter, pending = [0], []

    def remote(src, dst, dx=0, dk=0, dy=0, index=None, track=True):
        if index is None:
            index = counter[0]
            counter[0] += 1
        assert index < N_REMOTE
        copy = pltpu.make_async_remote_copy(
            src_ref=src, dst_ref=dst, send_sem=ss.at[index], recv_sem=rs.at[index],
            device_id={"row": ((x + dx + 4) % 4) * 2 + (k + dk) % 2, "col": (y + dy + 4) % 4}, device_id_type=MESH)
        if track:
            pending.append(copy)
        return copy

    lcounter = [0]

    def local(src, dst):
        index = lcounter[0]
        lcounter[0] += 1
        assert index < N_LOCAL
        copy = pltpu.make_async_copy(src, dst, ls.at[index])
        copy.start()
        return copy

    class Ring:
        def __init__(self, buf, rows, axis):
            def cp(s0, half, s1, step):
                return remote(buf.at[rows(s0, half)], buf.at[rows(s1, half)], **{axis: step})
            self.ra, self.lb = cp(0, 0, 1, 1), cp(0, 1, 3, -1)
            self.rb, self.la = cp(0, 1, 1, 1), cp(0, 0, 3, -1)
            self.fr, self.fl = cp(1, 0, 2, 1), cp(3, 1, 2, -1)

        def own(self):
            for c in (self.ra, self.lb, self.rb, self.la):
                c.start()

        def fwd(self):
            self.ra.wait_recv()
            self.fr.start()
            self.lb.wait_recv()
            self.fl.start()

        def near(self):
            self.rb.wait_recv()
            self.la.wait_recv()

        def far(self):
            self.fr.wait_recv()
            self.fl.wait_recv()

    def chunked(total, parts, body):
        size = total // parts

        @pl.loop(0, parts)
        def _(i):
            body(ds(i * size, size), i)

    cp_g = local(g_in, gf.at[krow])
    cp_gk = local(g_in.at[:, kcol], grf.at[krow])
    cp_ql = local(ql_in, qlf.at[krow])
    cp_qr = local(qr_in, rac)
    cp_own = [local(a.at[:, kcol], b.at[krow]) for a, b in ((m_in, mx), (v_in, vx), (w_in, wx))]
    cp_l = local(l_in, lst)
    barrier = pltpu.get_barrier_semaphore()
    for dx, dk, dy in ((1, 0, 0), (-1, 0, 0), (2, 0, 0), (0, 1, 0), (0, 0, 1), (0, 0, -1)):
        pl.semaphore_signal(barrier, inc=1, device_id={"row": ((x + dx + 4) % 4) * 2 + (k + dk) % 2, "col": (y + dy + 4) % 4},
                            device_id_type=MESH)
    pl.semaphore_wait(barrier, 6)

    d_gk = remote(g_in.at[:, ocol], grf.at[krow], dk=1)
    d_g0 = remote(g_in, gf.at[krow], dk=1)
    d_ql = remote(ql_in, qlf.at[krow], dk=1)
    d_own = [remote(a.at[:, ocol], b.at[krow], dk=1) for a, b in ((m_in, mx), (v_in, vx), (w_in, wx))]
    d_g0.start()
    d_gk.start()
    d_ql.start()

    def grow(s, half):
        return ds((s * 2 + k) * rc + half * (rc // 2), rc // 2)

    def slot_rows(n):
        return lambda s, half: ds(s * n + half * (n // 2), n // 2)

    def whole(s):
        return ds((s * 2 + k) * rc, rc)

    x1 = Ring(gf, grow, "dx")
    x2 = Ring(qr, slot_rows(hc), "dx")
    x3 = Ring(h, slot_rows(cr), "dx")
    x4 = Ring(nb, slot_rows(cr), "dx")
    y1 = Ring(gr, slot_rows(cr), "dy")
    y2 = Ring(qlr, slot_rows(cr), "dy")
    d_g = {s: remote(gf.at[whole(s)], gf.at[whole(s)], dk=1) for s in (1, 3, 2)}

    def prow(s, c):
        return ds((s * 2 + c) * rc, rc)

    p_src, p_fwd, q_src, q_fwd = {}, {}, {}, {}
    for s in (0, 1, 3, 2):
        pi, qi = counter[0], counter[0] + 1
        counter[0] += 2
        p_src[s] = remote(gf.at[prow(s, 0), kcol], px.at[prow(s, 0)], dy=1, index=pi, track=False)
        p_fwd[s] = remote(px.at[prow(s, 0)], px.at[prow(s, 0)], dy=1, index=pi, track=False)
        q_src[s] = remote(gf.at[prow(s, 1), kcol], px.at[prow(s, 1)], dy=-1, index=qi, track=False)
        q_fwd[s] = remote(px.at[prow(s, 1)], px.at[prow(s, 1)], dy=-1, index=qi, track=False)

    def panel_source(s):
        @pl.when(d == 0)
        def _():
            p_src[s].start()
            q_src[s].start()

    def panel_first(s):
        @pl.when(d == 1)
        def _():
            p_fwd[s].wait_recv()
            p_fwd[s].start()

        @pl.when(d == 3)
        def _():
            q_fwd[s].wait_recv()
            q_fwd[s].start()

    def panel_second(s):
        @pl.when(d == 2)
        def _():
            p_fwd[s].wait_recv()
            p_fwd[s].start()
            q_fwd[s].wait_recv()
            q_fwd[s].start()

    def panel_third(s):
        @pl.when(d == 3)
        def _():
            p_fwd[s].wait_recv()

        @pl.when(d == 1)
        def _():
            q_fwd[s].wait_recv()

    def h_part(s, cols):
        t = (d + s) % 4
        part = dot(gr[ds(t * cr, cr), :], qr[ds(s * hc, hc), cols])
        if s == 0:
            hp[:, cols] = part
        else:
            hp[:, cols] += part

    def split_right(p):
        base = p * kk

        def body(r, i):
            for q, piece in enumerate(split_three(gf[ds(base + i * (kk // 8), kk // 8, 8), :])):
                rhs3[ds(q * kk + i * (kk // 8), kk // 8, 8), :] = piece

        chunked(kk, 8, body)
        if p == 0:
            for q in range(3):
                la[ds(q * rc, rc), :] = rhs3[ds(q * kk + k * rc, rc, rc), :]

    def split_left(p):
        base = p * kk

        @pl.when(d == 0)
        def _():
            chunked(kk, 4, lambda r, i: px.__setitem__(
                (ds(base + i * (kk // 4), kk // 4, 8), slice(None)), gf[ds(base + i * (kk // 4), kk // 4, 8), kcol]))

        def body(cols, i):
            for q, piece in enumerate(split_three(px[ds(base + i * tb, tb, 8), :].T)):
                lhs3[ds(q * hc, hc), cols] = piece

        chunked(kk, kk // tb, body)

    def product(p, m):
        def body(cols, i):
            acc = sum(dot(lhs3[ds(a * hc + m * (hc // 2), hc // 2), :], rhs3[ds(b * kk, kk), cols]) for a, b in SIX_PASSES)
            at = (ds(m * (hc // 2), hc // 2), cols)
            if p == 0:
                rac[at] = BETA2 * rac[at] + (1.0 - BETA2) * acc
            else:
                rac[at] += (1.0 - BETA2) * acc

        chunked(cc, cc // nt, body)

    def l_slot(s):
        e = (x - y - s + 8) % 4
        at = [ds(q * kk + (s % 2) * cr, cr) for q in range(3)]
        high = dot(la[...], rhs3[at[0], :], ((1,), (1,)))
        middle = dot(la[ds(0, 2 * rc), :], rhs3[at[1], :], ((1,), (1,)))
        low = dot(la[ds(0, rc), :], rhs3[at[2], :], ((1,), (1,)))
        lc[ds(e * rc, rc), :] = high[:rc] + (high[rc:2 * rc] + middle[:rc]) + (high[2 * rc:] + middle[rc:] + low)

    class Sum:
        def __init__(self, buf, far, near, n, compute):
            self.buf, self.far_, self.near_, self.n, self.compute = buf, far, near, n, compute
            hn = n // 2
            self.rows = lambda e, half: ds(e * n + half * hn, hn)
            rows = self.rows
            self.fa = remote(buf.at[rows(2, 0)], far.at[ds(0, hn)], dy=1)
            self.fb = remote(buf.at[rows(2, 1)], far.at[ds(hn, hn)], dy=-1)
            self.r1b = remote(buf.at[rows(1, 1)], near.at[ds(hn, hn)], dy=1)
            self.l1a = remote(buf.at[rows(3, 0)], near.at[ds(n, hn)], dy=-1)
            self.r1a = remote(buf.at[rows(1, 0)], near.at[ds(0, hn)], dy=1)
            self.l1b = remote(buf.at[rows(3, 1)], near.at[ds(n + hn, hn)], dy=-1)

        def begin(self):
            self.compute(2)
            self.fa.start()
            self.fb.start()
            self.compute(1)
            self.r1b.start()
            self.compute(3)
            self.l1a.start()
            self.compute(0)

        def middle(self):
            hn, buf, far, rows = self.n // 2, self.buf, self.far_, self.rows
            self.fa.wait_recv()
            buf[rows(1, 0), :] += far[ds(0, hn), :]
            self.r1a.start()
            self.fb.wait_recv()
            buf[rows(3, 1), :] += far[ds(hn, hn), :]
            self.l1b.start()

        def finish(self):
            for c in (self.r1b, self.l1a, self.r1a, self.l1b):
                c.wait_recv()

        def total(self, start, size):
            n = self.n
            return self.buf[ds(start, size, 8), :] + (self.near_[ds(start, size, 8), :] + self.near_[ds(n + start, size, 8), :])

    cp_g.wait()
    x1.own()
    d_g0.wait_recv()
    panel_source(0)
    cp_gk.wait()
    d_gk.wait_recv()
    chunked(cr, 4, lambda r, i: gr.__setitem__((r, slice(None)), grf[r, :].astype(BF16)))
    y1.own()
    cp_ql.wait()
    d_ql.wait_recv()
    qlr[ds(0, cr), :] = qlf[...].astype(BF16)
    for c in d_own:
        c.start()
    cp_qr.wait()
    chunked(hc, 8, lambda r, i: qr.__setitem__((r, slice(None)), rac[r, :].astype(BF16)))
    cp_r = local(r_in, rac)
    x1.fwd()
    x2.own()
    panel_first(0)
    y1.fwd()
    x1.near()
    d_g[1].start()
    d_g[3].start()
    d_g[1].wait_recv()
    panel_source(1)
    d_g[3].wait_recv()
    panel_source(3)
    y1.near()
    y1.far()
    h_part(0, ocol)
    h_part(0, kcol)
    x1.far()
    d_g[2].start()
    d_g[2].wait_recv()
    panel_source(2)
    y2.own()
    split_right(0)
    panel_first(1)
    panel_second(0)
    panel_first(3)
    panel_second(1)
    panel_third(0)
    x2.fwd()
    panel_first(2)
    panel_second(3)
    panel_third(1)
    y2.fwd()
    cp_r.wait()
    split_left(0)
    product(0, 0)
    product(0, 1)
    l_slot(0)
    l_slot(1)
    x2.near()
    for s in (1, 3):
        h_part(s, ocol)
        h_part(s, kcol)
    y2.near()
    y2.far()
    qlc[ds(0, cr), :] = qlr[ds(d * cr, cr), :]
    a2a = []
    for s in (1, 3, 2):
        t = (y - x - s + 8) % 4
        a2a.append(remote(qlr.at[ds(t * cr + k * rc, rc, rc)], qlc.at[whole(s)], dx=s))
        a2a[-1].start()
    d_c = [remote(qlc.at[whole(s)], qlc.at[whole(s)], dk=1) for s in (1, 3, 2)]
    panel_second(2)
    panel_third(3)
    split_right(1)
    x2.far()
    d_h = remote(hp.at[:, ocol], hx, dk=1)
    h_part(2, ocol)
    d_h.start()
    h_part(2, kcol)
    d_h.wait_recv()
    chunked(cr, 4, lambda r, i: h.__setitem__((r, slice(None)), (hp[r, kcol] + hx[r, :]).astype(BF16)))
    x3.own()
    panel_third(2)
    split_left(1)
    product(1, 0)
    x3.fwd()
    product(1, 1)
    out_r = local(rac, r_out)
    for c, e in zip(a2a, d_c):
        c.wait_recv()
        e.start()
    for c in cp_own:
        c.wait()
    for c in d_own:
        c.wait_recv()
    for c in d_c:
        c.wait_recv()
    x3.near()
    x3.far()

    hx[...] = dot(qlc[...], h[...], ((0,), (0,)))

    def moments(r, i):
        rotated = hx[r, :]
        new_first = BETA1 * mx[r, :] + (1.0 - BETA1) * rotated
        new_second = BETA2 * vx[r, :] + (1.0 - BETA2) * rotated * rotated
        mx[r, :] = new_first
        vx[r, :] = new_second
        direction = (new_first / BIAS_ONE) / (jnp.sqrt(new_second / BIAS_TWO) + EPS)
        nb[r, :] = direction.astype(BF16)

    chunked(cr, 10 if cr % 160 == 0 else 1, moments)
    x4.own()
    outs = []
    for buf, out in ((mx, m_out), (vx, v_out)):
        outs.append(remote(buf.at[orow], out.at[:, kcol], dk=1))
        outs[-1].start()
    out_own = [local(buf.at[krow], out.at[:, kcol]) for buf, out in ((mx, m_out), (vx, v_out))]
    l_slot(2)
    l_slot(3)
    l_sum = Sum(lc, lf, ln, rc, lambda e: None)
    l_sum.begin()
    x4.fwd()
    l_sum.middle()
    x4.near()
    x4.far()

    kval = sum(dot(qlr[ds(((d + s) % 4) * cr, cr), :], nb[ds(s * cr, cr), :]) for s in range(4))
    kb[ds(k * cr, cr), :] = kval.astype(BF16)
    d_k = remote(kb.at[ds(k * cr, cr)], kb.at[ds(k * cr, cr)], dk=1)
    d_k.start()
    d_k.wait_recv()

    def u_chunk(e):
        s = (x - y - e + 8) % 4
        rows = ds(s * hc, hc)
        uc[ds(e * cr, cr), :] = (dot(kb[ds(0, cr), :], qr[rows, ds(0, hc)], ((1,), (1,)))
                                 + dot(kb[ds(cr, cr), :], qr[rows, ds(hc, hc)], ((1,), (1,))))

    u_sum = Sum(uc, uf, un, cr, u_chunk)
    u_sum.begin()
    l_sum.finish()
    cp_l.wait()
    lst[...] = BETA2 * lst[...] + (1.0 - BETA2) * l_sum.total(0, rc)
    out_l = local(lst, l_out)
    u_sum.middle()
    u_sum.finish()

    def final(r, i):
        wx[r, :] = wx[r, :] - LR * u_sum.total(i * (cr // 4), cr // 4)

    chunked(cr, 4, final)
    outs.append(remote(wx.at[orow], w_out.at[:, kcol], dk=1))
    outs[-1].start()
    out_own.append(local(wx.at[krow], w_out.at[:, kcol]))
    for c in outs:
        c.wait_recv()
    for c in out_own + [out_l, out_r]:
        c.wait()
    for c in pending:
        c.wait_send()
    for s in (0, 1, 3, 2):
        @pl.when(d != 3)
        def _():
            p_fwd[s].wait_send()

        @pl.when(d != 1)
        def _():
            q_fwd[s].wait_send()


def copy_kernel(*refs):
    n = (len(refs) - 2) // 3
    ins, outs, bufs, (si, so) = refs[:n], refs[n:2 * n], refs[2 * n:3 * n], refs[3 * n:]
    parts, reads, writes = [], [], []
    for a, b, o in zip(ins, bufs, outs):
        rows = a.shape[0]
        step = rows // 4 if rows % 32 == 0 and rows >= 512 else rows
        for r in range(0, rows, step):
            at = pl.ds(r, step)
            i = len(reads)
            reads.append(pltpu.make_async_copy(a.at[at], b.at[at], si.at[i]))
            writes.append(pltpu.make_async_copy(b.at[at], o.at[at], so.at[i]))
    for c in reads:
        c.start()
    for c, e in zip(reads, writes):
        c.wait()
        e.start()
    for e in writes:
        e.wait()


def solution(mesh):
    tile_spec = P(("layer", "row"), "col")

    def step(weight, grad_in, mom_first, mom_second, stat_left, stat_right, basis_left, basis_right):
        rc, cc = grad_in.shape
        cr, hc, q = 2 * rc, cc // 2, basis_left.shape[1]
        scratch = [
            ((4 * cr, cc), F32), ((4 * cr, hc), F32), ((hc, cc), F32), ((4 * hc, cc), BF16),
            ((cr, hc), F32), ((4 * cr, hc), BF16),
            ((cr, q), F32), ((4 * cr, q), BF16), ((4 * cr, q), BF16),
            ((cr, hc), F32), ((cr, hc), F32), ((cr, hc), F32),
            ((4 * cr, hc), BF16), ((4 * cr, hc), BF16), ((cr, cc), F32), ((cr, hc), F32),
            ((2 * cr, hc), BF16), ((4 * cr, hc), F32), ((cr, hc), F32), ((2 * cr, hc), F32),
            ((rc, q), F32), ((4 * rc, q), F32), ((rc, q), F32), ((2 * rc, q), F32),
            ((3 * hc, 2 * cr), BF16), ((6 * cr, cc), BF16), ((3 * rc, cc), BF16),
        ]
        args = (weight, grad_in, mom_first, mom_second, stat_left, stat_right, basis_left, basis_right)
        any_spec = pl.BlockSpec(memory_space=pl.ANY)
        sums = pl.pallas_call(
            kernel,
            out_shape=tuple(jax.ShapeDtypeStruct(a.shape, F32)
                            for a in (weight, mom_first, mom_second, stat_left, stat_right)),
            in_specs=[any_spec] * 8,
            out_specs=(any_spec,) * 5,
            scratch_shapes=[pltpu.VMEM(s, t) for s, t in scratch]
            + [pltpu.SemaphoreType.DMA((N_REMOTE,)), pltpu.SemaphoreType.DMA((N_REMOTE,)), pltpu.SemaphoreType.DMA((N_LOCAL,))],
            compiler_params=pltpu.CompilerParams(collective_id=0, has_side_effects=True, vmem_limit_bytes=67_000_000),
        )(*args)
        return pl.pallas_call(
            copy_kernel,
            out_shape=tuple(jax.ShapeDtypeStruct(a.shape, F32) for a in sums),
            in_specs=[any_spec] * 5,
            out_specs=(any_spec,) * 5,
            scratch_shapes=[pltpu.VMEM(a.shape, F32) for a in sums] + [pltpu.SemaphoreType.DMA((20,))] * 2,
        )(*sums)

    return jax.shard_map(step, mesh=mesh, in_specs=(tile_spec,) * 8, out_specs=(tile_spec,) * 5, check_vma=False)
```

```python
import jax
import jax.numpy as jnp
from jax import lax
from jax.experimental import pallas as pl
from jax.experimental.pallas import tpu as pltpu
from jax.sharding import PartitionSpec as P

BETA1 = 0.9
BETA2 = 0.9
EPS = 1e-8
LR = 0.1
STEP = 10
BIAS_ONE = 1.0 - BETA1 ** STEP
BIAS_TWO = 1.0 - BETA2 ** STEP
MESH = pl.DeviceIdType.MESH
N_REMOTE = 144
N_LOCAL = 16
VMEM_BYTES = 50_000_000
F32 = jnp.float32
BF16 = jnp.bfloat16
SIX_PASSES = ((0, 0), (0, 1), (1, 0), (0, 2), (1, 1), (2, 0))


def dot(a, b, dims=((1,), (0,))):
    return lax.dot_general(a, b, (dims, ((), ())), preferred_element_type=F32)


def split_three(a):
    hi = a.astype(BF16)
    rest = a - hi.astype(F32)
    mid = rest.astype(BF16)
    return hi, mid, (rest - mid.astype(F32)).astype(BF16)


def kernel(w_in, g_in, m_in, v_in, l_in, r_in, ql_in, qr_in, w_out, m_out, v_out, l_out, r_out,
           gf, px, qr, grf, gr, qlf, qlr, qlc, qlt, wx, mx, vx, h, nb, hp, hx, kb, uf, un, uo,
           lc, lf, ln, lhs3, rhs3, la, ss, rs, ls):
    rc, cc = g_in.shape
    cr, hc = 2 * rc, cc // 2
    kk = 2 * cr
    nt = 256 if cc % 256 == 0 else cc
    tb = 128 if kk % 128 == 0 else kk
    row, y = lax.axis_index("row"), lax.axis_index("col")
    x, k = row // 2, row % 2
    d = (y - x + 4) % 4
    rq = cr // 4
    uc, rot = px, grf
    pa = 128 * (hc * 2 // 5 // 128) if hc % 128 == 0 else hc // 2
    pieces = ((0, pa), (pa, hc - pa))

    def ds(start, size, unit=None):
        return pl.ds(start if isinstance(start, int) else pl.multiple_of(start, unit or size), size)

    kcol, ocol = ds(k * hc, hc), ds((1 - k) * hc, hc)
    krow, orow = ds(k * rc, rc), ds((1 - k) * rc, rc)

    counter, pending = [0], []

    def remote(src, dst, dx=0, dk=0, dy=0, index=None, track=True, receive=None):
        if index is None:
            index = counter[0]
            counter[0] += 1
        assert index < N_REMOTE
        copy = pltpu.make_async_remote_copy(
            src_ref=src, dst_ref=dst, send_sem=ss.at[index], recv_sem=rs.at[index if receive is None else receive],
            device_id={"row": ((x + dx + 4) % 4) * 2 + (k + dk) % 2, "col": (y + dy + 4) % 4}, device_id_type=MESH)
        if track:
            pending.append(copy)
        return copy

    lcounter = [0]

    def local(src, dst):
        index = lcounter[0]
        lcounter[0] += 1
        assert index < N_LOCAL
        copy = pltpu.make_async_copy(src, dst, ls.at[index])
        copy.start()
        return copy

    class Ring:
        def __init__(self, buf, at, axis, forward=None, absolute=False):
            def cp(s0, half, s1, step, at=at):
                return remote(buf.at[at(s0, half)], buf.at[at(s0 if absolute else s1, half)], **{axis: step})
            self.ra, self.lb = cp(0, 0, 1, 1), cp(0, 1, 3, -1)
            self.rb, self.la = cp(0, 1, 1, 1), cp(0, 0, 3, -1)
            self.fr, self.fl = [], []
            for part in (forward or [at]):
                self.fr.append(cp(1, 0, 2, 1, part))
                self.fl.append(cp(3, 1, 2, -1, part))

        def own(self):
            for c in (self.ra, self.lb, self.rb, self.la):
                c.start()

        def fwd(self):
            self.ra.wait_recv()
            for c in self.fr:
                c.start()
            self.lb.wait_recv()
            for c in self.fl:
                c.start()

        def near(self):
            self.rb.wait_recv()
            self.la.wait_recv()

        def far(self, parts=None):
            for i in range(len(self.fr)) if parts is None else parts:
                self.fr[i].wait_recv()
                self.fl[i].wait_recv()

    def chunked(total, parts, body):
        size = total // parts

        @pl.loop(0, parts)
        def _(i):
            body(ds(i * size, size), i)

    cp_g = local(g_in, gf.at[krow])
    cp_gk = local(g_in.at[:, kcol], grf.at[krow])
    cp_ql = local(ql_in, qlf.at[krow])
    cp_qr = local(qr_in, r_out)
    cp_own = [local(a.at[:, kcol], b.at[krow]) for a, b in ((m_in, mx), (v_in, vx))] + [local(w_in, wx)]
    cp_l = local(l_in, l_out)
    barrier = pltpu.get_barrier_semaphore()
    for dx, dk, dy in ((1, 0, 0), (-1, 0, 0), (2, 0, 0), (0, 1, 0), (0, 0, 1), (0, 0, -1), (0, 1, 1), (0, 1, -1)):
        pl.semaphore_signal(barrier, inc=1, device_id={"row": ((x + dx + 4) % 4) * 2 + (k + dk) % 2, "col": (y + dy + 4) % 4},
                            device_id_type=MESH)
    pl.semaphore_wait(barrier, 8)

    d_gk = remote(g_in.at[:, ocol], grf.at[krow], dk=1)
    d_g0 = remote(g_in, gf.at[krow], dk=1)
    d_ql = remote(ql_in, qlf.at[krow], dk=1)
    d_own = [remote(a.at[:, ocol], b.at[krow], dk=1) for a, b in ((m_in, mx), (v_in, vx))]
    d_g0.start()
    d_gk.start()
    d_ql.start()

    def grow(s, half):
        return ds((s * 2 + k) * rc + half * (rc // 2), rc // 2)

    def slot_rows(n, start=0, size=None, cols=None):
        size = n if size is None else size
        return lambda s, half: (ds(s * n + start + half * (size // 2), size // 2, 8), slice(None) if cols is None else ds(*cols))

    def whole(s):
        return ds((s * 2 + k) * rc, rc)

    x1 = Ring(gf, grow, "dx")
    x2 = Ring(qr, slot_rows(hc), "dx", [slot_rows(hc, cols=(c * hc + at, n)) for at, n in pieces for c in range(2)])
    x3 = [Ring(h, slot_rows(cr, cols=piece), "dx") for piece in pieces]
    x4 = [Ring(nb, slot_rows(cr, cols=piece), "dx") for piece in pieces]
    y1 = Ring(gr, slot_rows(cr), "dy")
    y2 = Ring(qlr, slot_rows(cr, start=k * rc, size=rc), "dy")
    y3 = Ring(qlc, lambda s, half: (pl.ds(1 + 2 * half, 2 - half), (y - s + 4) % 4), "dy", absolute=True)
    d_g = {s: remote(gf.at[whole(s)], gf.at[whole(s)], dk=1) for s in (1, 3, 2)}

    def prow(s, c):
        return ds((s * 2 + c) * rc, rc)

    p_src, p_fwd, q_src, q_fwd = {}, {}, {}, {}
    for s in (0, 1, 3, 2):
        pi, qi = counter[0], counter[0] + 1
        counter[0] += 2
        p_src[s] = remote(gf.at[prow(s, 0), kcol], px.at[prow(s, 0)], dy=1, index=pi, track=False)
        p_fwd[s] = remote(px.at[prow(s, 0)], px.at[prow(s, 0)], dy=1, index=pi, track=False)
        q_src[s] = remote(gf.at[prow(s, 1), kcol], px.at[prow(s, 1)], dy=-1, index=qi, track=False)
        q_fwd[s] = remote(px.at[prow(s, 1)], px.at[prow(s, 1)], dy=-1, index=qi, track=False)

    def panel_source(s):
        @pl.when(d == 0)
        def _():
            p_src[s].start()
            q_src[s].start()

    def panel_first(s):
        @pl.when(d == 1)
        def _():
            p_fwd[s].wait_recv()
            p_fwd[s].start()

        @pl.when(d == 3)
        def _():
            q_fwd[s].wait_recv()
            q_fwd[s].start()

    def panel_second(s):
        @pl.when(d == 2)
        def _():
            p_fwd[s].wait_recv()
            p_fwd[s].start()
            q_fwd[s].wait_recv()
            q_fwd[s].start()

    def panel_third(s):
        @pl.when(d == 3)
        def _():
            p_fwd[s].wait_recv()

        @pl.when(d == 1)
        def _():
            q_fwd[s].wait_recv()

    def h_part(s, cols):
        t = (d + s) % 4
        part = dot(gr[ds(t * cr, cr), :], qr[ds(s * hc, hc), cols])
        if s == 0:
            hp[:, cols] = part
        else:
            hp[:, cols] += part

    def split_right(p):
        base = p * kk

        def body(r, i):
            for q, piece in enumerate(split_three(gf[ds(base + i * (kk // 8), kk // 8, 8), :])):
                rhs3[ds(q * kk + i * (kk // 8), kk // 8, 8), :] = piece

        chunked(kk, 8, body)
        if p == 0:
            for q in range(3):
                la[ds(q * rc, rc), :] = rhs3[ds(q * kk + k * rc, rc, rc), :]

    def split_left(p):
        base = p * kk

        @pl.when(d == 0)
        def _():
            chunked(kk, 4, lambda r, i: px.__setitem__(
                (ds(base + i * (kk // 4), kk // 4, 8), slice(None)), gf[ds(base + i * (kk // 4), kk // 4, 8), kcol]))

        def body(cols, i):
            for q, piece in enumerate(split_three(px[ds(base + i * tb, tb, 8), :].T)):
                lhs3[ds(q * hc, hc), cols] = piece

        chunked(kk, kk // tb, body)

    def product(p, m):
        def body(cols, i):
            acc = sum(dot(lhs3[ds(a * hc + m * (hc // 2), hc // 2), :], rhs3[ds(b * kk, kk), cols]) for a, b in SIX_PASSES)
            at = (ds(m * (hc // 2), hc // 2), cols)
            if p == 0:
                r_out[at] = BETA2 * r_out[at] + (1.0 - BETA2) * acc
            else:
                r_out[at] += (1.0 - BETA2) * acc

        chunked(cc, cc // nt, body)

    def l_slot(s):
        e = (x - y - s + 8) % 4
        at = [ds(q * kk + (s % 2) * cr, cr) for q in range(3)]
        high = dot(la[...], rhs3[at[0], :], ((1,), (1,)))
        middle = dot(la[ds(0, 2 * rc), :], rhs3[at[1], :], ((1,), (1,)))
        low = dot(la[ds(0, rc), :], rhs3[at[2], :], ((1,), (1,)))
        lc[ds(e * rc, rc), :] = high[:rc] + (high[rc:2 * rc] + middle[:rc]) + (high[2 * rc:] + middle[rc:] + low)

    class Sum:
        def __init__(self, buf, far, near, n, compute):
            self.buf, self.far_, self.near_, self.n, self.compute = buf, far, near, n, compute
            hn = n // 2
            self.rows = lambda e, half: ds(e * n + half * hn, hn)
            rows = self.rows
            self.fa = remote(buf.at[rows(2, 0)], far.at[ds(0, hn)], dy=1)
            self.fb = remote(buf.at[rows(2, 1)], far.at[ds(hn, hn)], dy=-1)
            self.r1b = remote(buf.at[rows(1, 1)], near.at[ds(hn, hn)], dy=1)
            self.l1a = remote(buf.at[rows(3, 0)], near.at[ds(n, hn)], dy=-1)
            self.r1a = remote(buf.at[rows(1, 0)], near.at[ds(0, hn)], dy=1)
            self.l1b = remote(buf.at[rows(3, 1)], near.at[ds(n + hn, hn)], dy=-1)

        def begin(self):
            self.compute(2)
            self.fa.start()
            self.fb.start()
            self.compute(1)
            self.r1b.start()
            self.compute(3)
            self.l1a.start()
            self.compute(0)

        def middle(self):
            hn, buf, far, rows = self.n // 2, self.buf, self.far_, self.rows
            self.fa.wait_recv()
            buf[rows(1, 0), :] += far[ds(0, hn), :]
            self.r1a.start()
            self.fb.wait_recv()
            buf[rows(3, 1), :] += far[ds(hn, hn), :]
            self.l1b.start()

        def finish(self):
            for c in (self.r1b, self.l1a, self.r1a, self.l1b):
                c.wait_recv()

        def total(self, start, size):
            n = self.n
            return self.buf[ds(start, size, 8), :] + (self.near_[ds(start, size, 8), :] + self.near_[ds(n + start, size, 8), :])

    class RowSum(Sum):
        def __init__(self, buf, far, near, n, compute):
            self.buf, self.far_, self.near_, self.n, self.compute = buf, far, near, n, compute
            hn = n // 2
            self.rows = lambda e, half: ds(e * n + half * hn, hn)
            rows = self.rows
            self.fa = remote(buf.at[rows(2, 0)], far.at[ds(0, hn)], dy=1)
            self.fb = remote(buf.at[rows(2, 1)], far.at[ds(hn, hn)], dy=-1)
            base = counter[0]
            counter[0] += 4

            def send(e, half, side):
                return remote(buf.at[rows(e, half)], near.at[ds(side * hn, hn), kcol], dk=half - k + 2, dy=(1, -1)[side],
                              receive=base + side * 2 + k)
            self.r1b, self.r1a = send(1, 1, 0), send(1, 0, 0)
            self.l1a, self.l1b = send(3, 0, 1), send(3, 1, 1)
            self.arrivals = [remote(buf.at[rows(0, 0)], near.at[ds(side * hn, hn), ds(core * hc, hc)], dk=1, index=base + side * 2 + core,
                                    track=False) for side in range(2) for core in range(2)]

        def finish(self):
            for c in self.arrivals:
                c.wait_recv()

    cp_g.wait()
    x1.own()
    d_g0.wait_recv()
    panel_source(0)
    cp_gk.wait()
    d_gk.wait_recv()
    chunked(cr, 4, lambda r, i: gr.__setitem__((r, slice(None)), grf[r, :].astype(BF16)))
    y1.own()
    cp_ql.wait()
    d_ql.wait_recv()
    qlr[ds(0, cr), :] = qlf[...].astype(BF16)
    y2.own()
    for c in d_own:
        c.start()
    cp_qr.wait()
    chunked(hc, 8, lambda r, i: qr.__setitem__((r, slice(None)), r_out[r, :].astype(BF16)))
    cp_r = local(r_in, r_out)
    x1.fwd()
    x2.own()
    panel_first(0)
    y1.fwd()
    y2.fwd()
    x1.near()
    d_g[1].start()
    d_g[3].start()
    d_g[1].wait_recv()
    panel_source(1)
    d_g[3].wait_recv()
    panel_source(3)
    y1.near()
    y1.far()
    h_part(0, ocol)
    h_part(0, kcol)
    x1.far()
    d_g[2].start()
    d_g[2].wait_recv()
    panel_source(2)
    y2.near()
    y2.far()
    d_q = [remote(qlr.at[ds(s * cr + k * rc, rc)], qlr.at[ds(s * cr + k * rc, rc)], dk=1) for s in (1, 3, 2)]
    for c in d_q:
        c.start()
    for c in d_q:
        c.wait_recv()
    qlc[0] = qlr[ds(d * cr, cr), :].reshape(4, rq, qlr.shape[1])
    a2a = []
    for s in (1, 3, 2):
        t = (y - x - s + 8) % 4
        a2a.append(remote(qlr.at[ds(t * cr + y * rq, rq, rq)], qlc.at[s, y], dx=s))
        a2a[-1].start()
    split_right(0)
    panel_first(1)
    panel_second(0)
    panel_first(3)
    panel_second(1)
    panel_third(0)
    x2.fwd()
    panel_first(2)
    panel_second(3)
    panel_third(1)
    cp_r.wait()
    split_left(0)
    product(0, 0)
    product(0, 1)
    x2.near()
    for s in (1, 3):
        h_part(s, ocol)
        h_part(s, kcol)
    for c in a2a:
        c.wait_recv()
    y3.own()

    def columns(core, piece):
        at, n = pieces[piece]
        return ds(core * hc + at, n, 128)

    d_h = [remote(hp.at[:, columns(1 - k, p)], hx.at[:, ds(*pieces[p])], dk=1) for p in range(2)]

    def h_send(p):
        x2.far((2 * p, 2 * p + 1))
        h_part(2, columns(1 - k, p))
        d_h[p].start()
        h_part(2, columns(k, p))

    def h_finish(p):
        d_h[p].wait_recv()
        h[ds(0, cr), ds(*pieces[p])] = (hp[:, columns(k, p)] + hx[:, ds(*pieces[p])]).astype(BF16)
        x3[p].own()

    h_send(0)
    h_finish(0)
    y3.fwd()
    l_slot(0)
    l_slot(1)
    panel_second(2)
    panel_third(3)
    split_right(1)
    h_send(1)
    x3[0].fwd()
    h_finish(1)
    panel_third(2)
    split_left(1)
    product(1, 0)
    y3.near()
    y3.far()
    qlt[...] = qlc[...].reshape(4 * cr, qlc.shape[3]).T
    for c in cp_own:
        c.wait()
    for c in d_own:
        c.wait_recv()
    x3[1].fwd()

    def moments(p):
        x3[p].near()
        x3[p].far()
        cols = ds(*pieces[p])
        rot[:, cols] = dot(qlt[...], h[:, cols])

        def body(r, i):
            rotated = rot[r, cols]
            new_first = BETA1 * mx[r, cols] + (1.0 - BETA1) * rotated
            new_second = BETA2 * vx[r, cols] + (1.0 - BETA2) * rotated * rotated
            mx[r, cols] = new_first
            vx[r, cols] = new_second
            direction = (new_first / BIAS_ONE) / (jnp.sqrt(new_second / BIAS_TWO) + EPS)
            nb[r, cols] = direction.astype(BF16)

        chunked(cr, 10 if cr % 160 == 0 else 1, body)

    moments(0)
    x4[0].own()
    product(1, 1)
    moments(1)
    x4[0].fwd()
    x4[1].own()
    outs = []
    for buf, out in ((mx, m_out), (vx, v_out)):
        outs.append(remote(buf.at[orow], out.at[:, kcol], dk=1))
        outs[-1].start()
        out[:, kcol] = buf[krow, :]
    l_slot(2)
    l_slot(3)
    l_sum = Sum(lc, lf, ln, rc, lambda e: None)
    l_sum.begin()

    d_k = [remote(kb.at[ds(k * cr, cr), ds(*piece)], kb.at[ds(k * cr, cr), ds(*piece)], dk=1) for piece in pieces]

    def k_part(p, slots):
        cols = ds(*pieces[p])
        return sum(dot(qlr[ds(((d + s) % 4) * cr, cr), :], nb[ds(s * cr, cr), cols]) for s in slots)

    def u_part(e, p):
        s = (x - y - e + 8) % 4
        at, n = pieces[p]
        part = sum(dot(kb[ds(c * cr, cr), ds(at, n)], qr[ds(s * hc, hc), ds(c * hc + at, n)], ((1,), (1,))) for c in range(2))
        if p == 0:
            uc[ds(e * cr, cr), :] = part
        else:
            uc[ds(e * cr, cr), :] += part

    x4[0].near()
    x4[0].far()
    kb[ds(k * cr, cr), ds(*pieces[0])] = k_part(0, range(4)).astype(BF16)
    d_k[0].start()
    x4[1].fwd()
    for s in (0, 1, 3, 2):
        @pl.when(d != 3)
        def _():
            p_fwd[s].wait_send()

        @pl.when(d != 1)
        def _():
            q_fwd[s].wait_send()
    d_k[0].wait_recv()
    for e in (2, 1, 3, 0):
        u_part(e, 0)
    x4[1].near()
    rot[:, ds(*pieces[1])] = k_part(1, (0, 1, 3))
    l_sum.middle()
    x4[1].far()
    kb[ds(k * cr, cr), ds(*pieces[1])] = (rot[:, ds(*pieces[1])] + k_part(1, (2,))).astype(BF16)
    d_k[1].start()
    d_k[1].wait_recv()
    u_sum = RowSum(uc, uf, un, cr, lambda e: u_part(e, 1))
    u_sum.begin()
    d_u = remote(uc.at[orow], uo, dk=1)
    d_u.start()
    l_sum.finish()
    cp_l.wait()
    l_out[...] = BETA2 * l_out[...] + (1.0 - BETA2) * l_sum.total(0, rc)
    for c in outs:
        c.wait_recv()
    u_sum.middle()
    d_u.wait_recv()
    u_sum.finish()
    for mine, cols in ((True, kcol), (False, ocol)):
        total = (uc[krow, :] if mine else uo[...]) + (un[ds(0, rc), cols] + un[ds(rc, rc), cols])
        w_out[:, cols] = wx[:, cols] - LR * total
    for c in pending:
        c.wait_send()


def write_kernel(*refs):
    n = (len(refs) - 1) // 2
    copies = [pltpu.make_async_copy(a, b, refs[-1].at[i]) for i, (a, b) in enumerate(zip(refs[:n], refs[n:2 * n]))]
    for c in copies:
        c.start()
    for c in copies:
        c.wait()


def solution(mesh):
    tile_spec = P(("layer", "row"), "col")

    def step(weight, grad_in, mom_first, mom_second, stat_left, stat_right, basis_left, basis_right):
        rc, cc = grad_in.shape
        cr, hc, q = 2 * rc, cc // 2, basis_left.shape[1]
        scratch = [
            ((4 * cr, cc), F32), ((4 * cr, hc), F32), ((4 * hc, cc), BF16),
            ((cr, hc), F32), ((4 * cr, hc), BF16),
            ((cr, q), F32), ((4 * cr, q), BF16), ((4, 4, cr // 4, q), BF16), ((q, 4 * cr), BF16),
            ((rc, cc), F32), ((cr, hc), F32), ((cr, hc), F32),
            ((4 * cr, hc), BF16), ((4 * cr, hc), BF16), ((cr, cc), F32),
            ((cr, hc), F32),
            ((2 * cr, hc), BF16), ((cr, hc), F32), ((cr, cc), F32), ((rc, hc), F32),
            ((4 * rc, q), F32), ((rc, q), F32), ((2 * rc, q), F32),
            ((3 * hc, 2 * cr), BF16), ((6 * cr, cc), BF16), ((3 * rc, cc), BF16),
        ]
        args = (weight, grad_in, mom_first, mom_second, stat_left, stat_right, basis_left, basis_right)
        vmem_spec, any_spec = pl.BlockSpec(memory_space=pltpu.VMEM), pl.BlockSpec(memory_space=pl.ANY)
        outs = tuple(jax.ShapeDtypeStruct(a.shape, F32) for a in (weight, mom_first, mom_second, stat_left, stat_right))
        results = pl.pallas_call(
            kernel,
            out_shape=outs,
            in_specs=[pl.BlockSpec(memory_space=pltpu.HBM)] * 8,
            out_specs=(vmem_spec,) * 5,
            scratch_shapes=[pltpu.VMEM(s, t) for s, t in scratch]
            + [pltpu.SemaphoreType.DMA((N_REMOTE,)), pltpu.SemaphoreType.DMA((N_REMOTE,)), pltpu.SemaphoreType.DMA((N_LOCAL,))],
            compiler_params=pltpu.CompilerParams(collective_id=0, has_side_effects=True, vmem_limit_bytes=VMEM_BYTES),
        )(*(pltpu.with_memory_space_constraint(a, pltpu.HBM) for a in args))
        return pl.pallas_call(
            write_kernel,
            out_shape=outs,
            in_specs=[any_spec] * 5,
            out_specs=(any_spec,) * 5,
            scratch_shapes=[pltpu.SemaphoreType.DMA((5,))],
            compiler_params=pltpu.CompilerParams(vmem_limit_bytes=1_000_000),
        )(*(pltpu.with_memory_space_constraint(a, pltpu.VMEM) for a in results))

    return jax.shard_map(step, mesh=mesh, in_specs=(tile_spec,) * 8, out_specs=(tile_spec,) * 5, check_vma=False)
```

```python
import functools

import jax
import jax.numpy as jnp
from jax import lax
from jax.experimental import pallas as pl
from jax.experimental.pallas import tpu as pltpu
from jax.sharding import PartitionSpec as P

BETA1 = 0.9
BETA2 = 0.9
EPS = 1e-8
LR = 0.1
STEP = 10
BIAS_ONE = 1.0 - BETA1 ** STEP
BIAS_TWO = 1.0 - BETA2 ** STEP
MESH = pl.DeviceIdType.MESH
N_SEND, N_RECEIVE, N_LOCAL = 33, 71, 9
VMEM_BYTES = 50_000_000
F32 = jnp.float32
BF16 = jnp.bfloat16
SIX_PASSES = ((0, 0), (0, 1), (1, 0), (0, 2), (1, 1), (2, 0))


def dot(a, b, dims=((1,), (0,))):
    return lax.dot_general(a, b, (dims, ((), ())), preferred_element_type=F32)


def split_three(a):
    hi = a.astype(BF16)
    rest = a - hi.astype(F32)
    mid = rest.astype(BF16)
    return hi, mid, (rest - mid.astype(F32)).astype(BF16)


def kernel(w_in, g_in, m_in, v_in, l_in, r_in, ql_in, qr_in, w_out, m_out, v_out, l_out, r_out,
           gf, px, qr, grf, gr, qlf, qlr, qlc, qlt, wx, mx, vx, h, nb, hp, hx, kb, uf, un, uo,
           lc, lf, ln, lhs3, rhs3, la, ss, rs, ls):
    rc, cc = g_in.shape
    cr, hc = 2 * rc, cc // 2
    kk = 2 * cr
    nt = 256 if cc % 256 == 0 else cc
    tb = 128 if kk % 128 == 0 else kk
    row, y = lax.axis_index("row"), lax.axis_index("col")
    x, k = row // 2, row % 2
    d = (y - x + 4) % 4
    rq = cr // 4
    uc, rot = px, grf
    pa = 128 * (hc * 2 // 5 // 128) if hc % 128 == 0 else hc // 2
    pieces = ((0, pa), (pa, hc - pa))

    def ds(start, size, unit=None):
        return pl.ds(start if isinstance(start, int) else pl.multiple_of(start, unit or size), size)

    kcol, ocol = ds(k * hc, hc), ds((1 - k) * hc, hc)
    krow, orow = ds(k * rc, rc), ds((1 - k) * rc, rc)

    sends, receives, pending = [0], [0], []

    def new(counter, limit):
        counter[0] += 1
        assert counter[0] <= limit
        return counter[0] - 1

    def remote(src, dst, dx=0, dk=0, dy=0, send=None, receive=None):
        own = send is None
        copy = pltpu.make_async_remote_copy(
            src_ref=src, dst_ref=dst, send_sem=ss.at[new(sends, N_SEND) if own else send],
            recv_sem=rs.at[new(receives, N_RECEIVE) if receive is None else receive],
            device_id={"row": ((x + dx + 4) % 4) * 2 + (k + dk) % 2, "col": (y + dy + 4) % 4}, device_id_type=MESH)
        if own:
            pending.append(copy)
        return copy

    def group(ref):
        send, receive = new(sends, N_SEND), new(receives, N_RECEIVE)
        return send, receive, remote(ref, ref, dk=1, send=send, receive=receive)

    lcounter = [0]

    def local(src, dst):
        index = lcounter[0]
        lcounter[0] += 1
        assert index < N_LOCAL
        copy = pltpu.make_async_copy(src, dst, ls.at[index])
        copy.start()
        return copy

    class Ring:
        def __init__(self, buf, at, axis, total, near, far, forward=None, absolute=False):
            send = new(sends, N_SEND)
            pending.append(remote(buf.at[total], buf.at[total], dk=1, send=send, receive=0))

            def cp(s0, half, s1, step, receive=None, at=at):
                return remote(buf.at[at(s0, half)], buf.at[at(s0 if absolute else s1, half)], send=send, receive=receive, **{axis: step})

            def wait(view):
                receive = new(receives, N_RECEIVE)
                return receive, remote(buf.at[view], buf.at[view], dk=1, send=send, receive=receive)
            self.ra, self.lb = cp(0, 0, 1, 1), cp(0, 1, 3, -1)
            receive, self.near_ = wait(near)
            self.rb, self.la = cp(0, 1, 1, 1, receive), cp(0, 0, 3, -1, receive)
            self.fr, self.fl, self.far_ = [], [], []
            for parts, view in forward or [([at], far)]:
                receive, wait_far = wait(view)
                self.far_.append(wait_far)
                for part in parts:
                    self.fr.append(cp(1, 0, 2, 1, receive, part))
                    self.fl.append(cp(3, 1, 2, -1, receive, part))

        def own(self):
            for c in (self.ra, self.lb, self.rb, self.la):
                c.start()

        def fwd(self):
            self.ra.wait_recv()
            for c in self.fr:
                c.start()
            self.lb.wait_recv()
            for c in self.fl:
                c.start()

        def near(self):
            self.near_.wait_recv()

        def far(self, parts=None):
            for i in range(len(self.far_)) if parts is None else parts:
                self.far_[i].wait_recv()

    def chunked(total, parts, body):
        size = total // parts

        @pl.loop(0, parts)
        def _(i):
            body(ds(i * size, size), i)

    cp_g = local(g_in, gf.at[krow])
    cp_gk = local(g_in.at[:, kcol], grf.at[krow])
    cp_ql = local(ql_in, qlf.at[krow])
    cp_qr = local(qr_in, r_out)
    cp_own = [local(a.at[:, kcol], b.at[krow]) for a, b in ((m_in, mx), (v_in, vx))] + [local(w_in, wx)]
    cp_l = local(l_in, l_out)
    barrier = pltpu.get_barrier_semaphore()
    for dx, dk, dy in ((1, 0, 0), (-1, 0, 0), (2, 0, 0), (0, 1, 0), (0, 0, 1), (0, 0, -1), (0, 1, 1), (0, 1, -1)):
        pl.semaphore_signal(barrier, inc=1, device_id={"row": ((x + dx + 4) % 4) * 2 + (k + dk) % 2, "col": (y + dy + 4) % 4},
                            device_id_type=MESH)
    pl.semaphore_wait(barrier, 8)

    d_gk = remote(g_in.at[:, ocol], grf.at[krow], dk=1)
    d_g0 = remote(g_in, gf.at[krow], dk=1)
    d_ql = remote(ql_in, qlf.at[krow], dk=1)
    own_send, own_receive, d_own_all = group(mx)
    pending.append(d_own_all)
    d_own = [remote(a.at[:, ocol], b.at[krow], dk=1, send=own_send, receive=own_receive) for a, b in ((m_in, mx), (v_in, vx))]
    d_g0.start()
    d_gk.start()
    d_ql.start()

    def grow(s, half):
        return ds((s * 2 + k) * rc + half * (rc // 2), rc // 2)

    def slot_rows(n, start=0, size=None, cols=None):
        size = n if size is None else size
        return lambda s, half: (ds(s * n + start + half * (size // 2), size // 2, 8), slice(None) if cols is None else ds(*cols))

    def whole(s):
        return ds((s * 2 + k) * rc, rc)

    def tiles(n, cols=None):
        cols = slice(None) if cols is None else ds(*cols)
        return {"total": (ds(0, 3 * n), cols), "near": (ds(0, n), cols), "far": (ds(0, n), cols)}

    x1 = Ring(gf, grow, "dx", **tiles(rc))
    x2 = Ring(qr, slot_rows(hc), "dx", **tiles(hc), forward=[
        ([slot_rows(hc, cols=(c * hc + at, n)) for c in range(2)], (ds(0, hc), ds(0, 2 * n))) for at, n in pieces])
    x3 = [Ring(h, slot_rows(cr, cols=piece), "dx", **tiles(cr, piece)) for piece in pieces]
    x4 = [Ring(nb, slot_rows(cr, cols=piece), "dx", **tiles(cr, piece)) for piece in pieces]
    y1 = Ring(gr, slot_rows(cr), "dy", **tiles(cr))
    y2 = Ring(qlr, slot_rows(cr, start=k * rc, size=rc), "dy", **tiles(rc))
    y3 = Ring(qlc, lambda s, half: (pl.ds(1 + 2 * half, 2 - half), (y - s + 4) % 4), "dy", absolute=True,
              total=(pl.ds(0, 3), pl.ds(0, 3)), near=(pl.ds(0, 3), 0), far=(pl.ds(0, 3), 0))
    d_g = {s: remote(gf.at[whole(s)], gf.at[whole(s)], dk=1) for s in (1, 3, 2)}

    def prow(s, c):
        return ds((s * 2 + c) * rc, rc)

    p_src, p_fwd, q_src, q_fwd = {}, {}, {}, {}
    p_send, q_send = new(sends, N_SEND), new(sends, N_SEND)
    p_all, q_all = (remote(px.at[ds(0, 4 * rc)], px.at[ds(0, 4 * rc)], dk=1, send=i, receive=0) for i in (p_send, q_send))
    for s in (0, 1, 3, 2):
        pi, qi = new(receives, N_RECEIVE), new(receives, N_RECEIVE)
        p_src[s] = remote(gf.at[prow(s, 0), kcol], px.at[prow(s, 0)], dy=1, send=p_send, receive=pi)
        p_fwd[s] = remote(px.at[prow(s, 0)], px.at[prow(s, 0)], dy=1, send=p_send, receive=pi)
        q_src[s] = remote(gf.at[prow(s, 1), kcol], px.at[prow(s, 1)], dy=-1, send=q_send, receive=qi)
        q_fwd[s] = remote(px.at[prow(s, 1)], px.at[prow(s, 1)], dy=-1, send=q_send, receive=qi)

    def panel_source(s):
        @pl.when(d == 0)
        def _():
            p_src[s].start()
            q_src[s].start()

    def panel_first(s):
        @pl.when(d == 1)
        def _():
            p_fwd[s].wait_recv()
            p_fwd[s].start()

        @pl.when(d == 3)
        def _():
            q_fwd[s].wait_recv()
            q_fwd[s].start()

    def panel_second(s):
        @pl.when(d == 2)
        def _():
            p_fwd[s].wait_recv()
            p_fwd[s].start()
            q_fwd[s].wait_recv()
            q_fwd[s].start()

    def panel_third(s):
        @pl.when(d == 3)
        def _():
            p_fwd[s].wait_recv()

        @pl.when(d == 1)
        def _():
            q_fwd[s].wait_recv()

    def h_part(s, cols):
        t = (d + s) % 4
        part = dot(gr[ds(t * cr, cr), :], qr[ds(s * hc, hc), cols])
        if s == 0:
            hp[:, cols] = part
        else:
            hp[:, cols] += part

    units = 2 * (cc // nt)

    def split_right(p):
        base = p * kk

        def body(r, i):
            for q, piece in enumerate(split_three(gf[ds(base + i * (kk // 8), kk // 8, 8), :])):
                rhs3[ds(q * kk + i * (kk // 8), kk // 8, 8), :] = piece

        chunked(kk, 8, body)
        if p == 0:
            for q in range(3):
                la[ds(q * rc, rc), :] = rhs3[ds(q * kk + k * rc, rc, rc), :]

    def split_left(p):
        base = p * kk

        @pl.when(d == 0)
        def _():
            chunked(kk, 4, lambda r, i: px.__setitem__(
                (ds(base + i * (kk // 4), kk // 4, 8), slice(None)), gf[ds(base + i * (kk // 4), kk // 4, 8), kcol]))

        def body(cols, i):
            for q, piece in enumerate(split_three(px[ds(base + i * tb, tb, 8), :].T)):
                lhs3[ds(q * hc, hc), cols] = piece

        chunked(kk, kk // tb, body)

    def product(p, first, last):
        @pl.loop(first, last)
        def _(i):
            m, j = i // (cc // nt), i % (cc // nt)
            rows = ds(m * (hc // 2), hc // 2)
            cols = ds(j * nt, nt)
            acc = sum(dot(lhs3[ds(a * hc + m * (hc // 2), hc // 2), :], rhs3[ds(b * kk, kk), cols]) for a, b in SIX_PASSES)
            if p == 0:
                r_out[rows, cols] = BETA2 * r_out[rows, cols] + (1.0 - BETA2) * acc
            else:
                r_out[rows, cols] += (1.0 - BETA2) * acc

    def l_slot(s):
        e = (x - y - s + 8) % 4
        at = [ds(q * kk + (s % 2) * cr, cr) for q in range(3)]
        high = dot(la[...], rhs3[at[0], :], ((1,), (1,)))
        middle = dot(la[ds(0, 2 * rc), :], rhs3[at[1], :], ((1,), (1,)))
        low = dot(la[ds(0, rc), :], rhs3[at[2], :], ((1,), (1,)))
        lc[ds(e * rc, rc), :] = high[:rc] + (high[rc:2 * rc] + middle[:rc]) + (high[2 * rc:] + middle[rc:] + low)

    class Sum:
        def __init__(self, buf, far, near, n):
            self.buf, self.far_, self.near_, self.n = buf, far, near, n
            hn = n // 2
            self.rows = lambda e, half: ds(e * n + half * hn, hn)
            send = new(sends, N_SEND)
            receive = new(receives, N_RECEIVE)
            pending.append(remote(buf.at[ds(0, 3 * n)], buf.at[ds(0, 3 * n)], dk=1, send=send, receive=receive))
            self.arrivals = remote(near, near, dk=1, send=send, receive=receive)
            rows = self.rows
            self.fa = remote(buf.at[rows(2, 0)], far.at[ds(0, hn)], dy=1, send=send)
            self.fb = remote(buf.at[rows(2, 1)], far.at[ds(hn, hn)], dy=-1, send=send)
            self.r1b, self.r1a = self.to(1, 1, 0, send, receive), self.to(1, 0, 0, send, receive)
            self.l1a, self.l1b = self.to(3, 0, 1, send, receive), self.to(3, 1, 1, send, receive)

        def to(self, e, half, side, send, receive):
            return remote(self.buf.at[self.rows(e, half)], self.near_.at[ds(side * self.n + half * (self.n // 2), self.n // 2)],
                          dy=(1, -1)[side], send=send, receive=receive)

        def begin(self):
            for c in (self.fa, self.fb, self.r1b, self.l1a):
                c.start()

        def middle(self):
            hn, buf, far, rows = self.n // 2, self.buf, self.far_, self.rows
            self.fa.wait_recv()
            buf[rows(1, 0), :] += far[ds(0, hn), :]
            self.r1a.start()
            self.fb.wait_recv()
            buf[rows(3, 1), :] += far[ds(hn, hn), :]
            self.l1b.start()

        def finish(self):
            self.arrivals.wait_recv()

        def total(self, start, size):
            n = self.n
            return self.buf[ds(start, size, 8), :] + (self.near_[ds(start, size, 8), :] + self.near_[ds(n + start, size, 8), :])

    class RowSum(Sum):
        def to(self, e, half, side, send, receive):
            hn = self.n // 2
            return remote(self.buf.at[self.rows(e, half)], self.near_.at[ds(side * hn, hn), kcol], dk=half - k + 2,
                          dy=(1, -1)[side], send=send, receive=receive)

    cp_g.wait()
    x1.own()
    d_g0.wait_recv()
    panel_source(0)
    cp_gk.wait()
    d_gk.wait_recv()
    chunked(cr, 4, lambda r, i: gr.__setitem__((r, slice(None)), grf[r, :].astype(BF16)))
    y1.own()
    cp_ql.wait()
    d_ql.wait_recv()
    qlr[ds(0, cr), :] = qlf[...].astype(BF16)
    y2.own()
    for c in d_own:
        c.start()
    cp_qr.wait()
    chunked(hc, 8, lambda r, i: qr.__setitem__((r, slice(None)), r_out[r, :].astype(BF16)))
    cp_r = local(r_in, r_out)
    x1.fwd()
    x2.own()
    panel_first(0)
    y1.fwd()
    y2.fwd()
    x1.near()
    d_g[1].start()
    d_g[3].start()
    d_g[1].wait_recv()
    panel_source(1)
    d_g[3].wait_recv()
    panel_source(3)
    y1.near()
    y1.far()
    h_part(0, ocol)
    h_part(0, kcol)
    x1.far()
    d_g[2].start()
    d_g[2].wait_recv()
    panel_source(2)
    y2.near()
    y2.far()
    q_send, q_receive, d_q_all = group(qlr.at[ds(0, 3 * rc)])
    pending.append(d_q_all)
    for s in (1, 3, 2):
        at = ds(s * cr + k * rc, rc)
        remote(qlr.at[at], qlr.at[at], dk=1, send=q_send, receive=q_receive).start()
    d_q_all.wait_recv()
    qlc[0] = qlr[ds(d * cr, cr), :].reshape(4, rq, qlr.shape[1])
    a2a = []
    for s, core in ((1, 0), (3, 1), (2, 0)):
        t = (y - x - s + 8) % 4
        far, near = new(sends, N_SEND), new(sends, N_SEND)
        a2a.append((core, remote(qlr.at[ds(t * cr + y * rq, rq, rq)], qlc.at[s, y], dx=s, send=far),
                    remote(qlc.at[s, y], qlc.at[s, y], dk=1, send=near)))

    def quarters(action):
        for core, across, over in a2a:
            pl.when(k == core)(functools.partial(action, across, over))

    quarters(lambda across, over: across.start())
    split_right(0)
    panel_first(1)
    panel_second(0)
    panel_first(3)
    panel_second(1)
    panel_third(0)
    x2.fwd()
    panel_first(2)
    panel_second(3)
    panel_third(1)
    cp_r.wait()
    split_left(0)
    product(0, 0, units)
    x2.near()
    for s in (1, 3):
        h_part(s, ocol)
        h_part(s, kcol)
    def hand_over(across, over):
        across.wait_recv()
        over.start()

    quarters(hand_over)
    for core, _, over in a2a:
        pl.when(k != core)(over.wait_recv)
    y3.own()
    panel_second(2)
    panel_third(3)

    def columns(core, piece):
        at, n = pieces[piece]
        return ds(core * hc + at, n, 128)

    d_h = [remote(hp.at[:, columns(1 - k, p)], hx.at[:, ds(*pieces[p])], dk=1) for p in range(2)]

    def h_send(p):
        x2.far((p,))
        h_part(2, columns(1 - k, p))
        d_h[p].start()
        h_part(2, columns(k, p))

    def h_finish(p):
        d_h[p].wait_recv()
        h[ds(0, cr), ds(*pieces[p])] = (hp[:, columns(k, p)] + hx[:, ds(*pieces[p])]).astype(BF16)
        x3[p].own()

    h_send(0)
    h_finish(0)
    l_slot(0)
    l_slot(1)
    y3.fwd()
    split_right(1)
    l_slot(2)
    l_slot(3)
    l_sum = Sum(lc, lf, ln, rc)
    l_sum.begin()
    h_send(1)
    x3[0].fwd()
    h_finish(1)
    panel_third(2)
    split_left(1)
    product(1, 0, units // 5)
    for c in cp_own:
        c.wait()
    d_own_all.wait_recv()

    def moments(p):
        x3[p].near()
        x3[p].far()
        cols = ds(*pieces[p])
        rot[:, cols] = dot(qlt[...], h[:, cols])

        def body(r, i):
            rotated = rot[r, cols]
            new_first = BETA1 * mx[r, cols] + (1.0 - BETA1) * rotated
            new_second = BETA2 * vx[r, cols] + (1.0 - BETA2) * rotated * rotated
            mx[r, cols] = new_first
            vx[r, cols] = new_second
            direction = (new_first / BIAS_ONE) / (jnp.sqrt(new_second / BIAS_TWO) + EPS)
            nb[r, cols] = direction.astype(BF16)

        chunked(cr, 10 if cr % 160 == 0 else 1, body)

    y3.near()
    y3.far()
    qlt[...] = qlc[...].reshape(4 * cr, qlc.shape[3]).T
    moments(0)
    x3[1].fwd()
    x4[0].own()
    l_sum.middle()
    product(1, units // 5, units * 3 // 5)
    moments(1)
    x4[0].fwd()
    x4[1].own()
    out_send, out_receive, outs_all = group(mx)
    pending.append(outs_all)
    for buf, out in ((mx, m_out), (vx, v_out)):
        remote(buf.at[orow], out.at[:, kcol], dk=1, send=out_send, receive=out_receive).start()
        out[:, kcol] = buf[krow, :]
    product(1, units * 3 // 5, units)

    d_k = [remote(kb.at[ds(k * cr, cr), ds(*piece)], kb.at[ds(k * cr, cr), ds(*piece)], dk=1) for piece in pieces]

    def k_part(p, slots):
        cols = ds(*pieces[p])
        return sum(dot(qlr[ds(((d + s) % 4) * cr, cr), :], nb[ds(s * cr, cr), cols]) for s in slots)

    def u_part(e, p, core, half=None):
        s = (x - y - e + 8) % 4
        at, n = pieces[p]
        start, size = (0, cr) if half is None else (half * rc, rc)
        part = dot(kb[ds(core * cr + start, size, rc), ds(at, n)], qr[ds(s * hc, hc), ds(core * hc + at, n, 128)], ((1,), (1,)))
        return ds(e * cr + start, size), part

    def u_add(*which):
        rows, part = u_part(*which)
        uc[rows, :] += part

    x4[0].near()
    x4[0].far()
    kb[ds(k * cr, cr), ds(*pieces[0])] = k_part(0, range(4)).astype(BF16)
    d_k[0].start()
    x4[1].fwd()
    @pl.when(d != 3)
    def _():
        p_all.wait_send()

    @pl.when(d != 1)
    def _():
        q_all.wait_send()

    d_k[0].wait_recv()
    for e in (2, 1, 3, 0):
        rows, part = u_part(e, 0, 0)
        uc[rows, :] = part + u_part(e, 0, 1)[1]
    x4[1].near()
    rot[:, ds(*pieces[1])] = k_part(1, (0, 1, 3))
    x4[1].far()
    kb[ds(k * cr, cr), ds(*pieces[1])] = (rot[:, ds(*pieces[1])] + k_part(1, (2,))).astype(BF16)
    d_k[1].start()
    u_sum = RowSum(uc, uf, un, cr)
    for e in (2, 1):
        u_add(e, 1, k)
    d_k[1].wait_recv()
    u_add(2, 1, 1 - k, 0)
    u_sum.fa.start()
    u_add(2, 1, 1 - k, 1)
    u_sum.fb.start()
    u_add(1, 1, 1 - k)
    u_sum.r1b.start()
    u_add(3, 1, k)
    u_add(3, 1, 1 - k)
    u_sum.l1a.start()
    u_add(0, 1, k)
    u_add(0, 1, 1 - k)
    d_u = remote(uc.at[orow], uo, dk=1)
    d_u.start()
    l_sum.finish()
    cp_l.wait()
    l_out[...] = BETA2 * l_out[...] + (1.0 - BETA2) * l_sum.total(0, rc)
    outs_all.wait_recv()
    u_sum.middle()
    d_u.wait_recv()
    u_sum.finish()
    for mine, cols in ((True, kcol), (False, ocol)):
        total = (uc[krow, :] if mine else uo[...]) + (un[ds(0, rc), cols] + un[ds(rc, rc), cols])
        w_out[:, cols] = wx[:, cols] - LR * total
    for c in pending:
        c.wait_send()
    for core, across, over in a2a:
        @pl.when(k == core)
        def _():
            across.wait_send()
            over.wait_send()


def write_kernel(*refs):
    n = (len(refs) - 1) // 2
    copies = []
    for a, b in zip(refs[:n], refs[n:2 * n]):
        step = a.shape[0] // 4 if a.shape[0] % 32 == 0 and a.shape[0] > 256 else a.shape[0]
        for r in range(0, a.shape[0], step):
            copies.append(pltpu.make_async_copy(a.at[pl.ds(r, step)], b.at[pl.ds(r, step)], refs[-1].at[len(copies)]))
    for c in copies:
        c.start()
    for c in copies:
        c.wait()


def solution(mesh):
    tile_spec = P(("layer", "row"), "col")

    def step(weight, grad_in, mom_first, mom_second, stat_left, stat_right, basis_left, basis_right):
        rc, cc = grad_in.shape
        cr, hc, q = 2 * rc, cc // 2, basis_left.shape[1]
        scratch = [
            ((4 * cr, cc), F32), ((4 * cr, hc), F32), ((4 * hc, cc), BF16),
            ((cr, hc), F32), ((4 * cr, hc), BF16),
            ((cr, q), F32), ((4 * cr, q), BF16), ((4, 4, cr // 4, q), BF16), ((q, 4 * cr), BF16),
            ((rc, cc), F32), ((cr, hc), F32), ((cr, hc), F32),
            ((4 * cr, hc), BF16), ((4 * cr, hc), BF16), ((cr, cc), F32),
            ((cr, hc), F32),
            ((2 * cr, hc), BF16), ((cr, hc), F32), ((cr, cc), F32), ((rc, hc), F32),
            ((4 * rc, q), F32), ((rc, q), F32), ((2 * rc, q), F32),
            ((3 * hc, 2 * cr), BF16), ((6 * cr, cc), BF16), ((3 * rc, cc), BF16),
        ]
        args = (weight, grad_in, mom_first, mom_second, stat_left, stat_right, basis_left, basis_right)
        vmem_spec, any_spec = pl.BlockSpec(memory_space=pltpu.VMEM), pl.BlockSpec(memory_space=pl.ANY)
        outs = tuple(jax.ShapeDtypeStruct(a.shape, F32) for a in (weight, mom_first, mom_second, stat_left, stat_right))
        results = pl.pallas_call(
            kernel,
            out_shape=outs,
            in_specs=[pl.BlockSpec(memory_space=pltpu.HBM)] * 8,
            out_specs=(vmem_spec,) * 5,
            scratch_shapes=[pltpu.VMEM(s, t) for s, t in scratch]
            + [pltpu.SemaphoreType.DMA((n,)) for n in (N_SEND, N_RECEIVE, N_LOCAL)],
            compiler_params=pltpu.CompilerParams(collective_id=0, has_side_effects=True, vmem_limit_bytes=VMEM_BYTES),
        )(*(pltpu.with_memory_space_constraint(a, pltpu.HBM) for a in args))
        return pl.pallas_call(
            write_kernel,
            out_shape=outs,
            in_specs=[any_spec] * 5,
            out_specs=(any_spec,) * 5,
            scratch_shapes=[pltpu.SemaphoreType.DMA((8,))],
            compiler_params=pltpu.CompilerParams(vmem_limit_bytes=1_000_000),
        )(*(pltpu.with_memory_space_constraint(a, pltpu.VMEM) for a in results))

    return jax.shard_map(step, mesh=mesh, in_specs=(tile_spec,) * 8, out_specs=(tile_spec,) * 5, check_vma=False)
```

```python
import functools

import jax
import jax.numpy as jnp
from jax import lax
from jax.experimental import pallas as pl
from jax.experimental.pallas import tpu as pltpu
from jax.sharding import PartitionSpec as P

BETA1 = 0.9
BETA2 = 0.9
EPS = 1e-8
LR = 0.1
STEP = 10
BIAS_ONE = 1.0 - BETA1 ** STEP
BIAS_TWO = 1.0 - BETA2 ** STEP
MESH = pl.DeviceIdType.MESH
OTHERS = (1, 3, 2)
N_SEND, N_RECEIVE, N_LOCAL = 33, 71, 9
VMEM_BYTES = 50_000_000
F32 = jnp.float32
BF16 = jnp.bfloat16
SIX_PASSES = [(a, b) for a in range(3) for b in range(3 - a)]
NN, NT = (((1,), (i,)) for i in range(2))


def dot(a, b, dims=NN):
    return lax.dot_general(a, b, (dims, ((), ())), preferred_element_type=F32)


def split_three(a):
    hi = a.astype(BF16)
    rest = a - hi.astype(F32)
    mid = rest.astype(BF16)
    return hi, mid, (rest - mid.astype(F32)).astype(BF16)


def kernel(w_in, g_in, m_in, v_in, l_in, r_in, ql_in, qr_in, w_out, m_out, v_out, l_out, r_out,
           gf, px, qr, grf, gr, qlf, qlr, qlc, qlt, wx, mx, vx, h, nb, hp, hx, kb, uf, un, uo,
           lc, lf, ln, lhs3, rhs3, la, ss, rs, ls):
    rc, cc = g_in.shape
    cr, hc = 2 * rc, cc // 2
    kk = 2 * cr
    nt = 256 if cc % 256 == 0 else cc
    tb = 128 if kk % 128 == 0 else kk
    row, y = lax.axis_index("row"), lax.axis_index("col")
    x, k = row // 2, row % 2
    d = (y - x + 4) % 4
    rq = cr // 4
    uc, rot = px, grf
    pa = 128 * (hc * 2 // 5 // 128) if hc % 128 == 0 else hc // 2
    pieces = ((0, pa), (pa, hc - pa))

    def ds(start, size, unit=None):
        return pl.ds(start if isinstance(start, int) else pl.multiple_of(start, unit or size), size)

    kcol, ocol = ds(k * hc, hc), ds((1 - k) * hc, hc)
    krow, orow = ds(k * rc, rc), ds((1 - k) * rc, rc)

    sends, receives, pending = [0], [0], []

    def new(counter, limit):
        counter[0] += 1
        assert counter[0] <= limit
        return counter[0] - 1

    def device(dx=0, dk=0, dy=0):
        return {"row": ((x + dx + 4) % 4) * 2 + (k + dk) % 2, "col": (y + dy + 4) % 4}

    def remote(src, dst, dx=0, dk=0, dy=0, send=None, receive=None):
        own = send is None
        copy = pltpu.make_async_remote_copy(
            src_ref=src, dst_ref=dst, send_sem=ss.at[new(sends, N_SEND) if own else send],
            recv_sem=rs.at[new(receives, N_RECEIVE) if receive is None else receive],
            device_id=device(dx, dk, dy), device_id_type=MESH)
        if own:
            pending.append(copy)
        return copy

    def group(ref):
        send, receive = new(sends, N_SEND), new(receives, N_RECEIVE)
        return send, receive, remote(ref, ref, dk=1, send=send, receive=receive)

    lcounter = [0]

    def local(src, dst):
        index = lcounter[0]
        lcounter[0] += 1
        assert index < N_LOCAL
        copy = pltpu.make_async_copy(src, dst, ls.at[index])
        copy.start()
        return copy

    class Ring:
        def __init__(self, buf, at, axis, total, near, far, forward=None, absolute=False):
            send = new(sends, N_SEND)
            pending.append(remote(buf.at[total], buf.at[total], dk=1, send=send, receive=0))

            def cp(s0, half, s1, step, receive=None, at=at):
                return remote(buf.at[at(s0, half)], buf.at[at(s0 if absolute else s1, half)], send=send, receive=receive, **{axis: step})

            def wait(view):
                receive = new(receives, N_RECEIVE)
                return receive, remote(buf.at[view], buf.at[view], dk=1, send=send, receive=receive)
            self.ra, self.lb = cp(0, 0, 1, 1), cp(0, 1, 3, -1)
            receive, self.near_ = wait(near)
            self.rb, self.la = cp(0, 1, 1, 1, receive), cp(0, 0, 3, -1, receive)
            self.fr, self.fl, self.far_ = [], [], []
            for parts, view in forward or [([at], far)]:
                receive, wait_far = wait(view)
                self.far_.append(wait_far)
                for part in parts:
                    self.fr.append(cp(1, 0, 2, 1, receive, part))
                    self.fl.append(cp(3, 1, 2, -1, receive, part))

        def own(self):
            for c in (self.ra, self.lb, self.rb, self.la):
                c.start()

        def fwd(self):
            self.ra.wait_recv()
            for c in self.fr:
                c.start()
            self.lb.wait_recv()
            for c in self.fl:
                c.start()

        def near(self):
            self.near_.wait_recv()

        def far(self, parts=None):
            for i in range(len(self.far_)) if parts is None else parts:
                self.far_[i].wait_recv()

    def chunked(total, parts, body):
        size = total // parts

        @pl.loop(0, parts)
        def _(i):
            body(ds(i * size, size), i)

    cp_g = local(g_in, gf.at[krow])
    cp_gk = local(g_in.at[:, kcol], grf.at[krow])
    cp_ql = local(ql_in, qlf.at[krow])
    cp_qr = local(qr_in, r_out)
    cp_own = [local(a.at[:, kcol], b.at[krow]) for a, b in ((m_in, mx), (v_in, vx))] + [local(w_in, wx)]
    cp_l = local(l_in, l_out)
    barrier = pltpu.get_barrier_semaphore()
    partners = [device(dx=2), device(dk=1)]
    for step in (1, -1):
        partners += [device(dx=step), device(dy=step), device(dk=1, dy=step)]
    for partner in partners:
        pl.semaphore_signal(barrier, inc=1, device_id=partner, device_id_type=MESH)
    pl.semaphore_wait(barrier, len(partners))

    d_gk = remote(g_in.at[:, ocol], grf.at[krow], dk=1)
    d_g0 = remote(g_in, gf.at[krow], dk=1)
    d_ql = remote(ql_in, qlf.at[krow], dk=1)
    own_send, own_receive, d_own_all = group(mx)
    pending.append(d_own_all)
    d_own = [remote(a.at[:, ocol], b.at[krow], dk=1, send=own_send, receive=own_receive) for a, b in ((m_in, mx), (v_in, vx))]
    d_g0.start()
    d_gk.start()
    d_ql.start()

    def grow(s, half):
        return ds((s * 2 + k) * rc + half * (rc // 2), rc // 2)

    def slot_rows(n, start=0, size=None, cols=None):
        size = n if size is None else size
        return lambda s, half: (ds(s * n + start + half * (size // 2), size // 2, 8), slice(None) if cols is None else ds(*cols))

    def whole(s):
        return ds((s * 2 + k) * rc, rc)

    def tiles(n, cols=None):
        cols = slice(None) if cols is None else ds(*cols)
        return {"total": (ds(0, 3 * n), cols), "near": (ds(0, n), cols), "far": (ds(0, n), cols)}

    x1 = Ring(gf, grow, "dx", **tiles(rc))
    x2 = Ring(qr, slot_rows(hc), "dx", **tiles(hc), forward=[
        ([slot_rows(hc, cols=(c * hc + at, n)) for c in range(2)], (ds(0, hc), ds(0, 2 * n))) for at, n in pieces])
    x3 = [Ring(h, slot_rows(cr, cols=piece), "dx", **tiles(cr, piece)) for piece in pieces]
    x4 = [Ring(nb, slot_rows(cr, cols=piece), "dx", **tiles(cr, piece)) for piece in pieces]
    y1 = Ring(gr, slot_rows(cr), "dy", **tiles(cr))
    y2 = Ring(qlr, slot_rows(cr, start=k * rc, size=rc), "dy", **tiles(rc))
    three = pl.ds(0, 3)
    y3 = Ring(qlc, lambda s, half: (pl.ds(1 + 2 * half, 2 - half), (y - s + 4) % 4), "dy", absolute=True,
              total=(three, three), near=(three, 0), far=(three, 0))
    d_g = {s: remote(gf.at[whole(s)], gf.at[whole(s)], dk=1) for s in OTHERS}

    def prow(s, c):
        return ds((s * 2 + c) * rc, rc)

    p_src, p_fwd, q_src, q_fwd = {}, {}, {}, {}
    p_send, q_send = new(sends, N_SEND), new(sends, N_SEND)
    p_all, q_all = (remote(px.at[ds(0, 4 * rc)], px.at[ds(0, 4 * rc)], dk=1, send=i, receive=0) for i in (p_send, q_send))
    for s in (0, *OTHERS):
        pi, qi = new(receives, N_RECEIVE), new(receives, N_RECEIVE)
        p_src[s] = remote(gf.at[prow(s, 0), kcol], px.at[prow(s, 0)], dy=1, send=p_send, receive=pi)
        p_fwd[s] = remote(px.at[prow(s, 0)], px.at[prow(s, 0)], dy=1, send=p_send, receive=pi)
        q_src[s] = remote(gf.at[prow(s, 1), kcol], px.at[prow(s, 1)], dy=-1, send=q_send, receive=qi)
        q_fwd[s] = remote(px.at[prow(s, 1)], px.at[prow(s, 1)], dy=-1, send=q_send, receive=qi)

    def panel_source(s):
        @pl.when(d == 0)
        def _():
            p_src[s].start()
            q_src[s].start()

    def panel_first(s):
        @pl.when(d == 1)
        def _():
            p_fwd[s].wait_recv()
            p_fwd[s].start()

        @pl.when(d == 3)
        def _():
            q_fwd[s].wait_recv()
            q_fwd[s].start()

    def panel_second(s):
        @pl.when(d == 2)
        def _():
            p_fwd[s].wait_recv()
            p_fwd[s].start()
            q_fwd[s].wait_recv()
            q_fwd[s].start()

    def panel_third(s):
        @pl.when(d == 3)
        def _():
            p_fwd[s].wait_recv()

        @pl.when(d == 1)
        def _():
            q_fwd[s].wait_recv()

    def h_part(s, cols):
        t = (d + s) % 4
        part = dot(gr[ds(t * cr, cr), :], qr[ds(s * hc, hc), cols])
        if s == 0:
            hp[:, cols] = part
        else:
            hp[:, cols] += part

    units = 2 * (cc // nt)

    def split_right(p):
        base = p * kk

        def body(r, i):
            for q, piece in enumerate(split_three(gf[ds(base + i * (kk // 8), kk // 8, 8), :])):
                rhs3[ds(q * kk + i * (kk // 8), kk // 8, 8), :] = piece

        chunked(kk, 8, body)
        if p == 0:
            for q in range(3):
                la[ds(q * rc, rc), :] = rhs3[ds(q * kk + k * rc, rc, rc), :]

    def split_left(p):
        base = p * kk

        @pl.when(d == 0)
        def _():
            chunked(kk, 4, lambda r, i: px.__setitem__(
                (ds(base + i * (kk // 4), kk // 4, 8), slice(None)), gf[ds(base + i * (kk // 4), kk // 4, 8), kcol]))

        def body(cols, i):
            for q, piece in enumerate(split_three(px[ds(base + i * tb, tb, 8), :].T)):
                lhs3[ds(q * hc, hc), cols] = piece

        chunked(kk, kk // tb, body)

    def product(p, first, last):
        @pl.loop(first, last)
        def _(i):
            m, j = i // (cc // nt), i % (cc // nt)
            rows = ds(m * (hc // 2), hc // 2)
            cols = ds(j * nt, nt)
            acc = sum(dot(lhs3[ds(a * hc + m * (hc // 2), hc // 2), :], rhs3[ds(b * kk, kk), cols]) for a, b in SIX_PASSES)
            if p == 0:
                r_out[rows, cols] = BETA2 * r_out[rows, cols] + (1.0 - BETA2) * acc
            else:
                r_out[rows, cols] += (1.0 - BETA2) * acc

    def l_slot(s):
        e = (x - y - s + 8) % 4
        at = [ds(q * kk + (s % 2) * cr, cr) for q in range(3)]
        high = dot(la[...], rhs3[at[0], :], NT)
        middle = dot(la[ds(0, 2 * rc), :], rhs3[at[1], :], NT)
        low = dot(la[ds(0, rc), :], rhs3[at[2], :], NT)
        lc[ds(e * rc, rc), :] = high[:rc] + (high[rc:2 * rc] + middle[:rc]) + (high[2 * rc:] + middle[rc:] + low)

    class Sum:
        def __init__(self, buf, far, near, n):
            self.buf, self.far_, self.near_, self.n = buf, far, near, n
            hn = n // 2
            self.rows = lambda e, half: ds(e * n + half * hn, hn)
            send = new(sends, N_SEND)
            receive = new(receives, N_RECEIVE)
            pending.append(remote(buf.at[ds(0, 3 * n)], buf.at[ds(0, 3 * n)], dk=1, send=send, receive=receive))
            self.arrivals = remote(near, near, dk=1, send=send, receive=receive)
            rows = self.rows
            self.fa = remote(buf.at[rows(2, 0)], far.at[ds(0, hn)], dy=1, send=send)
            self.fb = remote(buf.at[rows(2, 1)], far.at[ds(hn, hn)], dy=-1, send=send)
            self.r1b, self.r1a = self.to(1, 1, 0, send, receive), self.to(1, 0, 0, send, receive)
            self.l1a, self.l1b = self.to(3, 0, 1, send, receive), self.to(3, 1, 1, send, receive)

        def to(self, e, half, side, send, receive):
            return remote(self.buf.at[self.rows(e, half)], self.near_.at[ds(side * self.n + half * (self.n // 2), self.n // 2)],
                          dy=(1, -1)[side], send=send, receive=receive)

        def begin(self):
            for c in (self.fa, self.fb, self.r1b, self.l1a):
                c.start()

        def middle(self):
            hn, buf, far, rows = self.n // 2, self.buf, self.far_, self.rows
            self.fa.wait_recv()
            buf[rows(1, 0), :] += far[ds(0, hn), :]
            self.r1a.start()
            self.fb.wait_recv()
            buf[rows(3, 1), :] += far[ds(hn, hn), :]
            self.l1b.start()

        def finish(self):
            self.arrivals.wait_recv()

        def total(self, start, size):
            n = self.n
            return self.buf[ds(start, size, 8), :] + (self.near_[ds(start, size, 8), :] + self.near_[ds(n + start, size, 8), :])

    class RowSum(Sum):
        def to(self, e, half, side, send, receive):
            hn = self.n // 2
            return remote(self.buf.at[self.rows(e, half)], self.near_.at[ds(side * hn, hn), kcol], dk=half - k + 2,
                          dy=(1, -1)[side], send=send, receive=receive)

    cp_g.wait()
    x1.own()
    d_g0.wait_recv()
    panel_source(0)
    cp_gk.wait()
    d_gk.wait_recv()
    chunked(cr, 4, lambda r, i: gr.__setitem__((r, slice(None)), grf[r, :].astype(BF16)))
    y1.own()
    cp_ql.wait()
    d_ql.wait_recv()
    qlr[ds(0, cr), :] = qlf[...].astype(BF16)
    y2.own()
    for c in d_own:
        c.start()
    cp_qr.wait()
    chunked(hc, 8, lambda r, i: qr.__setitem__((r, slice(None)), r_out[r, :].astype(BF16)))
    cp_r = local(r_in, r_out)
    x1.fwd()
    x2.own()
    panel_first(0)
    y1.fwd()
    y2.fwd()
    x1.near()
    d_g[1].start()
    d_g[3].start()
    d_g[1].wait_recv()
    panel_source(1)
    d_g[3].wait_recv()
    panel_source(3)
    y1.near()
    y1.far()
    h_part(0, ocol)
    h_part(0, kcol)
    x1.far()
    d_g[2].start()
    d_g[2].wait_recv()
    panel_source(2)
    y2.near()
    y2.far()
    q_send, q_receive, d_q_all = group(qlr.at[ds(0, 3 * rc)])
    pending.append(d_q_all)
    for s in OTHERS:
        at = ds(s * cr + k * rc, rc)
        remote(qlr.at[at], qlr.at[at], dk=1, send=q_send, receive=q_receive).start()
    d_q_all.wait_recv()
    qlc[0] = qlr[ds(d * cr, cr), :].reshape(4, rq, qlr.shape[1])
    a2a = []
    for s, core in ((1, 0), (3, 1), (2, 0)):
        t = (y - x - s + 8) % 4
        far, near = new(sends, N_SEND), new(sends, N_SEND)
        a2a.append((core, remote(qlr.at[ds(t * cr + y * rq, rq, rq)], qlc.at[s, y], dx=s, send=far),
                    remote(qlc.at[s, y], qlc.at[s, y], dk=1, send=near)))

    def quarters(action):
        for core, across, over in a2a:
            pl.when(k == core)(functools.partial(action, across, over))

    quarters(lambda across, over: across.start())
    split_right(0)
    panel_first(1)
    panel_second(0)
    panel_first(3)
    panel_second(1)
    panel_third(0)
    x2.fwd()
    panel_first(2)
    panel_second(3)
    panel_third(1)
    cp_r.wait()
    split_left(0)
    product(0, 0, units)
    x2.near()
    for s in (1, 3):
        h_part(s, ocol)
        h_part(s, kcol)
    def hand_over(across, over):
        across.wait_recv()
        over.start()

    quarters(hand_over)
    for core, _, over in a2a:
        pl.when(k != core)(over.wait_recv)
    y3.own()
    panel_second(2)
    panel_third(3)

    def columns(core, piece):
        at, n = pieces[piece]
        return ds(core * hc + at, n, 128)

    d_h = [remote(hp.at[:, columns(1 - k, p)], hx.at[:, ds(*pieces[p])], dk=1) for p in range(2)]

    def h_send(p):
        x2.far((p,))
        h_part(2, columns(1 - k, p))
        d_h[p].start()
        h_part(2, columns(k, p))

    def h_finish(p):
        d_h[p].wait_recv()
        h[ds(0, cr), ds(*pieces[p])] = (hp[:, columns(k, p)] + hx[:, ds(*pieces[p])]).astype(BF16)
        x3[p].own()

    h_send(0)
    h_finish(0)
    l_slot(0)
    l_slot(1)
    y3.fwd()
    split_right(1)
    l_slot(2)
    l_slot(3)
    l_sum = Sum(lc, lf, ln, rc)
    l_sum.begin()
    h_send(1)
    x3[0].fwd()
    h_finish(1)
    panel_third(2)
    split_left(1)
    product(1, 0, units // 5)
    for c in cp_own:
        c.wait()
    d_own_all.wait_recv()

    def moments(p):
        x3[p].near()
        x3[p].far()
        cols = ds(*pieces[p])
        rot[:, cols] = dot(qlt[...], h[:, cols])

        def body(r, i):
            rotated = rot[r, cols]
            new_first = BETA1 * mx[r, cols] + (1.0 - BETA1) * rotated
            new_second = BETA2 * vx[r, cols] + (1.0 - BETA2) * rotated * rotated
            mx[r, cols] = new_first
            vx[r, cols] = new_second
            direction = (new_first / BIAS_ONE) / (jnp.sqrt(new_second / BIAS_TWO) + EPS)
            nb[r, cols] = direction.astype(BF16)

        chunked(cr, 10 if cr % 160 == 0 else 1, body)

    y3.near()
    y3.far()
    qlt[...] = qlc[...].reshape(4 * cr, qlc.shape[3]).T
    moments(0)
    x3[1].fwd()
    x4[0].own()
    l_sum.middle()
    product(1, units // 5, units * 3 // 5)
    moments(1)
    x4[0].fwd()
    x4[1].own()
    out_send, out_receive, outs_all = group(mx)
    pending.append(outs_all)
    for buf, out in ((mx, m_out), (vx, v_out)):
        remote(buf.at[orow], out.at[:, kcol], dk=1, send=out_send, receive=out_receive).start()
        out[:, kcol] = buf[krow, :]
    product(1, units * 3 // 5, units)

    d_k = [remote(kb.at[ds(k * cr, cr), ds(*piece)], kb.at[ds(k * cr, cr), ds(*piece)], dk=1) for piece in pieces]

    def k_part(p, slots):
        cols = ds(*pieces[p])
        return sum(dot(qlr[ds(((d + s) % 4) * cr, cr), :], nb[ds(s * cr, cr), cols]) for s in slots)

    def u_part(e, p, core, half=None):
        s = (x - y - e + 8) % 4
        at, n = pieces[p]
        start, size = (0, cr) if half is None else (half * rc, rc)
        part = dot(kb[ds(core * cr + start, size, rc), ds(at, n)], qr[ds(s * hc, hc), ds(core * hc + at, n, 128)], NT)
        return ds(e * cr + start, size), part

    def u_add(*which):
        rows, part = u_part(*which)
        uc[rows, :] += part

    x4[0].near()
    x4[0].far()
    kb[ds(k * cr, cr), ds(*pieces[0])] = k_part(0, range(4)).astype(BF16)
    d_k[0].start()
    x4[1].fwd()
    @pl.when(d != 3)
    def _():
        p_all.wait_send()

    @pl.when(d != 1)
    def _():
        q_all.wait_send()

    d_k[0].wait_recv()
    for e in (2, 1, 3, 0):
        rows, part = u_part(e, 0, 0)
        uc[rows, :] = part + u_part(e, 0, 1)[1]
    x4[1].near()
    rot[:, ds(*pieces[1])] = k_part(1, (0, 1, 3))
    x4[1].far()
    kb[ds(k * cr, cr), ds(*pieces[1])] = (rot[:, ds(*pieces[1])] + k_part(1, (2,))).astype(BF16)
    d_k[1].start()
    u_sum = RowSum(uc, uf, un, cr)
    for e in (2, 1):
        u_add(e, 1, k)
    d_k[1].wait_recv()
    u_add(2, 1, 1 - k, 0)
    u_sum.fa.start()
    u_add(2, 1, 1 - k, 1)
    u_sum.fb.start()
    u_add(1, 1, 1 - k)
    u_sum.r1b.start()
    u_add(3, 1, k)
    u_add(3, 1, 1 - k)
    u_sum.l1a.start()
    u_add(0, 1, k)
    u_add(0, 1, 1 - k)
    d_u = remote(uc.at[orow], uo, dk=1)
    d_u.start()
    l_sum.finish()
    cp_l.wait()
    l_out[...] = BETA2 * l_out[...] + (1.0 - BETA2) * l_sum.total(0, rc)
    outs_all.wait_recv()
    u_sum.middle()
    d_u.wait_recv()
    u_sum.finish()
    for mine, cols in ((True, kcol), (False, ocol)):
        total = (uc[krow, :] if mine else uo[...]) + (un[ds(0, rc), cols] + un[ds(rc, rc), cols])
        w_out[:, cols] = wx[:, cols] - LR * total
    for c in pending:
        c.wait_send()
    for core, across, over in a2a:
        @pl.when(k == core)
        def _():
            across.wait_send()
            over.wait_send()


def write_kernel(*refs):
    n = (len(refs) - 1) // 2
    copies = [pltpu.make_async_copy(a, b, refs[-1].at[i]) for i, (a, b) in enumerate(zip(refs, refs[n:-1]))]
    for c in copies:
        c.start()
    for c in copies:
        c.wait()


def solution(mesh):
    tile_spec = P(("layer", "row"), "col")

    def step(weight, grad_in, mom_first, mom_second, stat_left, stat_right, basis_left, basis_right):
        rc, cc = grad_in.shape
        cr, hc, q = 2 * rc, cc // 2, basis_left.shape[1]
        scratch = [
            ((4 * cr, cc), F32), ((4 * cr, hc), F32), ((4 * hc, cc), BF16),
            ((cr, hc), F32), ((4 * cr, hc), BF16),
            ((cr, q), F32), ((4 * cr, q), BF16), ((4, 4, cr // 4, q), BF16), ((q, 4 * cr), BF16),
            ((rc, cc), F32), ((cr, hc), F32), ((cr, hc), F32),
            ((4 * cr, hc), BF16), ((4 * cr, hc), BF16), ((cr, cc), F32),
            ((cr, hc), F32),
            ((2 * cr, hc), BF16), ((cr, hc), F32), ((cr, cc), F32), ((rc, hc), F32),
            ((4 * rc, q), F32), ((rc, q), F32), ((2 * rc, q), F32),
            ((3 * hc, 2 * cr), BF16), ((6 * cr, cc), BF16), ((3 * rc, cc), BF16),
        ]
        args = (weight, grad_in, mom_first, mom_second, stat_left, stat_right, basis_left, basis_right)
        vmem_spec, any_spec = pl.BlockSpec(memory_space=pltpu.VMEM), pl.BlockSpec(memory_space=pl.ANY)
        outs = tuple(jax.ShapeDtypeStruct(a.shape, F32) for a in (weight, mom_first, mom_second, stat_left, stat_right))
        results = pl.pallas_call(
            kernel,
            out_shape=outs,
            in_specs=[pl.BlockSpec(memory_space=pltpu.HBM)] * 8,
            out_specs=(vmem_spec,) * 5,
            scratch_shapes=[pltpu.VMEM(s, t) for s, t in scratch]
            + [pltpu.SemaphoreType.DMA((n,)) for n in (N_SEND, N_RECEIVE, N_LOCAL)],
            compiler_params=pltpu.CompilerParams(collective_id=0, has_side_effects=True, vmem_limit_bytes=VMEM_BYTES),
        )(*(pltpu.with_memory_space_constraint(a, pltpu.HBM) for a in args))
        return pl.pallas_call(
            write_kernel,
            out_shape=outs,
            in_specs=[any_spec] * 5,
            out_specs=(any_spec,) * 5,
            scratch_shapes=[pltpu.SemaphoreType.DMA((len(outs),))],
            compiler_params=pltpu.CompilerParams(vmem_limit_bytes=1_000_000),
        )(*(pltpu.with_memory_space_constraint(a, pltpu.VMEM) for a in results))

    return jax.shard_map(step, mesh=mesh, in_specs=(tile_spec,) * 8, out_specs=(tile_spec,) * 5, check_vma=False)
```

```python
import math

import jax
import jax.numpy as jnp
from jax import lax
from jax.experimental import pallas as pl
from jax.experimental.pallas import tpu as pltpu
from jax.sharding import PartitionSpec as P

BETA1 = 0.9
BETA2 = 0.9
EPS = 1e-8
LR = 0.1
STEP = 10
BIAS_ONE = 1.0 - BETA1 ** STEP
BIAS_TWO = 1.0 - BETA2 ** STEP
MESH = pl.DeviceIdType.MESH
OTHERS = (1, 3, 2)
N_SEND, N_RECEIVE, N_LOCAL = 13, 51, 7
VMEM_BYTES = 50_000_000
F32 = jnp.float32
BF16 = jnp.bfloat16
SIX_PASSES = [(a, b) for a in range(3) for b in range(3 - a)]
NN, NT = (((1,), (i,)) for i in range(2))


def dot(a, b, dims=NN):
    return lax.dot_general(a, b, (dims, ((), ())), preferred_element_type=F32)


def split_three(a):
    hi = a.astype(BF16)
    rest = a - hi.astype(F32)
    mid = rest.astype(BF16)
    return hi, mid, (rest - mid.astype(F32)).astype(BF16)


def kernel(w_in, g_in, m_in, v_in, l_in, r_in, ql_in, qr_in, w_out, m_out, v_out, l_out, r_out,
           gf, px, qr, grf, gr, qlf, qlr, qlc, qlt, wx, mx, vx, h, nb, hp, hx, kb, uf, un, uo,
           lc, lf, ln, lhs3, rhs3, la, ss, rs, ls):
    rc, cc = g_in.shape
    cr, hc = 2 * rc, cc // 2
    kk = 2 * cr
    nt = 256 if cc % 256 == 0 else cc
    tb = 128 if kk % 128 == 0 else kk
    row, y = lax.axis_index("row"), lax.axis_index("col")
    x, k = row // 2, row % 2
    d = (y - x + 4) % 4
    rq = cr // 4
    uc, rot = px, grf
    pa = 128 * (hc * 2 // 5 // 128) if hc % 128 == 0 else hc // 2
    pieces = ((0, pa), (pa, hc - pa))

    def ds(start, size, unit=None):
        return pl.ds(start if isinstance(start, int) else pl.multiple_of(start, unit or size), size)

    kcol, ocol = ds(k * hc, hc), ds((1 - k) * hc, hc)
    krow, orow = ds(k * rc, rc), ds((1 - k) * rc, rc)

    sends, receives, pending = [0], [0], []

    def new(counter, limit):
        counter[0] += 1
        assert counter[0] <= limit
        return counter[0] - 1

    def device(dx=0, dk=0, dy=0):
        return {"row": ((x + dx + 4) % 4) * 2 + (k + dk) % 2, "col": (y + dy + 4) % 4}

    class Batch:
        def __init__(self):
            self.semaphore, self.bytes = new(sends, N_SEND), 0

        def wait(self):
            rows, rest = divmod(self.bytes, cc * gf.dtype.itemsize)
            assert rest == 0 and rows <= gf.shape[0]
            arrival(gf.at[ds(0, rows)], None, self.semaphore).wait_send()

    def remote(src, dst, dx=0, dk=0, dy=0, send=None, receive=None):
        if isinstance(send, Batch):
            send.bytes += math.prod(src.shape) * jnp.dtype(src.dtype).itemsize
            index = send.semaphore
        else:
            index = new(sends, N_SEND) if send is None else send
        copy = pltpu.make_async_remote_copy(
            src_ref=src, dst_ref=dst, send_sem=ss.at[index],
            recv_sem=rs.at[new(receives, N_RECEIVE) if receive is None else receive],
            device_id=device(dx, dk, dy), device_id_type=MESH)
        if send is None:
            pending.append(copy)
        return copy

    def arrival(view, receive, send=0):
        return remote(view, view, dk=1, send=send, receive=receive or 0)

    def group(view):
        receive = new(receives, N_RECEIVE)
        return receive, arrival(view, receive)

    batch_x, batch_xy, batch_first, batch_last = (Batch() for _ in range(4))
    lcounter = [0]

    def local(src, dst, index=None):
        if index is None:
            index = lcounter[0]
            lcounter[0] += 1
        assert index < N_LOCAL
        copy = pltpu.make_async_copy(src, dst, ls.at[index])
        copy.start()
        return copy

    class Ring:
        def __init__(self, buf, at, axis, near, rest, total=None, batch=None, forward=None, absolute=False, joined=False):
            if batch is None:
                batch = new(sends, N_SEND)
                pending.append(arrival(buf.at[total], None, batch))

            def cp(s0, half, s1, step, receive, at=at):
                return remote(buf.at[at(s0, half)], buf.at[at(s0 if absolute else s1, half)], send=batch, receive=receive, **{axis: step})

            first, self.first = group(buf.at[near])
            self.ra, self.lb = cp(0, 0, 1, 1, first), cp(0, 1, 3, -1, first)
            second, self.near_ = group(buf.at[rest if joined else near])
            self.rb, self.la = cp(0, 1, 1, 1, second), cp(0, 0, 3, -1, second)
            self.fr, self.fl, self.far_ = [], [], []
            for parts, view in forward or [([at], near)]:
                last, wait = (second, self.near_) if joined else group(buf.at[view])
                self.far_.append(wait)
                for part in parts:
                    self.fr.append(cp(1, 0, 2, 1, last, part))
                    self.fl.append(cp(3, 1, 2, -1, last, part))

        def own(self):
            for c in (self.ra, self.lb, self.rb, self.la):
                c.start()

        def fwd(self):
            self.first.wait_recv()
            for c in self.fr + self.fl:
                c.start()

        def near(self):
            self.near_.wait_recv()

        def far(self, parts=None):
            for i in range(len(self.far_)) if parts is None else parts:
                self.far_[i].wait_recv()

    def chunked(total, parts, body):
        size = total // parts

        @pl.loop(0, parts)
        def _(i):
            body(ds(i * size, size), i)

    cp_g = local(g_in, gf.at[krow])
    cp_gk = local(g_in.at[:, kcol], grf.at[krow])
    cp_ql = local(ql_in, qlf.at[krow])
    cp_qr = local(qr_in, r_out)
    cp_l = local(l_in, l_out)
    local(w_in, wx, lcounter[0])
    for a, b in ((m_in, mx), (v_in, vx)):
        local(a.at[:, kcol], b.at[krow], lcounter[0])
    cp_own = pltpu.make_async_copy(gf.at[ds(0, cr)], gf.at[ds(0, cr)], ls.at[lcounter[0]])
    lcounter[0] += 1
    barrier = pltpu.get_barrier_semaphore()
    partners = [device(dx=2), device(dk=1)]
    for step in (1, -1):
        partners += [device(dx=step), device(dy=step), device(dk=1, dy=step)]
    for partner in partners:
        pl.semaphore_signal(barrier, inc=1, device_id=partner, device_id_type=MESH)
    pl.semaphore_wait(barrier, len(partners))

    d_gk = remote(g_in.at[:, ocol], grf.at[krow], dk=1, send=batch_first)
    d_g0 = remote(g_in, gf.at[krow], dk=1, send=batch_first)
    d_ql = remote(ql_in, qlf.at[krow], dk=1)
    own_receive, d_own_all = group(mx)
    d_own = [remote(a.at[:, ocol], b.at[krow], dk=1, send=batch_first, receive=own_receive) for a, b in ((m_in, mx), (v_in, vx))]
    d_g0.start()
    d_gk.start()
    d_ql.start()

    def grow(s, half):
        return ds((s * 2 + k) * rc + half * (rc // 2), rc // 2)

    def slot_rows(n, start=0, size=None, cols=None):
        size = n if size is None else size
        return lambda s, half: (ds(s * n + start + half * (size // 2), size // 2, 8), slice(None) if cols is None else ds(*cols))

    def whole(s):
        return ds((s * 2 + k) * rc, rc)

    def tiles(n, cols=None):
        cols = slice(None) if cols is None else ds(*cols)
        return {"near": (ds(0, n), cols), "rest": (ds(0, 2 * n), cols)}

    x1 = Ring(gf, grow, "dx", **tiles(rc), batch=batch_xy)
    x2 = Ring(qr, slot_rows(hc), "dx", **tiles(hc), batch=batch_x, forward=[
        ([slot_rows(hc, cols=(c * hc + at, n)) for c in range(2)], (ds(0, hc), ds(0, 2 * n))) for at, n in pieces])
    x3 = [Ring(h, slot_rows(cr, cols=piece), "dx", **tiles(cr, piece), batch=batch_x, joined=True) for piece in pieces]
    x4 = [Ring(nb, slot_rows(cr, cols=piece), "dx", **tiles(cr, piece), batch=batch_xy, joined=p == 0) for p, piece in enumerate(pieces)]
    y1 = Ring(gr, slot_rows(cr), "dy", **tiles(cr), batch=batch_xy, joined=True)
    y2 = Ring(qlr, slot_rows(cr, start=k * rc, size=rc), "dy", **tiles(rc), total=ds(0, 3 * rc), joined=True)
    three = pl.ds(0, 3)
    y3 = Ring(qlc, lambda s, half: (pl.ds(1 + 2 * half, 2 - half), (y - s + 4) % 4), "dy", absolute=True,
              near=(three, 0), rest=(three, pl.ds(0, 2)), total=(three, three), joined=True)
    near_receive, d_g_near = group(gf.at[ds(0, cr)])
    d_g = {s: remote(gf.at[whole(s)], gf.at[whole(s)], dk=1, send=batch_first, receive=None if s == 2 else near_receive) for s in OTHERS}

    def prow(s, c):
        return ds((s * 2 + c) * rc, rc)

    p_src, p_fwd, q_src, q_fwd = {}, {}, {}, {}
    p_send, q_send = new(sends, N_SEND), new(sends, N_SEND)
    p_all, q_all = (arrival(px.at[ds(0, 4 * rc)], None, i) for i in (p_send, q_send))
    for s in (0, *OTHERS):
        pi, qi = new(receives, N_RECEIVE), new(receives, N_RECEIVE)
        p_src[s] = remote(gf.at[prow(s, 0), kcol], px.at[prow(s, 0)], dy=1, send=p_send, receive=pi)
        p_fwd[s] = remote(px.at[prow(s, 0)], px.at[prow(s, 0)], dy=1, send=p_send, receive=pi)
        q_src[s] = remote(gf.at[prow(s, 1), kcol], px.at[prow(s, 1)], dy=-1, send=q_send, receive=qi)
        q_fwd[s] = remote(px.at[prow(s, 1)], px.at[prow(s, 1)], dy=-1, send=q_send, receive=qi)

    def panel_source(s):
        @pl.when(d == 0)
        def _():
            p_src[s].start()
            q_src[s].start()

    def panel_first(s):
        @pl.when(d == 1)
        def _():
            p_fwd[s].wait_recv()
            p_fwd[s].start()

        @pl.when(d == 3)
        def _():
            q_fwd[s].wait_recv()
            q_fwd[s].start()

    def panel_second(s):
        @pl.when(d == 2)
        def _():
            p_fwd[s].wait_recv()
            p_fwd[s].start()
            q_fwd[s].wait_recv()
            q_fwd[s].start()

    def panel_third(s):
        @pl.when(d == 3)
        def _():
            p_fwd[s].wait_recv()

        @pl.when(d == 1)
        def _():
            q_fwd[s].wait_recv()

    def h_part(s, cols):
        t = (d + s) % 4
        part = dot(gr[ds(t * cr, cr), :], qr[ds(s * hc, hc), cols])
        if s == 0:
            hp[:, cols] = part
        else:
            hp[:, cols] += part

    units = 2 * (cc // nt)

    def split_right(p):
        base = p * kk

        def body(r, i):
            for q, piece in enumerate(split_three(gf[ds(base + i * (kk // 8), kk // 8, 8), :])):
                rhs3[ds(q * kk + i * (kk // 8), kk // 8, 8), :] = piece

        chunked(kk, 8, body)
        if p == 0:
            for q in range(3):
                la[ds(q * rc, rc), :] = rhs3[ds(q * kk + k * rc, rc, rc), :]

    def split_left(p):
        base = p * kk

        @pl.when(d == 0)
        def _():
            chunked(kk, 4, lambda r, i: px.__setitem__(
                (ds(base + i * (kk // 4), kk // 4, 8), slice(None)), gf[ds(base + i * (kk // 4), kk // 4, 8), kcol]))

        def body(cols, i):
            for q, piece in enumerate(split_three(px[ds(base + i * tb, tb, 8), :].T)):
                lhs3[ds(q * hc, hc), cols] = piece

        chunked(kk, kk // tb, body)

    def product(p, first, last):
        @pl.loop(first, last)
        def _(i):
            m, j = i // (cc // nt), i % (cc // nt)
            rows = ds(m * (hc // 2), hc // 2)
            cols = ds(j * nt, nt)
            acc = sum(dot(lhs3[ds(a * hc + m * (hc // 2), hc // 2), :], rhs3[ds(b * kk, kk), cols]) for a, b in SIX_PASSES)
            if p == 0:
                r_out[rows, cols] = BETA2 * r_out[rows, cols] + (1.0 - BETA2) * acc
            else:
                r_out[rows, cols] += (1.0 - BETA2) * acc

    def l_slot(s):
        e = (x - y - s + 8) % 4
        at = [ds(q * kk + (s % 2) * cr, cr) for q in range(3)]
        high = dot(la[...], rhs3[at[0], :], NT)
        middle = dot(la[ds(0, 2 * rc), :], rhs3[at[1], :], NT)
        low = dot(la[ds(0, rc), :], rhs3[at[2], :], NT)
        lc[ds(e * rc, rc), :] = high[:rc] + (high[rc:2 * rc] + middle[:rc]) + (high[2 * rc:] + middle[rc:] + low)

    class Sum:
        def __init__(self, buf, far, near, n, send=None):
            self.buf, self.far_, self.near_, self.n = buf, far, near, n
            hn = n // 2
            self.rows = lambda e, half: ds(e * n + half * hn, hn)
            if send is None:
                send = new(sends, N_SEND)
                pending.append(arrival(buf.at[ds(0, 3 * n)], None, send))
            receive, self.arrivals = group(near)
            rows = self.rows
            self.fa = remote(buf.at[rows(2, 0)], far.at[ds(0, hn)], dy=1, send=send)
            self.fb = remote(buf.at[rows(2, 1)], far.at[ds(hn, hn)], dy=-1, send=send)
            self.r1b, self.r1a = self.to(1, 1, 0, send, receive), self.to(1, 0, 0, send, receive)
            self.l1a, self.l1b = self.to(3, 0, 1, send, receive), self.to(3, 1, 1, send, receive)

        def to(self, e, half, side, send, receive):
            return remote(self.buf.at[self.rows(e, half)], self.near_.at[ds(side * self.n + half * (self.n // 2), self.n // 2)],
                          dy=(1, -1)[side], send=send, receive=receive)

        def begin(self):
            for c in (self.fa, self.fb, self.r1b, self.l1a):
                c.start()

        def middle(self):
            hn, buf, far, rows = self.n // 2, self.buf, self.far_, self.rows
            self.fa.wait_recv()
            buf[rows(1, 0), :] += far[ds(0, hn), :]
            self.r1a.start()
            self.fb.wait_recv()
            buf[rows(3, 1), :] += far[ds(hn, hn), :]
            self.l1b.start()

        def finish(self):
            self.arrivals.wait_recv()

        def total(self, start, size):
            n = self.n
            return self.buf[ds(start, size, 8), :] + (self.near_[ds(start, size, 8), :] + self.near_[ds(n + start, size, 8), :])

    class RowSum(Sum):
        def to(self, e, half, side, send, receive):
            hn = self.n // 2
            return remote(self.buf.at[self.rows(e, half)], self.near_.at[ds(side * hn, hn), kcol], dk=half - k + 2,
                          dy=(1, -1)[side], send=send, receive=receive)

    cp_g.wait()
    x1.own()
    d_g0.wait_recv()
    panel_source(0)
    cp_gk.wait()
    d_gk.wait_recv()
    chunked(cr, 4, lambda r, i: gr.__setitem__((r, slice(None)), grf[r, :].astype(BF16)))
    y1.own()
    cp_ql.wait()
    d_ql.wait_recv()
    qlr[ds(0, cr), :] = qlf[...].astype(BF16)
    y2.own()
    for c in d_own:
        c.start()
    cp_qr.wait()
    chunked(hc, 8, lambda r, i: qr.__setitem__((r, slice(None)), r_out[r, :].astype(BF16)))
    cp_r = local(r_in, r_out)
    x1.fwd()
    x2.own()
    panel_first(0)
    y1.fwd()
    y2.fwd()
    x1.near()
    d_g[1].start()
    d_g[3].start()
    d_g_near.wait_recv()
    panel_source(1)
    panel_source(3)
    y1.far()
    h_part(0, ocol)
    h_part(0, kcol)
    x1.far()
    d_g[2].start()
    d_g[2].wait_recv()
    panel_source(2)
    y2.far()
    q_receive, d_q_all = group(qlr.at[ds(0, 3 * rc)])
    q_send = new(sends, N_SEND)
    pending.append(arrival(qlr.at[ds(0, 3 * rc)], None, q_send))
    for s in OTHERS:
        at = ds(s * cr + k * rc, rc)
        remote(qlr.at[at], qlr.at[at], dk=1, send=q_send, receive=q_receive).start()
    d_q_all.wait_recv()
    qlc[0] = qlr[ds(d * cr, cr), :].reshape(4, rq, qlr.shape[1])
    across_receive, across_all = group(qlc.at[three, 0])
    across_send = new(sends, N_SEND)
    across = []
    for s in OTHERS:
        t = (y - x - s + 8) % 4
        across.append(remote(qlr.at[ds(t * cr + y * rq, rq, rq)], qlc.at[s, y], dx=s, send=across_send, receive=across_receive))
    over_send = new(sends, N_SEND)
    over = remote(qlc.at[pl.ds(1, 3), y], qlc.at[pl.ds(1, 3), y], dk=1, send=over_send)
    sent = [arrival(qlc.at[three, 0], None, across_send), over]

    @pl.when(k == 1)
    def _():
        for c in across:
            c.start()

    split_right(0)
    panel_first(1)
    panel_second(0)
    panel_first(3)
    panel_second(1)
    panel_third(0)
    x2.fwd()
    panel_first(2)
    panel_second(3)
    panel_third(1)
    cp_r.wait()
    split_left(0)
    product(0, 0, units)
    x2.near()
    for s in (1, 3):
        h_part(s, ocol)
        h_part(s, kcol)
    @pl.when(k == 1)
    def _():
        across_all.wait_recv()
        over.start()

    pl.when(k == 0)(over.wait_recv)
    y3.own()
    panel_second(2)
    panel_third(3)

    def columns(core, piece):
        at, n = pieces[piece]
        return ds(core * hc + at, n, 128)

    d_h = [remote(hp.at[:, columns(1 - k, p)], hx.at[:, ds(*pieces[p])], dk=1, send=batch_first) for p in range(2)]

    def h_send(p):
        x2.far((p,))
        h_part(2, columns(1 - k, p))
        d_h[p].start()
        h_part(2, columns(k, p))

    def h_finish(p):
        d_h[p].wait_recv()
        h[ds(0, cr), ds(*pieces[p])] = (hp[:, columns(k, p)] + hx[:, ds(*pieces[p])]).astype(BF16)
        x3[p].own()

    h_send(0)
    h_finish(0)
    l_slot(0)
    l_slot(1)
    y3.fwd()
    split_right(1)
    l_slot(2)
    l_slot(3)
    l_sum = Sum(lc, lf, ln, rc)
    l_sum.begin()
    h_send(1)
    x3[0].fwd()
    h_finish(1)
    panel_third(2)
    split_left(1)
    product(1, 0, units // 5)
    cp_own.wait()
    d_own_all.wait_recv()

    def moments(p):
        x3[p].far()
        cols = ds(*pieces[p])
        rot[:, cols] = dot(qlt[...], h[:, cols])

        def body(r, i):
            rotated = rot[r, cols]
            new_first = BETA1 * mx[r, cols] + (1.0 - BETA1) * rotated
            new_second = BETA2 * vx[r, cols] + (1.0 - BETA2) * rotated * rotated
            mx[r, cols] = new_first
            vx[r, cols] = new_second
            direction = (new_first / BIAS_ONE) / (jnp.sqrt(new_second / BIAS_TWO) + EPS)
            nb[r, cols] = direction.astype(BF16)

        chunked(cr, 10 if cr % 160 == 0 else 1, body)

    y3.far()
    qlt[...] = qlc[...].reshape(4 * cr, qlc.shape[3]).T
    moments(0)
    x3[1].fwd()
    x4[0].own()
    l_sum.middle()
    product(1, units // 5, units * 3 // 5)
    moments(1)
    x4[0].fwd()
    x4[1].own()
    out_receive, outs_all = group(mx)
    for buf, out in ((mx, m_out), (vx, v_out)):
        remote(buf.at[orow], out.at[:, kcol], dk=1, send=batch_last, receive=out_receive).start()
        out[:, kcol] = buf[krow, :]
    product(1, units * 3 // 5, units)

    d_k = [remote(kb.at[ds(k * cr, cr), ds(*piece)], kb.at[ds(k * cr, cr), ds(*piece)], dk=1, send=batch_last) for piece in pieces]

    def k_part(p, slots):
        cols = ds(*pieces[p])
        return sum(dot(qlr[ds(((d + s) % 4) * cr, cr), :], nb[ds(s * cr, cr), cols]) for s in slots)

    def u_part(e, p, core, half=None):
        s = (x - y - e + 8) % 4
        at, n = pieces[p]
        start, size = (0, cr) if half is None else (half * rc, rc)
        part = dot(kb[ds(core * cr + start, size, rc), ds(at, n)], qr[ds(s * hc, hc), ds(core * hc + at, n, 128)], NT)
        return ds(e * cr + start, size), part

    def u_add(*which):
        rows, part = u_part(*which)
        uc[rows, :] += part

    x4[0].far()
    kb[ds(k * cr, cr), ds(*pieces[0])] = k_part(0, range(4)).astype(BF16)
    d_k[0].start()
    x4[1].fwd()
    @pl.when(d != 3)
    def _():
        p_all.wait_send()

    @pl.when(d != 1)
    def _():
        q_all.wait_send()

    d_k[0].wait_recv()
    for e in (2, 1, 3, 0):
        rows, part = u_part(e, 0, 0)
        uc[rows, :] = part + u_part(e, 0, 1)[1]
    x4[1].near()
    rot[:, ds(*pieces[1])] = k_part(1, (0, 1, 3))
    x4[1].far()
    kb[ds(k * cr, cr), ds(*pieces[1])] = (rot[:, ds(*pieces[1])] + k_part(1, (2,))).astype(BF16)
    d_k[1].start()
    u_sum = RowSum(uc, uf, un, cr, batch_last)
    for e in (2, 1):
        u_add(e, 1, k)
    d_k[1].wait_recv()
    u_add(2, 1, 1 - k, 0)
    u_sum.fa.start()
    u_add(2, 1, 1 - k, 1)
    u_sum.fb.start()
    u_add(1, 1, 1 - k)
    u_sum.r1b.start()
    u_add(3, 1, k)
    u_add(3, 1, 1 - k)
    u_sum.l1a.start()
    u_add(0, 1, k)
    u_add(0, 1, 1 - k)
    d_u = remote(uc.at[orow], uo, dk=1, send=batch_last)
    d_u.start()
    l_sum.finish()
    cp_l.wait()
    l_out[...] = BETA2 * l_out[...] + (1.0 - BETA2) * l_sum.total(0, rc)
    outs_all.wait_recv()
    u_sum.middle()
    d_u.wait_recv()
    u_sum.finish()
    for mine, cols in ((True, kcol), (False, ocol)):
        total = (uc[krow, :] if mine else uo[...]) + (un[ds(0, rc), cols] + un[ds(rc, rc), cols])
        w_out[:, cols] = wx[:, cols] - LR * total
    for c in pending:
        c.wait_send()
    for batch in (batch_x, batch_xy, batch_first, batch_last):
        batch.wait()

    @pl.when(k == 1)
    def _():
        for c in sent:
            c.wait_send()


def write_kernel(*refs):
    n = (len(refs) - 1) // 2
    copies = [pltpu.make_async_copy(a, b, refs[-1].at[i]) for i, (a, b) in enumerate(zip(refs, refs[n:-1]))]
    for c in copies:
        c.start()
    for c in copies:
        c.wait()


def solution(mesh):
    tile_spec = P(("layer", "row"), "col")

    def step(weight, grad_in, mom_first, mom_second, stat_left, stat_right, basis_left, basis_right):
        rc, cc = grad_in.shape
        cr, hc, q = 2 * rc, cc // 2, basis_left.shape[1]
        scratch = [
            ((4 * cr, cc), F32), ((4 * cr, hc), F32), ((4 * hc, cc), BF16),
            ((cr, hc), F32), ((4 * cr, hc), BF16),
            ((cr, q), F32), ((4 * cr, q), BF16), ((4, 4, cr // 4, q), BF16), ((q, 4 * cr), BF16),
            ((rc, cc), F32), ((cr, hc), F32), ((cr, hc), F32),
            ((4 * cr, hc), BF16), ((4 * cr, hc), BF16), ((cr, cc), F32),
            ((cr, hc), F32),
            ((2 * cr, hc), BF16), ((cr, hc), F32), ((cr, cc), F32), ((rc, hc), F32),
            ((4 * rc, q), F32), ((rc, q), F32), ((2 * rc, q), F32),
            ((3 * hc, 2 * cr), BF16), ((6 * cr, cc), BF16), ((3 * rc, cc), BF16),
        ]
        args = (weight, grad_in, mom_first, mom_second, stat_left, stat_right, basis_left, basis_right)
        vmem_spec, any_spec = pl.BlockSpec(memory_space=pltpu.VMEM), pl.BlockSpec(memory_space=pl.ANY)
        outs = tuple(jax.ShapeDtypeStruct(a.shape, F32) for a in (weight, mom_first, mom_second, stat_left, stat_right))
        results = pl.pallas_call(
            kernel,
            out_shape=outs,
            in_specs=[pl.BlockSpec(memory_space=pltpu.HBM)] * 8,
            out_specs=(vmem_spec,) * 5,
            scratch_shapes=[pltpu.VMEM(s, t) for s, t in scratch]
            + [pltpu.SemaphoreType.DMA((n,)) for n in (N_SEND, N_RECEIVE, N_LOCAL)],
            compiler_params=pltpu.CompilerParams(collective_id=0, has_side_effects=True, vmem_limit_bytes=VMEM_BYTES),
        )(*(pltpu.with_memory_space_constraint(a, pltpu.HBM) for a in args))
        return pl.pallas_call(
            write_kernel,
            out_shape=outs,
            in_specs=[any_spec] * 5,
            out_specs=(any_spec,) * 5,
            scratch_shapes=[pltpu.SemaphoreType.DMA((len(outs),))],
            compiler_params=pltpu.CompilerParams(vmem_limit_bytes=1_000_000),
        )(*(pltpu.with_memory_space_constraint(a, pltpu.VMEM) for a in results))

    return jax.shard_map(step, mesh=mesh, in_specs=(tile_spec,) * 8, out_specs=(tile_spec,) * 5, check_vma=False)
```

```python
import math

import jax
import jax.numpy as jnp
from jax import lax
from jax.experimental import pallas as pl
from jax.experimental.pallas import tpu as pltpu
from jax.sharding import PartitionSpec as P

BETA1 = 0.9
BETA2 = 0.9
EPS = 1e-8
LR = 0.1
STEP = 10
BIAS_ONE = 1.0 - BETA1 ** STEP
BIAS_TWO = 1.0 - BETA2 ** STEP
MESH = pl.DeviceIdType.MESH
OTHERS = (1, 3, 2)
N_SEND, N_RECEIVE, N_LOCAL = 13, 60, 7
VMEM_BYTES = 50_000_000
F32 = jnp.float32
BF16 = jnp.bfloat16
SIX_PASSES = [(a, b) for a in range(3) for b in range(3 - a)]
NN, NT = (((1,), (i,)) for i in range(2))


def dot(a, b, dims=NN):
    return lax.dot_general(a, b, (dims, ((), ())), preferred_element_type=F32)


def split_three(a):
    hi = a.astype(BF16)
    rest = a - hi.astype(F32)
    mid = rest.astype(BF16)
    return hi, mid, (rest - mid.astype(F32)).astype(BF16)


def kernel(w_in, g_in, m_in, v_in, l_in, r_in, ql_in, qr_in, w_out, m_out, v_out, l_out, r_out,
           gf, px, qr, grf, gr, qlf, qlr, qlc, qlt, wx, mx, vx, h, nb, hp, hx, kb, uf, un, uo,
           lc, lf, ln, lhs3, rhs3, la, ss, rs, ls):
    rc, cc = g_in.shape
    cr, hc = 2 * rc, cc // 2
    kk = 2 * cr
    nt = 256 if cc % 256 == 0 else cc
    tb = 128 if kk % 128 == 0 else kk
    row, y = lax.axis_index("row"), lax.axis_index("col")
    x, k = row // 2, row % 2
    d = (y - x + 4) % 4
    rq = cr // 4
    uc, rot = px, grf
    pa = 128 * (hc * 2 // 5 // 128) if hc % 128 == 0 else hc // 2
    pieces = ((0, pa), (pa, hc - pa))

    def ds(start, size, unit=None):
        return pl.ds(start if isinstance(start, int) else pl.multiple_of(start, unit or size), size)

    kcol, ocol = ds(k * hc, hc), ds((1 - k) * hc, hc)
    krow, orow = ds(k * rc, rc), ds((1 - k) * rc, rc)

    sends, receives, pending = [0], [0], []

    def new(counter, limit):
        counter[0] += 1
        assert counter[0] <= limit
        return counter[0] - 1

    def device(dx=0, dk=0, dy=0):
        return {"row": ((x + dx + 4) % 4) * 2 + (k + dk) % 2, "col": (y + dy + 4) % 4}

    class Batch:
        def __init__(self):
            self.semaphore, self.bytes = new(sends, N_SEND), 0

        def wait(self):
            rows, rest = divmod(self.bytes, cc * gf.dtype.itemsize)
            assert rest == 0 and rows <= gf.shape[0]
            arrival(gf.at[ds(0, rows)], None, self.semaphore).wait_send()

    def remote(src, dst, dx=0, dk=0, dy=0, send=None, receive=None):
        if isinstance(send, Batch):
            send.bytes += math.prod(src.shape) * jnp.dtype(src.dtype).itemsize
            index = send.semaphore
        else:
            index = new(sends, N_SEND) if send is None else send
        copy = pltpu.make_async_remote_copy(
            src_ref=src, dst_ref=dst, send_sem=ss.at[index],
            recv_sem=rs.at[new(receives, N_RECEIVE) if receive is None else receive],
            device_id=device(dx, dk, dy), device_id_type=MESH)
        if send is None:
            pending.append(copy)
        return copy

    def arrival(view, receive, send=0):
        return remote(view, view, dk=1, send=send, receive=receive or 0)

    def group(view):
        receive = new(receives, N_RECEIVE)
        return receive, arrival(view, receive)

    batch_x, batch_xy, batch_first, batch_last = (Batch() for _ in range(4))
    lcounter = [0]

    def local(src, dst, index=None):
        if index is None:
            index = lcounter[0]
            lcounter[0] += 1
        assert index < N_LOCAL
        copy = pltpu.make_async_copy(src, dst, ls.at[index])
        copy.start()
        return copy

    class Ring:
        def __init__(self, buf, at, axis, near, rest, total=None, batch=None, forward=None, absolute=False, joined=False):
            if batch is None:
                batch = new(sends, N_SEND)
                pending.append(arrival(buf.at[total], None, batch))

            def cp(s0, half, s1, step, receive, at=at):
                return remote(buf.at[at(s0, half)], buf.at[at(s0 if absolute else s1, half)], send=batch, receive=receive, **{axis: step})

            self.ra, self.lb = cp(0, 0, 1, 1, None), cp(0, 1, 3, -1, None)
            second, self.near_ = group(buf.at[rest if joined else near])
            self.rb, self.la = cp(0, 1, 1, 1, second), cp(0, 0, 3, -1, second)
            self.fr, self.fl, self.far_ = [], [], []
            for parts, view in forward or [([at], near)]:
                last, wait = (second, self.near_) if joined else group(buf.at[view])
                self.far_.append(wait)
                for part in parts:
                    self.fr.append(cp(1, 0, 2, 1, last, part))
                    self.fl.append(cp(3, 1, 2, -1, last, part))

        def own(self):
            for c in (self.ra, self.lb, self.rb, self.la):
                c.start()

        def fwd(self):
            for first, parts in ((self.ra, self.fr), (self.lb, self.fl)):
                first.wait_recv()
                for c in parts:
                    c.start()

        def near(self):
            self.near_.wait_recv()

        def far(self, parts=None):
            for i in range(len(self.far_)) if parts is None else parts:
                self.far_[i].wait_recv()

    def chunked(total, parts, body):
        size = total // parts

        @pl.loop(0, parts)
        def _(i):
            body(ds(i * size, size), i)

    cp_g = local(g_in, gf.at[krow])
    cp_gk = local(g_in.at[:, kcol], grf.at[krow])
    cp_ql = local(ql_in, qlf.at[krow])
    cp_qr = local(qr_in, r_out)
    cp_l = local(l_in, l_out)
    local(w_in, wx, lcounter[0])
    for a, b in ((m_in, mx), (v_in, vx)):
        local(a.at[:, kcol], b.at[krow], lcounter[0])
    cp_own = pltpu.make_async_copy(gf.at[ds(0, cr)], gf.at[ds(0, cr)], ls.at[lcounter[0]])
    lcounter[0] += 1
    barrier = pltpu.get_barrier_semaphore()
    partners = [device(dx=2), device(dk=1)]
    for step in (1, -1):
        partners += [device(dx=step), device(dy=step), device(dk=1, dy=step)]
    for partner in partners:
        pl.semaphore_signal(barrier, inc=1, device_id=partner, device_id_type=MESH)
    pl.semaphore_wait(barrier, len(partners))

    d_gk = remote(g_in.at[:, ocol], grf.at[krow], dk=1, send=batch_first)
    d_g0 = remote(g_in, gf.at[krow], dk=1, send=batch_first)
    d_ql = remote(ql_in, qlf.at[krow], dk=1)
    own_receive, d_own_all = group(mx)
    d_own = [remote(a.at[:, ocol], b.at[krow], dk=1, send=batch_first, receive=own_receive) for a, b in ((m_in, mx), (v_in, vx))]
    d_g0.start()
    d_gk.start()
    d_ql.start()

    def grow(s, half):
        return ds((s * 2 + k) * rc + half * (rc // 2), rc // 2)

    def slot_rows(n, start=0, size=None, cols=None):
        size = n if size is None else size
        return lambda s, half: (ds(s * n + start + half * (size // 2), size // 2, 8), slice(None) if cols is None else ds(*cols))

    def whole(s):
        return ds((s * 2 + k) * rc, rc)

    def tiles(n, cols=None):
        cols = slice(None) if cols is None else ds(*cols)
        return {"near": (ds(0, n), cols), "rest": (ds(0, 2 * n), cols)}

    x1 = Ring(gf, grow, "dx", **tiles(rc), batch=batch_xy)
    x2 = Ring(qr, slot_rows(hc), "dx", **tiles(hc), batch=batch_x, forward=[
        ([slot_rows(hc, cols=(c * hc + at, n)) for c in range(2)], (ds(0, hc), ds(0, 2 * n))) for at, n in pieces])
    x3 = [Ring(h, slot_rows(cr, cols=piece), "dx", **tiles(cr, piece), batch=batch_x, joined=True) for piece in pieces]
    x4 = [Ring(nb, slot_rows(cr, cols=piece), "dx", **tiles(cr, piece), batch=batch_xy, joined=p == 0) for p, piece in enumerate(pieces)]
    y1 = Ring(gr, slot_rows(cr), "dy", **tiles(cr), batch=batch_xy, joined=True)
    y2 = Ring(qlr, slot_rows(cr, start=k * rc, size=rc), "dy", **tiles(rc), total=ds(0, 3 * rc), joined=True)
    three = pl.ds(0, 3)
    y3 = Ring(qlc, lambda s, half: (pl.ds(1 + 2 * half, 2 - half), (y - s + 4) % 4), "dy", absolute=True,
              near=(three, 0), rest=(three, pl.ds(0, 2)), total=(three, three), joined=True)
    near_receive, d_g_near = group(gf.at[ds(0, cr)])
    d_g = {s: remote(gf.at[whole(s)], gf.at[whole(s)], dk=1, send=batch_first, receive=None if s == 2 else near_receive) for s in OTHERS}

    def prow(s, c):
        return ds((s * 2 + c) * rc, rc)

    p_src, p_fwd, q_src, q_fwd = {}, {}, {}, {}
    p_send, q_send = new(sends, N_SEND), new(sends, N_SEND)
    p_all, q_all = (arrival(px.at[ds(0, 4 * rc)], None, i) for i in (p_send, q_send))
    for s in (0, *OTHERS):
        pi, qi = new(receives, N_RECEIVE), new(receives, N_RECEIVE)
        p_src[s] = remote(gf.at[prow(s, 0), kcol], px.at[prow(s, 0)], dy=1, send=p_send, receive=pi)
        p_fwd[s] = remote(px.at[prow(s, 0)], px.at[prow(s, 0)], dy=1, send=p_send, receive=pi)
        q_src[s] = remote(gf.at[prow(s, 1), kcol], px.at[prow(s, 1)], dy=-1, send=q_send, receive=qi)
        q_fwd[s] = remote(px.at[prow(s, 1)], px.at[prow(s, 1)], dy=-1, send=q_send, receive=qi)

    def panel_source(s):
        @pl.when(d == 0)
        def _():
            p_src[s].start()
            q_src[s].start()

    def panel_first(s):
        @pl.when(d == 1)
        def _():
            p_fwd[s].wait_recv()
            p_fwd[s].start()

        @pl.when(d == 3)
        def _():
            q_fwd[s].wait_recv()
            q_fwd[s].start()

    def panel_second(s):
        @pl.when(d == 2)
        def _():
            p_fwd[s].wait_recv()
            p_fwd[s].start()
            q_fwd[s].wait_recv()
            q_fwd[s].start()

    def panel_third(s):
        @pl.when(d == 3)
        def _():
            p_fwd[s].wait_recv()

        @pl.when(d == 1)
        def _():
            q_fwd[s].wait_recv()

    def h_part(s, cols):
        t = (d + s) % 4
        part = dot(gr[ds(t * cr, cr), :], qr[ds(s * hc, hc), cols])
        if s == 0:
            hp[:, cols] = part
        else:
            hp[:, cols] += part

    units = 2 * (cc // nt)

    def split_right(p):
        base = p * kk

        def body(r, i):
            for q, piece in enumerate(split_three(gf[ds(base + i * (kk // 8), kk // 8, 8), :])):
                rhs3[ds(q * kk + i * (kk // 8), kk // 8, 8), :] = piece

        chunked(kk, 8, body)
        if p == 0:
            for q in range(3):
                la[ds(q * rc, rc), :] = rhs3[ds(q * kk + k * rc, rc, rc), :]

    def split_left(p):
        base = p * kk

        @pl.when(d == 0)
        def _():
            chunked(kk, 4, lambda r, i: px.__setitem__(
                (ds(base + i * (kk // 4), kk // 4, 8), slice(None)), gf[ds(base + i * (kk // 4), kk // 4, 8), kcol]))

        def body(cols, i):
            for q, piece in enumerate(split_three(px[ds(base + i * tb, tb, 8), :].T)):
                lhs3[ds(q * hc, hc), cols] = piece

        chunked(kk, kk // tb, body)

    def product(p, first, last):
        @pl.loop(first, last)
        def _(i):
            m, j = i // (cc // nt), i % (cc // nt)
            rows = ds(m * (hc // 2), hc // 2)
            cols = ds(j * nt, nt)
            acc = sum(dot(lhs3[ds(a * hc + m * (hc // 2), hc // 2), :], rhs3[ds(b * kk, kk), cols]) for a, b in SIX_PASSES)
            if p == 0:
                r_out[rows, cols] = BETA2 * r_out[rows, cols] + (1.0 - BETA2) * acc
            else:
                r_out[rows, cols] += (1.0 - BETA2) * acc

    def l_slot(s):
        e = (x - y - s + 8) % 4
        at = [ds(q * kk + (s % 2) * cr, cr) for q in range(3)]
        high = dot(la[...], rhs3[at[0], :], NT)
        middle = dot(la[ds(0, 2 * rc), :], rhs3[at[1], :], NT)
        low = dot(la[ds(0, rc), :], rhs3[at[2], :], NT)
        lc[ds(e * rc, rc), :] = high[:rc] + (high[rc:2 * rc] + middle[:rc]) + (high[2 * rc:] + middle[rc:] + low)

    class Sum:
        def __init__(self, buf, far, near, n, send=None):
            self.buf, self.far_, self.near_, self.n = buf, far, near, n
            hn = n // 2
            self.rows = lambda e, half: ds(e * n + half * hn, hn)
            if send is None:
                send = new(sends, N_SEND)
                pending.append(arrival(buf.at[ds(0, 3 * n)], None, send))
            receive, self.arrivals = group(near)
            rows = self.rows
            self.fa = remote(buf.at[rows(2, 0)], far.at[ds(0, hn)], dy=1, send=send)
            self.fb = remote(buf.at[rows(2, 1)], far.at[ds(hn, hn)], dy=-1, send=send)
            self.r1b, self.r1a = self.to(1, 1, 0, send, receive), self.to(1, 0, 0, send, receive)
            self.l1a, self.l1b = self.to(3, 0, 1, send, receive), self.to(3, 1, 1, send, receive)

        def to(self, e, half, side, send, receive):
            return remote(self.buf.at[self.rows(e, half)], self.near_.at[ds(side * self.n + half * (self.n // 2), self.n // 2)],
                          dy=(1, -1)[side], send=send, receive=receive)

        def begin(self):
            for c in (self.fa, self.fb, self.r1b, self.l1a):
                c.start()

        def middle(self):
            hn, buf, far, rows = self.n // 2, self.buf, self.far_, self.rows
            self.fa.wait_recv()
            buf[rows(1, 0), :] += far[ds(0, hn), :]
            self.r1a.start()
            self.fb.wait_recv()
            buf[rows(3, 1), :] += far[ds(hn, hn), :]
            self.l1b.start()

        def finish(self):
            self.arrivals.wait_recv()

        def total(self, start, size):
            n = self.n
            return self.buf[ds(start, size, 8), :] + (self.near_[ds(start, size, 8), :] + self.near_[ds(n + start, size, 8), :])

    class RowSum(Sum):
        def to(self, e, half, side, send, receive):
            hn = self.n // 2
            return remote(self.buf.at[self.rows(e, half)], self.near_.at[ds(side * hn, hn), kcol], dk=half - k + 2,
                          dy=(1, -1)[side], send=send, receive=receive)

    cp_g.wait()
    x1.own()
    d_g0.wait_recv()
    panel_source(0)
    cp_gk.wait()
    d_gk.wait_recv()
    chunked(cr, 4, lambda r, i: gr.__setitem__((r, slice(None)), grf[r, :].astype(BF16)))
    y1.own()
    cp_ql.wait()
    d_ql.wait_recv()
    qlr[ds(0, cr), :] = qlf[...].astype(BF16)
    y2.own()
    for c in d_own:
        c.start()
    cp_qr.wait()
    chunked(hc, 8, lambda r, i: qr.__setitem__((r, slice(None)), r_out[r, :].astype(BF16)))
    cp_r = local(r_in, r_out)
    x1.fwd()
    x2.own()
    panel_first(0)
    y1.fwd()
    y2.fwd()
    x1.near()
    d_g[1].start()
    d_g[3].start()
    d_g_near.wait_recv()
    panel_source(1)
    panel_source(3)
    y1.far()
    h_part(0, ocol)
    h_part(0, kcol)
    x1.far()
    d_g[2].start()
    d_g[2].wait_recv()
    panel_source(2)
    y2.far()
    q_receive, d_q_all = group(qlr.at[ds(0, 3 * rc)])
    q_send = new(sends, N_SEND)
    pending.append(arrival(qlr.at[ds(0, 3 * rc)], None, q_send))
    for s in OTHERS:
        at = ds(s * cr + k * rc, rc)
        remote(qlr.at[at], qlr.at[at], dk=1, send=q_send, receive=q_receive).start()
    d_q_all.wait_recv()
    qlc[0] = qlr[ds(d * cr, cr), :].reshape(4, rq, qlr.shape[1])
    across_receive, across_all = group(qlc.at[three, 0])
    across_send = new(sends, N_SEND)
    across = []
    for s in OTHERS:
        t = (y - x - s + 8) % 4
        across.append(remote(qlr.at[ds(t * cr + y * rq, rq, rq)], qlc.at[s, y], dx=s, send=across_send, receive=across_receive))
    over_send = new(sends, N_SEND)
    over = remote(qlc.at[pl.ds(1, 3), y], qlc.at[pl.ds(1, 3), y], dk=1, send=over_send)
    sent = [arrival(qlc.at[three, 0], None, across_send), over]

    @pl.when(k == 1)
    def _():
        for c in across:
            c.start()

    split_right(0)
    panel_first(1)
    panel_second(0)
    panel_first(3)
    panel_second(1)
    panel_third(0)
    x2.fwd()
    panel_first(2)
    panel_second(3)
    panel_third(1)
    cp_r.wait()
    split_left(0)
    product(0, 0, units)
    x2.near()
    for s in (1, 3):
        h_part(s, ocol)
        h_part(s, kcol)
    @pl.when(k == 1)
    def _():
        across_all.wait_recv()
        over.start()

    pl.when(k == 0)(over.wait_recv)
    y3.own()
    panel_second(2)
    panel_third(3)

    def columns(core, piece):
        at, n = pieces[piece]
        return ds(core * hc + at, n, 128)

    d_h = [remote(hp.at[:, columns(1 - k, p)], hx.at[:, ds(*pieces[p])], dk=1, send=batch_first) for p in range(2)]

    def h_send(p):
        x2.far((p,))
        h_part(2, columns(1 - k, p))
        d_h[p].start()
        h_part(2, columns(k, p))

    def h_finish(p):
        d_h[p].wait_recv()
        h[ds(0, cr), ds(*pieces[p])] = (hp[:, columns(k, p)] + hx[:, ds(*pieces[p])]).astype(BF16)
        x3[p].own()

    h_send(0)
    h_finish(0)
    l_slot(0)
    l_slot(1)
    y3.fwd()
    split_right(1)
    l_slot(2)
    l_slot(3)
    l_sum = Sum(lc, lf, ln, rc)
    l_sum.begin()
    h_send(1)
    x3[0].fwd()
    h_finish(1)
    panel_third(2)
    split_left(1)
    product(1, 0, units // 5)
    cp_own.wait()
    d_own_all.wait_recv()

    def moments(p):
        x3[p].far()
        cols = ds(*pieces[p])
        rot[:, cols] = dot(qlt[...], h[:, cols])

        def body(r, i):
            rotated = rot[r, cols]
            new_first = BETA1 * mx[r, cols] + (1.0 - BETA1) * rotated
            new_second = BETA2 * vx[r, cols] + (1.0 - BETA2) * rotated * rotated
            mx[r, cols] = new_first
            vx[r, cols] = new_second
            direction = (new_first / BIAS_ONE) / (jnp.sqrt(new_second / BIAS_TWO) + EPS)
            nb[r, cols] = direction.astype(BF16)

        chunked(cr, 10 if cr % 160 == 0 else 1, body)

    y3.far()
    qlt[...] = qlc[...].reshape(4 * cr, qlc.shape[3]).T
    moments(0)
    x3[1].fwd()
    x4[0].own()
    l_sum.middle()
    product(1, units // 5, units * 3 // 5)
    moments(1)
    x4[0].fwd()
    x4[1].own()
    out_receive, outs_all = group(mx)
    for buf, out in ((mx, m_out), (vx, v_out)):
        remote(buf.at[orow], out.at[:, kcol], dk=1, send=batch_last, receive=out_receive).start()
        out[:, kcol] = buf[krow, :]
    product(1, units * 3 // 5, units)

    d_k = [remote(kb.at[ds(k * cr, cr), ds(*piece)], kb.at[ds(k * cr, cr), ds(*piece)], dk=1, send=batch_last) for piece in pieces]

    def k_part(p, slots):
        cols = ds(*pieces[p])
        return sum(dot(qlr[ds(((d + s) % 4) * cr, cr), :], nb[ds(s * cr, cr), cols]) for s in slots)

    def u_part(e, p, core, half=None):
        s = (x - y - e + 8) % 4
        at, n = pieces[p]
        start, size = (0, cr) if half is None else (half * rc, rc)
        part = dot(kb[ds(core * cr + start, size, rc), ds(at, n)], qr[ds(s * hc, hc), ds(core * hc + at, n, 128)], NT)
        return ds(e * cr + start, size), part

    def u_add(*which):
        rows, part = u_part(*which)
        uc[rows, :] += part

    x4[0].far()
    kb[ds(k * cr, cr), ds(*pieces[0])] = k_part(0, range(4)).astype(BF16)
    d_k[0].start()
    x4[1].fwd()
    @pl.when(d != 3)
    def _():
        p_all.wait_send()

    @pl.when(d != 1)
    def _():
        q_all.wait_send()

    d_k[0].wait_recv()
    for e in (2, 1, 3, 0):
        rows, part = u_part(e, 0, 0)
        uc[rows, :] = part + u_part(e, 0, 1)[1]
    x4[1].near()
    rot[:, ds(*pieces[1])] = k_part(1, (0, 1, 3))
    x4[1].far()
    kb[ds(k * cr, cr), ds(*pieces[1])] = (rot[:, ds(*pieces[1])] + k_part(1, (2,))).astype(BF16)
    d_k[1].start()
    u_sum = RowSum(uc, uf, un, cr, batch_last)
    for e in (2, 1):
        u_add(e, 1, k)
    d_k[1].wait_recv()
    u_add(2, 1, 1 - k, 0)
    u_sum.fa.start()
    u_add(2, 1, 1 - k, 1)
    u_sum.fb.start()
    u_add(1, 1, 1 - k)
    u_sum.r1b.start()
    u_add(3, 1, k)
    u_add(3, 1, 1 - k)
    u_sum.l1a.start()
    u_add(0, 1, k)
    u_add(0, 1, 1 - k)
    d_u = remote(uc.at[orow], uo, dk=1, send=batch_last)
    d_u.start()
    l_sum.finish()
    cp_l.wait()
    l_out[...] = BETA2 * l_out[...] + (1.0 - BETA2) * l_sum.total(0, rc)
    outs_all.wait_recv()
    u_sum.middle()
    d_u.wait_recv()
    u_sum.finish()
    for mine, cols in ((True, kcol), (False, ocol)):
        total = (uc[krow, :] if mine else uo[...]) + (un[ds(0, rc), cols] + un[ds(rc, rc), cols])
        w_out[:, cols] = wx[:, cols] - LR * total
    for c in pending:
        c.wait_send()
    for batch in (batch_x, batch_xy, batch_first, batch_last):
        batch.wait()

    @pl.when(k == 1)
    def _():
        for c in sent:
            c.wait_send()


def write_kernel(*refs):
    n = (len(refs) - 1) // 2
    copies = [pltpu.make_async_copy(a, b, refs[-1].at[i]) for i, (a, b) in enumerate(zip(refs, refs[n:-1]))]
    for c in copies:
        c.start()
    for c in copies:
        c.wait()


def solution(mesh):
    tile_spec = P(("layer", "row"), "col")

    def step(weight, grad_in, mom_first, mom_second, stat_left, stat_right, basis_left, basis_right):
        rc, cc = grad_in.shape
        cr, hc, q = 2 * rc, cc // 2, basis_left.shape[1]
        scratch = [
            ((4 * cr, cc), F32), ((4 * cr, hc), F32), ((4 * hc, cc), BF16),
            ((cr, hc), F32), ((4 * cr, hc), BF16),
            ((cr, q), F32), ((4 * cr, q), BF16), ((4, 4, cr // 4, q), BF16), ((q, 4 * cr), BF16),
            ((rc, cc), F32), ((cr, hc), F32), ((cr, hc), F32),
            ((4 * cr, hc), BF16), ((4 * cr, hc), BF16), ((cr, cc), F32),
            ((cr, hc), F32),
            ((2 * cr, hc), BF16), ((cr, hc), F32), ((cr, cc), F32), ((rc, hc), F32),
            ((4 * rc, q), F32), ((rc, q), F32), ((2 * rc, q), F32),
            ((3 * hc, 2 * cr), BF16), ((6 * cr, cc), BF16), ((3 * rc, cc), BF16),
        ]
        args = (weight, grad_in, mom_first, mom_second, stat_left, stat_right, basis_left, basis_right)
        vmem_spec, any_spec = pl.BlockSpec(memory_space=pltpu.VMEM), pl.BlockSpec(memory_space=pl.ANY)
        outs = tuple(jax.ShapeDtypeStruct(a.shape, F32) for a in (weight, mom_first, mom_second, stat_left, stat_right))
        results = pl.pallas_call(
            kernel,
            out_shape=outs,
            in_specs=[pl.BlockSpec(memory_space=pltpu.HBM)] * 8,
            out_specs=(vmem_spec,) * 5,
            scratch_shapes=[pltpu.VMEM(s, t) for s, t in scratch]
            + [pltpu.SemaphoreType.DMA((n,)) for n in (N_SEND, N_RECEIVE, N_LOCAL)],
            compiler_params=pltpu.CompilerParams(collective_id=0, has_side_effects=True, vmem_limit_bytes=VMEM_BYTES),
        )(*(pltpu.with_memory_space_constraint(a, pltpu.HBM) for a in args))
        return pl.pallas_call(
            write_kernel,
            out_shape=outs,
            in_specs=[any_spec] * 5,
            out_specs=(any_spec,) * 5,
            scratch_shapes=[pltpu.SemaphoreType.DMA((len(outs),))],
            compiler_params=pltpu.CompilerParams(vmem_limit_bytes=1_000_000),
        )(*(pltpu.with_memory_space_constraint(a, pltpu.VMEM) for a in results))

    return jax.shard_map(step, mesh=mesh, in_specs=(tile_spec,) * 8, out_specs=(tile_spec,) * 5, check_vma=False)
```

```python
import math

import jax
import jax.numpy as jnp
from jax import lax
from jax.experimental import pallas as pl
from jax.experimental.pallas import tpu as pltpu
from jax.sharding import PartitionSpec as P

BETA1 = 0.9
BETA2 = 0.9
EPS = 1e-8
LR = 0.1
STEP = 10
BIAS_ONE = 1.0 - BETA1 ** STEP
BIAS_TWO = 1.0 - BETA2 ** STEP
MESH = pl.DeviceIdType.MESH
OTHERS = (1, 3, 2)
N_SEND, N_RECEIVE, N_LOCAL = 13, 61, 7
VMEM_BYTES = 50_000_000
F32 = jnp.float32
BF16 = jnp.bfloat16
SIX_PASSES = [(a, b) for a in range(3) for b in range(3 - a)]
NN, NT = (((1,), (i,)) for i in range(2))


def dot(a, b, dims=NN):
    return lax.dot_general(a, b, (dims, ((), ())), preferred_element_type=F32)


def split_three(a):
    hi = a.astype(BF16)
    rest = a - hi.astype(F32)
    mid = rest.astype(BF16)
    return hi, mid, (rest - mid.astype(F32)).astype(BF16)


def kernel(w_in, g_in, m_in, v_in, l_in, r_in, ql_in, qr_in, w_out, m_out, v_out, l_out, r_out,
           gf, px, qr, grf, gr, qlf, qlr, qlc, qlt, wx, mx, vx, h, nb, hp, hx, kb, uf, un, uo,
           lc, lf, ln, lhs3, rhs3, la, ss, rs, ls):
    rc, cc = g_in.shape
    cr, hc = 2 * rc, cc // 2
    kk = 2 * cr
    nt = 256 if cc % 256 == 0 else cc
    tb = 128 if kk % 128 == 0 else kk
    row, y = lax.axis_index("row"), lax.axis_index("col")
    x, k = row // 2, row % 2
    d = (y - x + 4) % 4
    rq = cr // 4
    uc, rot = px, grf
    pa = 128 * (hc * 2 // 5 // 128) if hc % 128 == 0 else hc // 2
    pieces = ((0, pa), (pa, hc - pa))

    def ds(start, size, unit=None):
        return pl.ds(start if isinstance(start, int) else pl.multiple_of(start, unit or size), size)

    kcol, ocol = ds(k * hc, hc), ds((1 - k) * hc, hc)
    krow, orow = ds(k * rc, rc), ds((1 - k) * rc, rc)

    sends, receives, pending = [0], [0], []

    def new(counter, limit):
        counter[0] += 1
        assert counter[0] <= limit
        return counter[0] - 1

    def device(dx=0, dk=0, dy=0):
        return {"row": ((x + dx + 4) % 4) * 2 + (k + dk) % 2, "col": (y + dy + 4) % 4}

    class Batch:
        def __init__(self):
            self.semaphore, self.bytes = new(sends, N_SEND), 0

        def wait(self):
            rows, rest = divmod(self.bytes, cc * gf.dtype.itemsize)
            assert rest == 0 and rows <= gf.shape[0]
            arrival(gf.at[ds(0, rows)], None, self.semaphore).wait_send()

    def remote(src, dst, dx=0, dk=0, dy=0, send=None, receive=None):
        if isinstance(send, Batch):
            send.bytes += math.prod(src.shape) * jnp.dtype(src.dtype).itemsize
            index = send.semaphore
        else:
            index = new(sends, N_SEND) if send is None else send
        copy = pltpu.make_async_remote_copy(
            src_ref=src, dst_ref=dst, send_sem=ss.at[index],
            recv_sem=rs.at[new(receives, N_RECEIVE) if receive is None else receive],
            device_id=device(dx, dk, dy), device_id_type=MESH)
        if send is None:
            pending.append(copy)
        return copy

    def arrival(view, receive, send=0):
        return remote(view, view, dk=1, send=send, receive=receive or 0)

    def group(view):
        receive = new(receives, N_RECEIVE)
        return receive, arrival(view, receive)

    batch_x, batch_xy, batch_first, batch_last = (Batch() for _ in range(4))
    lcounter = [0]

    def local(src, dst, index=None):
        if index is None:
            index = lcounter[0]
            lcounter[0] += 1
        assert index < N_LOCAL
        copy = pltpu.make_async_copy(src, dst, ls.at[index])
        copy.start()
        return copy

    class Ring:
        def __init__(self, buf, at, axis, near, rest, total=None, batch=None, forward=None, absolute=False, joined=False):
            if batch is None:
                batch = new(sends, N_SEND)
                pending.append(arrival(buf.at[total], None, batch))

            def cp(s0, half, s1, step, receive, at=at):
                return remote(buf.at[at(s0, half)], buf.at[at(s0 if absolute else s1, half)], send=batch, receive=receive, **{axis: step})

            self.ra, self.lb = cp(0, 0, 1, 1, None), cp(0, 1, 3, -1, None)
            second, self.near_ = group(buf.at[rest if joined else near])
            self.rb, self.la = cp(0, 1, 1, 1, second), cp(0, 0, 3, -1, second)
            self.fr, self.fl, self.far_ = [], [], []
            for parts, view in forward or [([at], near)]:
                last, wait = (second, self.near_) if joined else group(buf.at[view])
                self.far_.append(wait)
                for part in parts:
                    self.fr.append(cp(1, 0, 2, 1, last, part))
                    self.fl.append(cp(3, 1, 2, -1, last, part))

        def own(self):
            for c in (self.ra, self.lb, self.rb, self.la):
                c.start()

        def fwd(self):
            for first, parts in ((self.ra, self.fr), (self.lb, self.fl)):
                first.wait_recv()
                for c in parts:
                    c.start()

        def near(self):
            self.near_.wait_recv()

        def far(self, parts=None):
            for i in range(len(self.far_)) if parts is None else parts:
                self.far_[i].wait_recv()

    def chunked(total, parts, body):
        size = total // parts

        @pl.loop(0, parts)
        def _(i):
            body(ds(i * size, size), i)

    cp_g = local(g_in, gf.at[krow])
    cp_gk = local(g_in.at[:, kcol], grf.at[krow])
    cp_ql = local(ql_in, qlf.at[krow])
    cp_qr = local(qr_in, r_out)
    cp_l = local(l_in, l_out)
    local(w_in, wx, lcounter[0])
    for a, b in ((m_in, mx), (v_in, vx)):
        local(a.at[:, kcol], b.at[krow], lcounter[0])
    cp_own = pltpu.make_async_copy(gf.at[ds(0, cr)], gf.at[ds(0, cr)], ls.at[lcounter[0]])
    lcounter[0] += 1
    barrier = pltpu.get_barrier_semaphore()
    partners = [device(dx=2), device(dk=1)]
    for step in (1, -1):
        partners += [device(dx=step), device(dy=step), device(dk=1, dy=step)]
    for partner in partners:
        pl.semaphore_signal(barrier, inc=1, device_id=partner, device_id_type=MESH)
    pl.semaphore_wait(barrier, len(partners))

    d_gk = remote(g_in.at[:, ocol], grf.at[krow], dk=1, send=batch_first)
    d_g0 = remote(g_in, gf.at[krow], dk=1, send=batch_first)
    d_ql = remote(ql_in, qlf.at[krow], dk=1)
    own_receive, d_own_all = group(mx)
    d_own = [remote(a.at[:, ocol], b.at[krow], dk=1, send=batch_first, receive=own_receive) for a, b in ((m_in, mx), (v_in, vx))]
    d_g0.start()
    d_gk.start()
    d_ql.start()

    def grow(s, half):
        return ds((s * 2 + k) * rc + half * (rc // 2), rc // 2)

    def slot_rows(n, start=0, size=None, cols=None):
        size = n if size is None else size
        return lambda s, half: (ds(s * n + start + half * (size // 2), size // 2, 8), slice(None) if cols is None else ds(*cols))

    def whole(s):
        return ds((s * 2 + k) * rc, rc)

    def tiles(n, cols=None):
        cols = slice(None) if cols is None else ds(*cols)
        return {"near": (ds(0, n), cols), "rest": (ds(0, 2 * n), cols)}

    x1 = Ring(gf, grow, "dx", **tiles(rc), batch=batch_xy)
    x2 = Ring(qr, slot_rows(hc), "dx", **tiles(hc), batch=batch_x, forward=[
        ([slot_rows(hc, cols=(c * hc + at, n)) for c in range(2)], (ds(0, hc), ds(0, 2 * n))) for at, n in pieces])
    x3 = [Ring(h, slot_rows(cr, cols=piece), "dx", **tiles(cr, piece), batch=batch_x, joined=True) for piece in pieces]
    x4 = [Ring(nb, slot_rows(cr, cols=piece), "dx", **tiles(cr, piece), batch=batch_xy, joined=p == 0) for p, piece in enumerate(pieces)]
    y1 = Ring(gr, slot_rows(cr), "dy", **tiles(cr), batch=batch_xy, joined=True)
    y2 = Ring(qlr, slot_rows(cr, start=k * rc, size=rc), "dy", **tiles(rc), total=ds(0, 3 * rc), joined=True)
    three = pl.ds(0, 3)
    y3 = Ring(qlc, lambda s, half: (pl.ds(1 + 2 * half, 2 - half), (y - s + 4) % 4), "dy", absolute=True,
              near=(three, 0), rest=(three, pl.ds(0, 2)), total=(three, three), joined=True)
    near_receive, d_g_near = group(gf.at[ds(0, cr)])
    d_g = {s: remote(gf.at[whole(s)], gf.at[whole(s)], dk=1, send=batch_first, receive=None if s == 2 else near_receive) for s in OTHERS}

    def prow(s, c):
        return ds((s * 2 + c) * rc, rc)

    p_src, p_fwd, q_src, q_fwd = {}, {}, {}, {}
    p_send, q_send = new(sends, N_SEND), new(sends, N_SEND)
    p_all, q_all = (arrival(px.at[ds(0, 4 * rc)], None, i) for i in (p_send, q_send))
    for s in (0, *OTHERS):
        pi, qi = new(receives, N_RECEIVE), new(receives, N_RECEIVE)
        p_src[s] = remote(gf.at[prow(s, 0), kcol], px.at[prow(s, 0)], dy=1, send=p_send, receive=pi)
        p_fwd[s] = remote(px.at[prow(s, 0)], px.at[prow(s, 0)], dy=1, send=p_send, receive=pi)
        q_src[s] = remote(gf.at[prow(s, 1), kcol], px.at[prow(s, 1)], dy=-1, send=q_send, receive=qi)
        q_fwd[s] = remote(px.at[prow(s, 1)], px.at[prow(s, 1)], dy=-1, send=q_send, receive=qi)

    def panel_source(s):
        @pl.when(d == 0)
        def _():
            p_src[s].start()
            q_src[s].start()

    def panel_first(s):
        @pl.when(d == 1)
        def _():
            p_fwd[s].wait_recv()
            p_fwd[s].start()

        @pl.when(d == 3)
        def _():
            q_fwd[s].wait_recv()
            q_fwd[s].start()

    def panel_second(s):
        @pl.when(d == 2)
        def _():
            p_fwd[s].wait_recv()
            p_fwd[s].start()
            q_fwd[s].wait_recv()
            q_fwd[s].start()

    def panel_third(s):
        @pl.when(d == 3)
        def _():
            p_fwd[s].wait_recv()

        @pl.when(d == 1)
        def _():
            q_fwd[s].wait_recv()

    def h_part(s, cols):
        t = (d + s) % 4
        part = dot(gr[ds(t * cr, cr), :], qr[ds(s * hc, hc), cols])
        if s == 0:
            hp[:, cols] = part
        else:
            hp[:, cols] += part

    units = 2 * (cc // nt)

    def split_right(p):
        base = p * kk

        def body(r, i):
            for q, piece in enumerate(split_three(gf[ds(base + i * (kk // 8), kk // 8, 8), :])):
                rhs3[ds(q * kk + i * (kk // 8), kk // 8, 8), :] = piece

        chunked(kk, 8, body)
        if p == 0:
            for q in range(3):
                la[ds(q * rc, rc), :] = rhs3[ds(q * kk + k * rc, rc, rc), :]

    def split_left(p):
        base = p * kk

        @pl.when(d == 0)
        def _():
            chunked(kk, 4, lambda r, i: px.__setitem__(
                (ds(base + i * (kk // 4), kk // 4, 8), slice(None)), gf[ds(base + i * (kk // 4), kk // 4, 8), kcol]))

        def body(cols, i):
            for q, piece in enumerate(split_three(px[ds(base + i * tb, tb, 8), :].T)):
                lhs3[ds(q * hc, hc), cols] = piece

        chunked(kk, kk // tb, body)

    def product(p, first, last):
        @pl.loop(first, last)
        def _(i):
            m, j = i // (cc // nt), i % (cc // nt)
            rows = ds(m * (hc // 2), hc // 2)
            cols = ds(j * nt, nt)
            acc = sum(dot(lhs3[ds(a * hc + m * (hc // 2), hc // 2), :], rhs3[ds(b * kk, kk), cols]) for a, b in SIX_PASSES)
            if p == 0:
                r_out[rows, cols] = BETA2 * r_out[rows, cols] + (1.0 - BETA2) * acc
            else:
                r_out[rows, cols] += (1.0 - BETA2) * acc

    def l_slot(s):
        e = (x - y - s + 8) % 4
        at = [ds(q * kk + (s % 2) * cr, cr) for q in range(3)]
        high = dot(la[...], rhs3[at[0], :], NT)
        middle = dot(la[ds(0, 2 * rc), :], rhs3[at[1], :], NT)
        low = dot(la[ds(0, rc), :], rhs3[at[2], :], NT)
        lc[ds(e * rc, rc), :] = high[:rc] + (high[rc:2 * rc] + middle[:rc]) + (high[2 * rc:] + middle[rc:] + low)

    class Sum:
        def __init__(self, buf, far, near, n, send=None):
            self.buf, self.far_, self.near_, self.n = buf, far, near, n
            hn = n // 2
            self.rows = lambda e, half: ds(e * n + half * hn, hn)
            if send is None:
                send = new(sends, N_SEND)
                pending.append(arrival(buf.at[ds(0, 3 * n)], None, send))
            receive, self.arrivals = group(near)
            rows = self.rows
            self.fa = remote(buf.at[rows(2, 0)], far.at[ds(0, hn)], dy=1, send=send)
            self.fb = remote(buf.at[rows(2, 1)], far.at[ds(hn, hn)], dy=-1, send=send)
            self.r1b, self.r1a = self.to(1, 1, 0, send, receive), self.to(1, 0, 0, send, receive)
            self.l1a, self.l1b = self.to(3, 0, 1, send, receive), self.to(3, 1, 1, send, receive)

        def to(self, e, half, side, send, receive):
            return remote(self.buf.at[self.rows(e, half)], self.near_.at[ds(side * self.n + half * (self.n // 2), self.n // 2)],
                          dy=(1, -1)[side], send=send, receive=receive)

        def begin(self):
            for c in (self.fa, self.fb, self.r1b, self.l1a):
                c.start()

        def middle(self):
            hn, buf, far, rows = self.n // 2, self.buf, self.far_, self.rows
            self.fa.wait_recv()
            buf[rows(1, 0), :] += far[ds(0, hn), :]
            self.r1a.start()
            self.fb.wait_recv()
            buf[rows(3, 1), :] += far[ds(hn, hn), :]
            self.l1b.start()

        def finish(self):
            self.arrivals.wait_recv()

        def total(self, start, size):
            n = self.n
            return self.buf[ds(start, size, 8), :] + (self.near_[ds(start, size, 8), :] + self.near_[ds(n + start, size, 8), :])

    class RowSum(Sum):
        def to(self, e, half, side, send, receive):
            hn = self.n // 2
            return remote(self.buf.at[self.rows(e, half)], self.near_.at[ds(side * hn, hn), kcol], dk=half - k + 2,
                          dy=(1, -1)[side], send=send, receive=receive)

    cp_g.wait()
    x1.own()
    d_g0.wait_recv()
    panel_source(0)
    cp_gk.wait()
    d_gk.wait_recv()
    chunked(cr, 4, lambda r, i: gr.__setitem__((r, slice(None)), grf[r, :].astype(BF16)))
    y1.own()
    cp_ql.wait()
    d_ql.wait_recv()
    qlr[ds(0, cr), :] = qlf[...].astype(BF16)
    y2.own()
    for c in d_own:
        c.start()
    cp_qr.wait()
    chunked(hc, 8, lambda r, i: qr.__setitem__((r, slice(None)), r_out[r, :].astype(BF16)))
    cp_r = local(r_in, r_out)
    x1.fwd()
    x2.own()
    panel_first(0)
    y1.fwd()
    y2.fwd()
    x1.near()
    d_g[1].start()
    d_g[3].start()
    d_g_near.wait_recv()
    panel_source(1)
    panel_source(3)
    y1.far()
    h_part(0, ocol)
    h_part(0, kcol)
    x1.far()
    d_g[2].start()
    d_g[2].wait_recv()
    panel_source(2)
    y2.far()
    q_receive, d_q_all = group(qlr.at[ds(0, 3 * rc)])
    q_send = new(sends, N_SEND)
    pending.append(arrival(qlr.at[ds(0, 3 * rc)], None, q_send))
    for s in OTHERS:
        at = ds(s * cr + k * rc, rc)
        remote(qlr.at[at], qlr.at[at], dk=1, send=q_send, receive=q_receive).start()
    d_q_all.wait_recv()
    qlc[0] = qlr[ds(d * cr, cr), :].reshape(4, rq, qlr.shape[1])
    across_receive, across_all = group(qlc.at[three, 0])
    across_send = new(sends, N_SEND)
    across = []
    for s in OTHERS:
        t = (y - x - s + 8) % 4
        across.append(remote(qlr.at[ds(t * cr + y * rq, rq, rq)], qlc.at[s, y], dx=s, send=across_send, receive=across_receive))
    over_send = new(sends, N_SEND)
    over = remote(qlc.at[pl.ds(1, 3), y], qlc.at[pl.ds(1, 3), y], dk=1, send=over_send)
    sent = [arrival(qlc.at[three, 0], None, across_send), over]

    @pl.when(k == 1)
    def _():
        for c in across:
            c.start()

    split_right(0)
    panel_first(1)
    panel_second(0)
    panel_first(3)
    panel_second(1)
    panel_third(0)
    x2.fwd()
    panel_first(2)
    panel_second(3)
    panel_third(1)
    cp_r.wait()
    split_left(0)
    product(0, 0, units)
    x2.near()
    for s in (1, 3):
        h_part(s, ocol)
        h_part(s, kcol)
    @pl.when(k == 1)
    def _():
        across_all.wait_recv()
        over.start()

    pl.when(k == 0)(over.wait_recv)
    y3.own()
    panel_second(2)
    panel_third(3)

    def columns(core, piece):
        at, n = pieces[piece]
        return ds(core * hc + at, n, 128)

    d_h = [remote(hp.at[:, columns(1 - k, p)], hx.at[:, ds(*pieces[p])], dk=1, send=batch_first) for p in range(2)]

    def h_send(p):
        x2.far((p,))
        h_part(2, columns(1 - k, p))
        d_h[p].start()
        h_part(2, columns(k, p))

    def h_finish(p):
        d_h[p].wait_recv()
        h[ds(0, cr), ds(*pieces[p])] = (hp[:, columns(k, p)] + hx[:, ds(*pieces[p])]).astype(BF16)
        x3[p].own()

    h_send(0)
    h_finish(0)
    l_slot(0)
    l_slot(1)
    y3.fwd()
    split_right(1)
    l_slot(2)
    l_slot(3)
    l_sum = Sum(lc, lf, ln, rc)
    l_sum.begin()
    h_send(1)
    x3[0].fwd()
    h_finish(1)
    panel_third(2)
    split_left(1)
    product(1, 0, units // 5)
    cp_own.wait()
    d_own_all.wait_recv()

    def moments(p):
        x3[p].far()
        cols = ds(*pieces[p])
        rot[:, cols] = dot(qlt[...], h[:, cols])

        def body(r, i):
            rotated = rot[r, cols]
            new_first = BETA1 * mx[r, cols] + (1.0 - BETA1) * rotated
            new_second = BETA2 * vx[r, cols] + (1.0 - BETA2) * rotated * rotated
            mx[r, cols] = new_first
            vx[r, cols] = new_second
            direction = (new_first / BIAS_ONE) / (jnp.sqrt(new_second / BIAS_TWO) + EPS)
            nb[r, cols] = direction.astype(BF16)

        chunked(cr, 10 if cr % 160 == 0 else 1, body)

    y3.far()
    qlt[...] = qlc[...].reshape(4 * cr, qlc.shape[3]).T
    moments(0)
    x3[1].fwd()
    x4[0].own()
    l_sum.middle()
    product(1, units // 5, units * 3 // 5)
    moments(1)
    x4[0].fwd()
    x4[1].own()
    out_receive, outs_all = group(mx)
    for buf, out in ((mx, m_out), (vx, v_out)):
        remote(buf.at[orow], out.at[:, kcol], dk=1, send=batch_last, receive=out_receive).start()
        out[:, kcol] = buf[krow, :]
    product(1, units * 3 // 5, units)

    first, last = (ds(*piece) for piece in pieces)
    d_k = remote(kb.at[ds(k * cr, cr), first], kb.at[ds(k * cr, cr), first], dk=1, send=batch_last)
    halves = [(ds(half * rc, rc), ds(k * cr + half * rc, rc), ds((d + 2) % 4 * cr + half * rc, rc)) for half in range(2)]
    d_kb = [remote(kb.at[at, last], kb.at[at, last], dk=1, send=batch_last) for _, at, _ in halves]

    def k_part(p, slots):
        cols = ds(*pieces[p])
        return sum(dot(qlr[ds(((d + s) % 4) * cr, cr), :], nb[ds(s * cr, cr), cols]) for s in slots)

    def u_part(e, p, core, half=None):
        s = (x - y - e + 8) % 4
        at, n = pieces[p]
        start, size = (0, cr) if half is None else (half * rc, rc)
        part = dot(kb[ds(core * cr + start, size, rc), ds(at, n)], qr[ds(s * hc, hc), ds(core * hc + at, n, 128)], NT)
        return ds(e * cr + start, size), part

    def u_add(*which):
        rows, part = u_part(*which)
        uc[rows, :] += part

    x4[0].far()
    kb[ds(k * cr, cr), ds(*pieces[0])] = k_part(0, range(4)).astype(BF16)
    d_k.start()
    x4[1].fwd()
    @pl.when(d != 3)
    def _():
        p_all.wait_send()

    @pl.when(d != 1)
    def _():
        q_all.wait_send()

    d_k.wait_recv()
    for e in (2, 1, 3, 0):
        rows, part = u_part(e, 0, 0)
        uc[rows, :] = part + u_part(e, 0, 1)[1]
    x4[1].near()
    rot[:, ds(*pieces[1])] = k_part(1, (0, 1, 3))
    x4[1].far()
    for (rows, at, left), c in zip(halves, d_kb):
        kb[at, last] = (rot[rows, last] + dot(qlr[left, :], nb[ds(2 * cr, cr), last])).astype(BF16)
        c.start()
    u_sum = RowSum(uc, uf, un, cr, batch_last)
    for e in (2, 1):
        u_add(e, 1, k)
    d_kb[0].wait_recv()
    u_add(2, 1, 1 - k, 0)
    u_sum.fa.start()
    d_kb[1].wait_recv()
    u_add(2, 1, 1 - k, 1)
    u_sum.fb.start()
    u_add(1, 1, 1 - k)
    u_sum.r1b.start()
    u_add(3, 1, k)
    u_add(3, 1, 1 - k)
    u_sum.l1a.start()
    u_add(0, 1, k)
    u_add(0, 1, 1 - k)
    d_u = remote(uc.at[orow], uo, dk=1, send=batch_last)
    d_u.start()
    l_sum.finish()
    cp_l.wait()
    l_out[...] = BETA2 * l_out[...] + (1.0 - BETA2) * l_sum.total(0, rc)
    outs_all.wait_recv()
    u_sum.middle()
    d_u.wait_recv()
    u_sum.finish()
    for mine, cols in ((True, kcol), (False, ocol)):
        total = (uc[krow, :] if mine else uo[...]) + (un[ds(0, rc), cols] + un[ds(rc, rc), cols])
        w_out[:, cols] = wx[:, cols] - LR * total
    for c in pending:
        c.wait_send()
    for batch in (batch_x, batch_xy, batch_first, batch_last):
        batch.wait()

    @pl.when(k == 1)
    def _():
        for c in sent:
            c.wait_send()


def write_kernel(*refs):
    n = (len(refs) - 1) // 2
    copies = [pltpu.make_async_copy(a, b, refs[-1].at[i]) for i, (a, b) in enumerate(zip(refs, refs[n:-1]))]
    for c in copies:
        c.start()
    for c in copies:
        c.wait()


def solution(mesh):
    tile_spec = P(("layer", "row"), "col")

    def step(weight, grad_in, mom_first, mom_second, stat_left, stat_right, basis_left, basis_right):
        rc, cc = grad_in.shape
        cr, hc, q = 2 * rc, cc // 2, basis_left.shape[1]
        scratch = [
            ((4 * cr, cc), F32), ((4 * cr, hc), F32), ((4 * hc, cc), BF16),
            ((cr, hc), F32), ((4 * cr, hc), BF16),
            ((cr, q), F32), ((4 * cr, q), BF16), ((4, 4, cr // 4, q), BF16), ((q, 4 * cr), BF16),
            ((rc, cc), F32), ((cr, hc), F32), ((cr, hc), F32),
            ((4 * cr, hc), BF16), ((4 * cr, hc), BF16), ((cr, cc), F32),
            ((cr, hc), F32),
            ((2 * cr, hc), BF16), ((cr, hc), F32), ((cr, cc), F32), ((rc, hc), F32),
            ((4 * rc, q), F32), ((rc, q), F32), ((2 * rc, q), F32),
            ((3 * hc, 2 * cr), BF16), ((6 * cr, cc), BF16), ((3 * rc, cc), BF16),
        ]
        args = (weight, grad_in, mom_first, mom_second, stat_left, stat_right, basis_left, basis_right)
        vmem_spec, any_spec = pl.BlockSpec(memory_space=pltpu.VMEM), pl.BlockSpec(memory_space=pl.ANY)
        outs = tuple(jax.ShapeDtypeStruct(a.shape, F32) for a in (weight, mom_first, mom_second, stat_left, stat_right))
        results = pl.pallas_call(
            kernel,
            out_shape=outs,
            in_specs=[pl.BlockSpec(memory_space=pltpu.HBM)] * 8,
            out_specs=(vmem_spec,) * 5,
            scratch_shapes=[pltpu.VMEM(s, t) for s, t in scratch]
            + [pltpu.SemaphoreType.DMA((n,)) for n in (N_SEND, N_RECEIVE, N_LOCAL)],
            compiler_params=pltpu.CompilerParams(collective_id=0, has_side_effects=True, vmem_limit_bytes=VMEM_BYTES),
        )(*(pltpu.with_memory_space_constraint(a, pltpu.HBM) for a in args))
        return pl.pallas_call(
            write_kernel,
            out_shape=outs,
            in_specs=[any_spec] * 5,
            out_specs=(any_spec,) * 5,
            scratch_shapes=[pltpu.SemaphoreType.DMA((len(outs),))],
            compiler_params=pltpu.CompilerParams(vmem_limit_bytes=1_000_000),
        )(*(pltpu.with_memory_space_constraint(a, pltpu.VMEM) for a in results))

    return jax.shard_map(step, mesh=mesh, in_specs=(tile_spec,) * 8, out_specs=(tile_spec,) * 5, check_vma=False)
```
